32 devices in a mesh: dp: 8 (over z, y), tensor: 4 (over x, core).
Axes of the slice: x: 2, y: 2, z: 4, core: 2. Of those that a mesh axis runs over, the one named last changes fastest.
Arguments:
- layer_in: bfloat16 [16384, 768], P('dp'), may hold values from -6 to 6
- block_of: int32 [16, 1024], P('dp'), may hold values from 0 to 7, never falling along the last dimension, each value on 1 to 256 neighbouring positions
- block_links: int32 [16, 8, 8], P('dp'), may hold values 0 or 1
- w_query: bfloat16 [768, 768], P(None, 'tensor'), may hold values from -0.21875 to 0.21875
- b_query: float32 [768], P('tensor'), may hold values from -1.5 to 1.5
- w_key: bfloat16 [768, 768], P(None, 'tensor'), may hold values from -0.21875 to 0.21875
- w_value: bfloat16 [768, 768], P(None, 'tensor'), may hold values from -0.21875 to 0.21875
- b_value: float32 [768], P('tensor'), may hold values from -1.5 to 1.5
- w_out: bfloat16 [768, 768], P('tensor'), may hold values from -1.75 to 1.75
- b_out: float32 [768], replicated, may hold values from -1.5 to 1.5
- gain_one: float32 [768], replicated, may hold values from 0.5 to 1.5
- shift_one: float32 [768], replicated, may hold values from -1.5 to 1.5
- w_up: bfloat16 [768, 3072], P(None, 'tensor'), may hold values from -0.21875 to 0.21875
- b_up: float32 [3072], P('tensor'), may hold values from -1.5 to 1.5
- w_down: bfloat16 [3072, 768], P('tensor'), may hold values from -0.109375 to 0.109375
- b_down: float32 [768], replicated, may hold values from -1.5 to 1.5
- gain_two: float32 [768], replicated, may hold values from 0.5 to 1.5
- shift_two: float32 [768], replicated, may hold values from -1.5 to 1.5
- grad_out: bfloat16 [16384, 768], P(('dp', 'tensor')), may hold values from -6 to 6
Outputs:
- layer_out: bfloat16 [16384, 768], P(('dp', 'tensor'))
- grad_in: float32 [16384, 768], P(('dp', 'tensor'))
- grad_w_query: float32 [768, 768], P('dp', 'tensor')
- grad_b_query: float32 [768], P('tensor')
- grad_w_key: float32 [768, 768], P('dp', 'tensor')
- grad_w_value: float32 [768, 768], P('dp', 'tensor')
- grad_b_value: float32 [768], P('tensor')
- grad_w_out: float32 [768, 768], P('tensor', 'dp')
- grad_b_out: float32 [768], replicated
- grad_gain_one: float32 [768], replicated
- grad_shift_one: float32 [768], replicated
- grad_w_up: float32 [768, 3072], P('dp', 'tensor')
- grad_b_up: float32 [3072], P('tensor')
- grad_w_down: float32 [3072, 768], P('tensor', 'dp')
- grad_b_down: float32 [768], replicated
- grad_gain_two: float32 [768], replicated
- grad_shift_two: float32 [768], replicated
The draws below stay inside these ranges and needn't reach their ends.
Inputs may be any that keep to these rules, and one draw needn't show every extreme that they name: `block_of`: within a sequence the block numbers never fall and all 8 blocks occur; each block has 1 to 256 positions and one has exactly 256. `block_links`: only entries [sequence, i, j] with j < i are read.
All inputs are finite; a program needn't handle non-finite values. No bound on the sum of `block_links` on one device may be relied on, other than what follows from the above.
Results may differ from the reference program's by a relative error of at most 0.018.
Values may be sent and summed in bfloat16 or wider, within the bound.
No kernel may reach another device: no remote copies, remote signals or barrier semaphores. Data moves between devices by JAX's collectives and lax.ppermute only.
A program may use at most 128 MiB of HBM per device.

```python
import math
import jax
import jax.numpy as jnp
import numpy as np
from jax import lax

D = 768
HEADS = 12
FF = 3072
SEQ_LEN = 1024
NSEG = 8
BLOCK_MOST = 256
SEQ_DEV = 2
SEQUENCES = 16
TOKENS = 16384


def touch_ends(array, key, least, high):
    shape = array.shape
    index_at = [jax.random.randint(jax.random.fold_in(key, axis), (), 0, shape[axis]) for axis in range(len(shape))]
    array = array.at[tuple(index_at)].set(least)
    longest = shape.index(max(shape))
    index_at[longest] = (index_at[longest] + 1) % shape[longest]
    return array.at[tuple(index_at)].set(high)


def strengthened(drawn, stream_key, source, target, shards_of, factor):
    def block_of(position):
        return (jnp.arange(drawn.shape[position]) // (drawn.shape[position] // shards_of)).reshape((-1,) + (1,) * (drawn.ndim - 1 - position))

    one_side = jax.random.permutation(stream_key, shards_of)[block_of(target)]
    far = (block_of(target) + shards_of // 2) % shards_of
    return jnp.where((block_of(source) == one_side) | (block_of(source) == far), factor * drawn, drawn)


def level_of(own_key, extent, split, smallest, high):
    loudness = 1.0
    for axis_at, parts in split:
        steps = jax.random.uniform(jax.random.fold_in(jax.random.fold_in(own_key, 6), axis_at), (parts,), jnp.float32, smallest / len(split), high / len(split))
        loudness = loudness * jnp.repeat(jnp.exp(steps), extent[axis_at] // parts).reshape((-1,) + (1,) * (len(extent) - 1 - axis_at))
    return loudness


def length_profile(amount, total, most, slope):
    weights = [(1 << 20) // math.isqrt(rank ** slope) + 1 for rank in range(2, amount + 1)]
    surplus, counts = total - most - (amount - 1), [1] * (amount - 1)
    while surplus > 0:
        movable = [i for i in range(amount - 1) if counts[i] < most]
        mass, budget = sum([weights[i] for i in movable]), surplus
        for i in movable:
            addition = min(most - counts[i], max(1, budget * weights[i] // mass), surplus)
            counts[i] = counts[i] + addition
            surplus = surplus - addition
    return np.array([most] + counts)


def ragged_sizes(key, number_of, total, reach, lean):
    if number_of == 2:
        one = jax.random.randint(key, (), max(1, total - reach), min(reach, total - 1) + 1)
        return jnp.stack([one, total - one])
    sizes = jnp.asarray(length_profile(number_of, total, reach, lean), jnp.int32)
    couples = (number_of - 1) // 2
    source_of, taker = sizes[1:1 + 2 * couples:2], sizes[2:2 + 2 * couples:2]
    room = jnp.minimum(source_of - 1, reach - taker)
    moved = jax.random.randint(jax.random.fold_in(key, 1), (couples,), 0, 1 << 20) % (room + 1)
    sizes = sizes.at[1:1 + 2 * couples:2].set(source_of - moved).at[2:2 + 2 * couples:2].set(taker + moved)
    return sizes[jax.random.permutation(jax.random.fold_in(key, 2), number_of)]


def scatter_about(key, extent, width, bound, shards=(), kind=jnp.bfloat16):
    entries = jax.random.normal(key, extent, jnp.float32) * width
    if len(shards) > 0:
        entries = level_of(key, extent, shards, -0.22, 0.18) * entries
    return jnp.clip(entries, min=-bound, max=bound).astype(kind)


def gaussian_with(stream_key, extent, deviation, bound, shards, heavy, kind=jnp.bfloat16):
    entries = deviation * jax.random.normal(stream_key, extent, jnp.float32)
    if shards:
        entries = entries * level_of(stream_key, extent, shards, -0.22, 0.18)
    return jnp.clip(strengthened(entries, jax.random.fold_in(stream_key, 3), *heavy), -bound, bound).astype(kind)


def setup_inputs(seed: int = 0) -> dict:
    key_list = jax.random.split(jax.random.key(seed), 20)
    return {
        "layer_in": scatter_about(key_list[0], (TOKENS, D), 1.0, 6.0, ((0, 8),)),
        "block_of": jax.vmap(lambda own: jnp.searchsorted(jnp.cumsum(ragged_sizes(own, NSEG, SEQ_LEN, BLOCK_MOST, 1)), jnp.arange(SEQ_LEN), side="right"))(jax.random.split(key_list[1], SEQUENCES)).reshape((SEQUENCES, SEQ_LEN)).astype(jnp.int32),
        "block_links": touch_ends((jax.random.randint(key_list[2], (SEQUENCES, NSEG, NSEG), 0, 2) < 1).astype(jnp.int32), jax.random.fold_in(key_list[2], 1), 0, 1),
        "w_query": scatter_about(key_list[3], (D, D), D ** -0.5, 0.21875, ((1, 4),)),
        "b_query": scatter_about(key_list[4], (D,), 0.3, 1.5, ((0, 4),), jnp.float32),
        "w_key": scatter_about(key_list[5], (D, D), D ** -0.5, 0.21875, ((1, 4),)),
        "w_value": scatter_about(key_list[6], (D, D), D ** -0.5, 0.21875, ((1, 4),)),
        "b_value": scatter_about(key_list[7], (D,), 0.3, 1.5, ((0, 4),), jnp.float32),
        "w_out": scatter_about(key_list[8], (D, D), (D // 64) ** -0.5, 1.75, ((0, 4),)),
        "b_out": scatter_about(key_list[9], (D,), 0.3, 1.5, (), jnp.float32),
        "gain_one": jnp.clip(1.0 + 0.1 * jax.random.normal(key_list[10], (D,), jnp.float32), 0.5, 1.5),
        "shift_one": scatter_about(key_list[11], (D,), 0.3, 1.5, (), jnp.float32),
        "w_up": scatter_about(key_list[12], (D, FF), D ** -0.5, 0.21875, ((1, 4),)),
        "b_up": scatter_about(key_list[13], (FF,), 0.3, 1.5, ((0, 4),), jnp.float32),
        "w_down": scatter_about(key_list[14], (FF, D), FF ** -0.5, 0.109375, ((0, 4),)),
        "b_down": scatter_about(key_list[15], (D,), 0.3, 1.5, (), jnp.float32),
        "gain_two": jnp.clip(1.0 + 0.1 * jax.random.normal(key_list[16], (D,), jnp.float32), 0.5, 1.5),
        "shift_two": scatter_about(key_list[17], (D,), 0.3, 1.5, (), jnp.float32),
        "grad_out": gaussian_with(key_list[18], (TOKENS, D), 1.0, 6.0, ((0, 32),), (0, 1, 32, 2.75)),
    }


@jax.custom_vjp
def low(v):
    return lax.optimization_barrier(v.astype(jnp.bfloat16)).astype(jnp.float32)

@jax.custom_vjp
def low_back(v):
    return v

def low_keep(v):
    return (low(v), None)

def low_pass(kept, grad):
    return (grad,)

def back_keep(v):
    return (v, None)

def back_low(kept, grad):
    return (low(grad),)
low.defvjp(low_keep, low_pass)
low_back.defvjp(back_keep, back_low)
EPS = 1e-06
NEG = -1e+30
HIGH = lax.Precision.HIGHEST

def matmul(left, right):
    return jnp.dot(left, right, precision=HIGH, preferred_element_type=jnp.float32)

def layer_norm(values, gain, shift):
    centre = values - lax.optimization_barrier(jnp.mean(values, axis=-1, keepdims=True))
    return centre * lax.rsqrt(lax.optimization_barrier(jnp.mean(centre * centre, axis=-1, keepdims=True)) + EPS) * gain + shift

def attend(query, key, value, block_row, link_row):
    length = query.shape[0]
    head_dim = D // HEADS
    query_heads = query.reshape(length, HEADS, head_dim)
    key_heads = key.reshape(length, HEADS, head_dim)
    value_heads = value.reshape(length, HEADS, head_dim)
    raw = jnp.einsum('qhd,khd->hqk', query_heads, key_heads, precision=HIGH) * float(head_dim) ** (-0.5)
    raw = low_back(raw)
    blocks = jnp.arange(NSEG, dtype=jnp.int32)
    table = (blocks[:, None] == blocks[None, :]) | (blocks[:, None] > blocks[None, :]) & (link_row == 1)
    seen = table[block_row[:, None], block_row[None, :]]
    masked = jnp.where(seen[None], raw, NEG)
    highest = lax.optimization_barrier(jnp.max(masked, axis=-1, keepdims=True))
    exponent = jnp.exp(masked - highest)
    probs = exponent / lax.optimization_barrier(jnp.sum(exponent, axis=-1, keepdims=True))
    mixed = jnp.einsum('hqk,khd->qhd', low(probs), value_heads, precision=HIGH)
    return mixed.reshape(length, D)

def forward(inputs, params, block_rows, link_rows):
    w_query, b_query, w_key, w_value, b_value, w_out, b_out, gain_one, shift_one, w_up, b_up, w_down, b_down, gain_two, shift_two = params
    query = low(low_back(matmul(inputs, w_query)) + b_query)
    key = low(low_back(matmul(inputs, w_key)))
    value = low(low_back(matmul(inputs, w_value)) + b_value)
    seqs = block_rows.shape[0]
    kept = jax.checkpoint(attend)
    context = lax.map(lambda packed: kept(*packed), (query.reshape(seqs, SEQ_LEN, D), key.reshape(seqs, SEQ_LEN, D), value.reshape(seqs, SEQ_LEN, D), block_rows, link_rows))
    context = low(low_back(context.reshape(-1, D)))
    hidden_one = layer_norm(inputs + low_back(matmul(context, w_out)) + b_out, gain_one, shift_one)
    up = low_back(matmul(low(hidden_one), w_up)) + b_up
    active = low(jax.nn.gelu(up, approximate=False))
    return layer_norm(hidden_one + low_back(matmul(active, w_down)) + b_down, gain_two, shift_two)

def reference(layer_in, block_of, block_links, w_query, b_query, w_key, w_value, b_value, w_out, b_out, gain_one, shift_one, w_up, b_up, w_down, b_down, gain_two, shift_two, grad_out):
    params = tuple((weight.astype(jnp.float32) for weight in (w_query, b_query, w_key, w_value, b_value, w_out, b_out, gain_one, shift_one, w_up, b_up, w_down, b_down, gain_two, shift_two)))
    groups = SEQUENCES // SEQ_DEV
    inputs = layer_in.astype(jnp.float32).reshape(groups, SEQ_DEV * SEQ_LEN, D)
    cotangent = grad_out.astype(jnp.float32).reshape(groups, SEQ_DEV * SEQ_LEN, D)
    block_groups = block_of.reshape(groups, SEQ_DEV, SEQ_LEN)
    link_groups = block_links.reshape(groups, SEQ_DEV, NSEG, NSEG)

    def step(running, packed):
        group_in, group_blocks, group_links, group_grad = packed
        outputs, pull = jax.vjp(lambda first, second: forward(first, second, group_blocks, group_links), group_in, params)
        input_grad, param_grads = pull(group_grad)
        return (jax.tree.map(jnp.add, running, param_grads), (outputs, input_grad))
    zeros = jax.tree.map(jnp.zeros_like, params)
    totals, (outputs, input_grads) = lax.scan(step, zeros, (inputs, block_groups, link_groups, cotangent))
    layer_out = outputs.reshape(TOKENS, D).astype(jnp.bfloat16)
    grad_in = input_grads.reshape(TOKENS, D)
    return (layer_out, grad_in, totals[0], totals[1], totals[2], totals[3], totals[4], totals[5], totals[6], totals[7], totals[8], totals[9], totals[10], totals[11], totals[12], totals[13], totals[14])
```

```python
import jax
import jax.numpy as jnp
from jax import lax
from jax.sharding import PartitionSpec as P

D = 768
HEADS = 12
HEAD_DIM = D // HEADS

EPS = 1e-06
NEG = -1e30
ROOT_HALF = 0.7071067811865476
INV_ROOT_TWO_PI = 0.3989422804014327
BF16 = jnp.bfloat16
F32 = jnp.float32


def matmul(left, right):
    return jnp.dot(left, right, preferred_element_type=F32)


def matmul_tn(left, right):
    return lax.dot_general(left, right, (((0,), (0,)), ((), ())), preferred_element_type=F32)


def matmul_nt(left, right):
    return lax.dot_general(left, right, (((1,), (1,)), ((), ())), preferred_element_type=F32)


def normalize(values):
    centre = values - jnp.mean(values, axis=-1, keepdims=True)
    inverse = lax.rsqrt(jnp.mean(centre * centre, axis=-1, keepdims=True) + EPS)
    return (centre * inverse, inverse)


def norm_back(upstream, normed, inverse, gain):
    shaped = upstream * gain
    centred = jnp.mean(shaped, axis=-1, keepdims=True)
    aligned = jnp.mean(shaped * normed, axis=-1, keepdims=True)
    return inverse * (shaped - centred - normed * aligned)


def visible(blocks, link_table):
    count = link_table.shape[0]
    numbers = lax.iota(jnp.int32, count)
    same_block = numbers[:, None] == numbers[None, :]
    earlier = (numbers[:, None] > numbers[None, :]) & (link_table == 1)
    table = (same_block | earlier).astype(F32)
    onehot = (blocks[:, None] == numbers[None, :]).astype(F32)
    return matmul_nt(matmul(onehot, table), onehot) > 0.5


def split_heads(tensor):
    return tensor.reshape(tensor.shape[0], tensor.shape[1] // HEAD_DIM, HEAD_DIM)


def attend_forward(query, key, value, allowed, scale):
    query, key, value = (split_heads(tensor) for tensor in (query, key, value))
    raw = jnp.einsum("qhd,khd->hqk", query, key, preferred_element_type=F32) * scale
    scores = jnp.where(allowed[None], raw, NEG)
    highest = jnp.max(scores, axis=-1, keepdims=True)
    exponent = jnp.exp(scores - highest)
    summed = jnp.sum(exponent, axis=-1, keepdims=True)
    weights = (exponent / summed).astype(BF16)
    mixed = jnp.einsum("hqk,khd->qhd", weights, value, preferred_element_type=F32)
    return (
        mixed.reshape(query.shape[0], -1).astype(BF16),
        (highest + jnp.log(summed))[:, :, 0],
    )


def attend_backward(query, key, value, grad_context, log_totals, allowed, scale):
    query, key, value, grad = (split_heads(tensor) for tensor in (query, key, value, grad_context))
    length = query.shape[0]
    raw = jnp.einsum("qhd,khd->hqk", query, key, preferred_element_type=F32) * scale
    scores = jnp.where(allowed[None], raw, NEG)
    probs = jnp.exp(scores - log_totals[:, :, None])
    pulled = jnp.einsum("qhd,khd->hqk", grad, value, preferred_element_type=F32)
    centre = jnp.sum(pulled * probs, axis=-1, keepdims=True)
    score_grad = (probs * (pulled - centre)).astype(BF16)
    grad_query = (
        jnp.einsum("hqk,khd->qhd", score_grad, key, preferred_element_type=F32) * scale
    )
    grad_key = (
        jnp.einsum("hqk,qhd->khd", score_grad, query, preferred_element_type=F32) * scale
    )
    grad_value = jnp.einsum(
        "hqk,qhd->khd", probs.astype(BF16), grad, preferred_element_type=F32
    )
    return tuple(t.reshape(length, -1) for t in (grad_query, grad_key, grad_value))


def swap_tensor(array, mask):
    ways = lax.axis_size("tensor")
    return lax.ppermute(array, "tensor", [(i, i ^ mask) for i in range(ways)])


def swap_dp(array, mask):
    ways = lax.axis_size("dp")
    return lax.ppermute(array, "dp", [(i, i ^ mask) for i in range(ways)])


def across(array):
    return swap_tensor(array, 2)


def partner(array):
    return swap_tensor(array, 1)


def scatter_rows(grad):
    ways = lax.axis_size("dp")
    pieces = lax.all_to_all(
        grad.reshape(ways, grad.shape[0] // ways, grad.shape[1]), "dp", 0, 0
    )
    return jnp.sum(pieces.astype(F32), axis=0)


def on_device(
    layer_in,
    block_of,
    block_links,
    w_query,
    b_query,
    w_key,
    w_value,
    b_value,
    w_out,
    b_out,
    gain_one,
    shift_one,
    w_up,
    b_up,
    w_down,
    b_down,
    gain_two,
    shift_two,
    grad_out,
):
    length = block_of.shape[1]
    half = length // 2
    place = lax.axis_index("tensor")
    sequence = place // 2
    core = place % 2
    scale = float(HEAD_DIM) ** (-0.5)
    width = w_query.shape[1]
    hidden = w_up.shape[1]

    qkv_mine = jnp.concatenate([w_query, w_key, w_value], axis=1)
    small_mine = jnp.concatenate([b_query, b_value, b_up])
    qkv_other = across(qkv_mine)
    small_other = across(small_mine)
    out_other = across(w_out)
    up_other = across(w_up)
    down_other = across(w_down)

    tokens = lax.dynamic_slice_in_dim(layer_in, sequence * length, length, 0)
    tokens_mine = lax.dynamic_slice_in_dim(tokens, core * half, half, 0).astype(F32)
    blocks = lax.dynamic_index_in_dim(block_of, sequence, 0, keepdims=False)
    links = lax.dynamic_index_in_dim(block_links, sequence, 0, keepdims=False)
    allowed = visible(blocks, links)

    def project(weights, bias_query, bias_value):
        all_three = matmul(tokens, weights)
        query = (all_three[:, :width] + bias_query).astype(BF16)
        key = all_three[:, width : 2 * width].astype(BF16)
        value = (all_three[:, 2 * width :] + bias_value).astype(BF16)
        return query, key, value

    heads_mine = project(qkv_mine, b_query, b_value)
    context_mine, totals_mine = attend_forward(*heads_mine, allowed, scale)
    heads_other = project(qkv_other, small_other[:width], small_other[width : 2 * width])
    context_other, totals_other = attend_forward(*heads_other, allowed, scale)
    context = jnp.concatenate([context_mine, context_other], axis=1)
    out_both = jnp.concatenate([w_out, out_other], axis=0)

    far = lax.dynamic_slice_in_dim(context, (1 - core) * half, half, 0)
    near = lax.dynamic_slice_in_dim(context, core * half, half, 0)
    branch = matmul(near, out_both) + partner(matmul(far, out_both).astype(BF16)).astype(F32)
    normed_one, inverse_one = normalize(tokens_mine + branch + b_out)
    hidden_one = normed_one * gain_one + shift_one
    hidden_low_mine = hidden_one.astype(BF16)
    hidden_low = jnp.concatenate([hidden_low_mine, partner(hidden_low_mine)], axis=0)

    def rise(weights, bias):
        up = matmul(hidden_low, weights) + bias
        phi = 0.5 * (1.0 + lax.erf(up * ROOT_HALF))
        slope = phi + up * INV_ROOT_TWO_PI * jnp.exp(-0.5 * up * up)
        return (up * phi).astype(BF16), slope

    active_mine, slope_mine = rise(w_up, b_up)
    active_other, slope_other = rise(up_other, small_other[2 * width :])
    ffn_terms = matmul(active_mine, w_down) + matmul(active_other, down_other)
    ffn = ffn_terms[:half] + partner(ffn_terms[half:].astype(BF16)).astype(F32)
    normed_two, inverse_two = normalize(hidden_one + ffn + b_down)
    layer_out = (normed_two * gain_two + shift_two).astype(BF16)

    upstream = grad_out.astype(F32)
    grad_gain_two = jnp.sum(upstream * normed_two, axis=0)
    grad_shift_two = jnp.sum(upstream, axis=0)
    grad_two = norm_back(upstream, normed_two, inverse_two, gain_two)
    grad_b_down = jnp.sum(grad_two, axis=0)
    ffn_grad_mine = grad_two.astype(BF16)
    ffn_grad = jnp.concatenate([ffn_grad_mine, partner(ffn_grad_mine)], axis=0)

    grad_up_other = matmul_nt(ffn_grad, down_other) * slope_other
    grad_up_mine = matmul_nt(ffn_grad, w_down) * slope_mine
    up_low_other = grad_up_other.astype(BF16)
    up_low_mine = grad_up_mine.astype(BF16)
    hidden_terms = matmul_nt(up_low_mine, w_up) + matmul_nt(up_low_other, up_other)
    grad_hidden = grad_two + hidden_terms[:half] + partner(
        hidden_terms[half:].astype(BF16)
    ).astype(F32)

    down_sum = matmul_tn(ffn_grad, active_mine) + across(
        matmul_tn(ffn_grad, active_other).astype(BF16)
    ).astype(F32)
    up_sum = matmul_tn(hidden_low, up_low_mine) + across(
        matmul_tn(hidden_low, up_low_other).astype(BF16)
    ).astype(F32)
    grad_w_down = scatter_rows(down_sum.astype(BF16)).T
    grad_w_up = scatter_rows(up_sum.astype(BF16))

    grad_gain_one = jnp.sum(grad_hidden * normed_one, axis=0)
    grad_shift_one = jnp.sum(grad_hidden, axis=0)
    grad_one = norm_back(grad_hidden, normed_one, inverse_one, gain_one)
    grad_b_out = jnp.sum(grad_one, axis=0)
    one_low = grad_one.astype(BF16)
    one_partner = partner(one_low)
    pair = jnp.concatenate([one_low, one_partner, one_low], axis=0)
    branch_grad = lax.dynamic_slice_in_dim(pair, core * half, length, 0)
    grad_context = matmul_nt(branch_grad, out_both).astype(BF16)
    out_sum = matmul_tn(branch_grad, context_mine) + across(
        matmul_tn(branch_grad, context_other).astype(BF16)
    ).astype(F32)

    row_sums = jnp.stack(
        [grad_b_out, grad_gain_one, grad_shift_one, grad_b_down, grad_gain_two, grad_shift_two]
    )
    row_sums = row_sums + partner(row_sums)
    row_sums = row_sums + across(row_sums)
    hidden_sums = jnp.sum(grad_up_mine, axis=0) + across(jnp.sum(grad_up_other, axis=0))
    sums = jnp.concatenate([row_sums, hidden_sums.reshape(-1, D)], axis=0)
    mask = 1
    while mask < lax.axis_size("dp"):
        sums = sums + swap_dp(sums, mask)
        mask = mask * 2

    grads_other = attend_backward(
        *heads_other, grad_context[:, width:], totals_other, allowed, scale
    )
    grads_mine = attend_backward(
        *heads_mine, grad_context[:, :width], totals_mine, allowed, scale
    )
    low_other = jnp.concatenate(grads_other, axis=1).astype(BF16)
    low_mine = jnp.concatenate(grads_mine, axis=1).astype(BF16)
    bias_mine = jnp.concatenate([jnp.sum(grads_mine[0], axis=0), jnp.sum(grads_mine[2], axis=0)])
    bias_other = jnp.concatenate(
        [jnp.sum(grads_other[0], axis=0), jnp.sum(grads_other[2], axis=0)]
    )
    bias_sums = bias_mine + across(bias_other)
    qkv_sum = matmul_tn(tokens, low_mine) + across(
        matmul_tn(tokens, low_other).astype(BF16)
    ).astype(F32)

    in_terms = matmul_nt(low_mine, qkv_mine) + matmul_nt(low_other, qkv_other)
    in_far = lax.dynamic_slice_in_dim(in_terms, (1 - core) * half, half, 0)
    in_near = lax.dynamic_slice_in_dim(in_terms, core * half, half, 0)
    grad_in = grad_one + in_near + partner(in_far.astype(BF16)).astype(F32)

    mask = 1
    while mask < lax.axis_size("dp"):
        bias_sums = bias_sums + swap_dp(bias_sums, mask)
        mask = mask * 2
    attention = jnp.concatenate([qkv_sum, out_sum], axis=1).astype(BF16)
    attention = scatter_rows(attention)

    return (
        layer_out,
        grad_in,
        attention[:, :width],
        bias_sums[:width],
        attention[:, width : 2 * width],
        attention[:, 2 * width : 3 * width],
        bias_sums[width:],
        attention[:, 3 * width :].T,
        sums[0],
        sums[1],
        sums[2],
        grad_w_up,
        sums[6:].reshape(-1),
        grad_w_down,
        sums[3],
        sums[4],
        sums[5],
    )


def solution(mesh):
    in_specs = (
        P("dp", None),
        P("dp", None),
        P("dp", None, None),
        P(None, "tensor"),
        P("tensor"),
        P(None, "tensor"),
        P(None, "tensor"),
        P("tensor"),
        P("tensor", None),
        P(),
        P(),
        P(),
        P(None, "tensor"),
        P("tensor"),
        P("tensor", None),
        P(),
        P(),
        P(),
        P(("dp", "tensor"), None),
    )
    out_specs = (
        P(("dp", "tensor"), None),
        P(("dp", "tensor"), None),
        P("dp", "tensor"),
        P("tensor"),
        P("dp", "tensor"),
        P("dp", "tensor"),
        P("tensor"),
        P("tensor", "dp"),
        P(),
        P(),
        P(),
        P("dp", "tensor"),
        P("tensor"),
        P("tensor", "dp"),
        P(),
        P(),
        P(),
    )
    return jax.shard_map(
        on_device, mesh=mesh, in_specs=in_specs, out_specs=out_specs, check_vma=False
    )
```

```python
import functools

import jax
import jax.numpy as jnp
from jax import lax
from jax.experimental import pallas as pl
from jax.experimental.pallas import tpu as pltpu
from jax.sharding import PartitionSpec as P

D = 768
HEADS = 12
HEAD_DIM = D // HEADS

EPS = 1e-06
NEG = -1e30
ROOT_HALF = 0.7071067811865476
INV_ROOT_TWO_PI = 0.3989422804014327
BF16 = jnp.bfloat16
F32 = jnp.float32
BLOCK_MOST = 256
EXTRA = 8
QTILE = 256
KTILE = 256


def matmul(left, right):
    return jnp.dot(left, right, preferred_element_type=F32)


def matmul_tn(left, right):
    return lax.dot_general(left, right, (((0,), (0,)), ((), ())), preferred_element_type=F32)


def matmul_nt(left, right):
    return lax.dot_general(left, right, (((1,), (1,)), ((), ())), preferred_element_type=F32)


def normalize(values):
    centre = values - jnp.mean(values, axis=-1, keepdims=True)
    inverse = lax.rsqrt(jnp.mean(centre * centre, axis=-1, keepdims=True) + EPS)
    return (centre * inverse, inverse)


def norm_back(upstream, normed, inverse, gain):
    shaped = upstream * gain
    centred = jnp.mean(shaped, axis=-1, keepdims=True)
    aligned = jnp.mean(shaped * normed, axis=-1, keepdims=True)
    return inverse * (shaped - centred - normed * aligned)


def pieces_of(column):
    high = column.astype(BF16).astype(F32)
    middle = (column - high).astype(BF16).astype(F32)
    return high, middle, column - high - middle


def with_pieces(base, lane, first, column):
    high, middle, low = pieces_of(column)
    base = jnp.where(lane == first, -high, base)
    base = jnp.where(lane == first + 1, -middle, base)
    return jnp.where(lane == first + 2, -low, base)


def lanes_of(head, rows):
    odd = lax.rem(head, 2)
    lane = lax.broadcasted_iota(jnp.int32, (rows, 2 * HEAD_DIM), 1)
    own = (lane >= HEAD_DIM * odd) & (lane < HEAD_DIM * (odd + 1))
    return odd, lane, own, HEAD_DIM * (1 - odd) + EXTRA


def nt(left, right):
    return lax.dot_general(left, right, (((1,), (1,)), ((), ())), preferred_element_type=F32)


def forward_kernel(
    reach, place_ref, tokens_ref, weights_ref, table_ref, marks_ref,
    context_ref, query_ref, key_ref, value_ref, query_s, key_s, value_s, context_s
):
    length = tokens_ref.shape[0]
    width = weights_ref.shape[1] // 3
    tiles = pl.cdiv(width, 128)
    depth = tokens_ref.shape[1]
    tokens = tokens_ref[...]
    bias = jnp.sum(weights_ref[depth:].astype(F32), axis=0, keepdims=True)
    for kind, (store, factor) in enumerate(
        ((query_s, HEAD_DIM**-0.5), (key_s, 1.0), (value_s, 1.0))
    ):
        columns = slice(kind * width, (kind + 1) * width)
        made = (nn(tokens, weights_ref[:depth, columns]) + bias[:, columns]) * factor
        for tile in range(tiles):
            last = min(128, width - 128 * tile)
            store[tile, :, :last] = made[:, 128 * tile : 128 * tile + last]

    def one_head(head, carry):
        tile = head // 2
        odd, lane, own, first = lanes_of(head, length)
        marks = marks_ref[odd].astype(F32)
        key_ref[head] = jnp.where(own, key_s[tile], marks).astype(BF16)
        ones = jnp.where((lane >= first) & (lane < first + 3), 1.0, 0.0)
        value_ref[head] = jnp.where(own, value_s[tile], ones).astype(BF16)
        odd, lane, own, first = lanes_of(head, QTILE)
        for start in range(0, length, QTILE):
            rows = slice(start, start + QTILE)
            seen = min(length, start + QTILE + reach)
            query = jnp.where(own, query_s[tile, rows], table_ref[odd, rows].astype(F32))
            scores = nt(query.astype(BF16), key_ref[head, :seen])
            highest = jnp.max(scores, axis=-1, keepdims=True)
            weights = jnp.exp(scores - highest).astype(BF16)
            mixed = nn(weights, value_ref[head, :seen])
            total = jnp.sum(jnp.where(lane == first, mixed, 0.0), axis=-1, keepdims=True)
            context_s[tile, rows] = jnp.where(own, mixed * (1.0 / total), context_s[tile, rows])
            query_ref[head, rows] = with_pieces(
                query, lane, first, highest + jnp.log(total)
            ).astype(BF16)
        return carry

    lax.fori_loop(0, width // HEAD_DIM, one_head, 0)
    for tile in range(tiles):
        last = min(128, width - 128 * tile)
        context_ref[:, 128 * tile : 128 * tile + last] = context_s[tile, :, :last].astype(BF16)


def nn(left, right):
    return jnp.dot(left, right, preferred_element_type=F32)


def tn(left, right):
    return lax.dot_general(left, right, (((0,), (0,)), ((), ())), preferred_element_type=F32)


def attend_forward(place, layer_in, weights, table, marks, length):
    width = weights.shape[1] // 3
    heads = width // HEAD_DIM
    tiles = pl.cdiv(width, 128)
    whole = pl.BlockSpec(memory_space=pltpu.VMEM)
    big = jax.ShapeDtypeStruct((heads, length, 128), BF16)
    return pl.pallas_call(
        functools.partial(forward_kernel, BLOCK_MOST),
        out_shape=(jax.ShapeDtypeStruct((length, width), BF16), big, big, big),
        grid_spec=pltpu.PrefetchScalarGridSpec(
            num_scalar_prefetch=1,
            grid=(1,),
            in_specs=[
                pl.BlockSpec((length, layer_in.shape[1]), lambda i, at: (at[0], 0)),
                whole,
                whole,
                whole,
            ],
            out_specs=(whole,) * 4,
            scratch_shapes=[pltpu.VMEM((tiles, length, 128), F32)] * 4,
        ),
        cost_estimate=pl.CostEstimate(
            flops=2 * length * D * 3 * width + 4 * length * length * 128 * heads,
            bytes_accessed=2 * (length * D + D * 3 * width + 4 * length * width),
            transcendentals=length * length * heads,
        ),
        name="attend_forward",
    )(place, layer_in, weights, table, marks)


def backward_kernel(
    reach, upstream_ref, out_ref, context_ref, query_ref, key_ref, value_ref,
    grads_ref, sums_ref, grad_s, context_s, query_s, query_t, key_s, value_s, extended_s
):
    length, width = context_ref.shape
    tiles = pl.cdiv(width, 128)
    made = nt(upstream_ref[...], out_ref[:width]).astype(BF16).astype(F32)
    context = context_ref[...].astype(F32)
    for tile in range(tiles):
        last = min(128, width - 128 * tile)
        grad_s[tile, :, :last] = made[:, 128 * tile : 128 * tile + last]
        context_s[tile, :, :last] = (made * context)[:, 128 * tile : 128 * tile + last]

    def one_head(head, carry):
        tile = head // 2
        odd, lane, own, first = lanes_of(head, length)
        centre = jnp.sum(jnp.where(own, context_s[tile], 0.0), axis=-1, keepdims=True)
        grad = jnp.where(own, grad_s[tile], 0.0)
        extended_s[...] = with_pieces(grad, lane, first, centre).astype(BF16)
        odd, lane, own, first = lanes_of(head, KTILE)
        query_s[...] = jnp.zeros_like(query_s)
        for start in range(0, length, KTILE):
            rows = slice(start, start + KTILE)
            seen = max(0, start - reach)
            scores = nt(key_ref[head, rows], query_ref[head, seen:])
            probs = jnp.exp(scores)
            pulled = nt(value_ref[head, rows], extended_s[seen:])
            changed = (probs * pulled).astype(BF16)
            grad_value = nn(probs.astype(BF16), extended_s[seen:])
            grad_key = nn(changed, query_ref[head, seen:])
            value_s[tile, rows] = jnp.where(own, grad_value, value_s[tile, rows])
            key_s[tile, rows] = jnp.where(own, grad_key, key_s[tile, rows])
            query_s[seen:] += tn(changed, key_ref[head, rows])
        odd, lane, own, first = lanes_of(head, length)
        query_t[tile] = jnp.where(own, query_s[...] * HEAD_DIM**-0.5, query_t[tile])
        return carry

    lax.fori_loop(0, width // HEAD_DIM, one_head, 0)
    for kind, store in enumerate((query_t, key_s, value_s)):
        for tile in range(tiles):
            last = min(128, width - 128 * tile)
            made = store[tile, :, :last]
            begin = kind * width + 128 * tile
            grads_ref[:, begin : begin + last] = made.astype(BF16)
            if kind != 1:
                sums_ref[kind : kind + 1, 128 * tile : 128 * tile + last] = jnp.sum(
                    made, axis=0, keepdims=True
                )


def attend_backward(upstream, out, saved):
    context, query, key, value = saved
    length, width = context.shape
    heads = width // HEAD_DIM
    tiles = pl.cdiv(width, 128)
    whole = pl.BlockSpec(memory_space=pltpu.VMEM)
    tall = pltpu.VMEM((tiles, length, 128), F32)
    return pl.pallas_call(
        functools.partial(backward_kernel, BLOCK_MOST),
        out_shape=(
            jax.ShapeDtypeStruct((length, 3 * width), BF16),
            jax.ShapeDtypeStruct((3, width), F32),
        ),
        in_specs=[whole] * 6,
        out_specs=(whole, whole),
        scratch_shapes=[
            tall, tall, pltpu.VMEM((length, 128), F32), tall, tall, tall,
            pltpu.VMEM((length, 128), BF16),
        ],
        cost_estimate=pl.CostEstimate(
            flops=2 * length * D * width + 10 * length * length * 128 * heads,
            bytes_accessed=2 * (length * D + 10 * length * width),
            transcendentals=length * length * heads,
        ),
        name="attend_backward",
    )(upstream, out, context, query, key, value)


def mask_terms(blocks, links):
    count = links.shape[0]
    numbers = lax.iota(jnp.int32, count)
    same_block = numbers[:, None] == numbers[None, :]
    earlier = (numbers[:, None] > numbers[None, :]) & (links == 1)
    table = jnp.where(same_block | earlier, 0.0, NEG).astype(BF16)
    onehot = (blocks[:, None] == numbers[None, :]).astype(BF16)
    seen = matmul(onehot, table).astype(BF16)
    ones = jnp.ones((blocks.shape[0], 3), BF16)
    marks = jnp.concatenate([onehot, ones], axis=1)

    def both(terms):
        after = ((0, 0), (HEAD_DIM, HEAD_DIM - terms.shape[1]))
        before = ((0, 0), (0, 2 * HEAD_DIM - terms.shape[1]))
        return jnp.stack([jnp.pad(terms, after), jnp.pad(terms, before)])

    return both(seen), both(marks)


def swap_tensor(array, mask):
    ways = lax.axis_size("tensor")
    return lax.ppermute(array, "tensor", [(i, i ^ mask) for i in range(ways)])


def swap_dp(array, mask):
    ways = lax.axis_size("dp")
    return lax.ppermute(array, "dp", [(i, i ^ mask) for i in range(ways)])


def across(array):
    return swap_tensor(array, 2)


def partner(array):
    return swap_tensor(array, 1)


def after(array, *earlier):
    return lax.optimization_barrier((array,) + earlier)[0]


def three_terms(row):
    high = lax.reduce_precision(row, 8, 7)
    middle = lax.reduce_precision(row - high, 8, 7)
    terms = jnp.stack([high, middle, row - high - middle]).astype(BF16)
    return jnp.pad(terms, ((0, 5), (0, 0)))


def scatter_pieces(pieces):
    return jnp.sum(lax.all_to_all(pieces, "dp", 0, 0).astype(F32), axis=0)


def by_rows(grad):
    ways = lax.axis_size("dp")
    return grad.reshape(ways, grad.shape[0] // ways, grad.shape[1])


def from_halves(first, second, swapped):
    return jnp.where(
        swapped,
        jnp.concatenate([second, first], axis=0),
        jnp.concatenate([first, second], axis=0),
    )


def on_device(
    layer_in,
    block_of,
    block_links,
    w_query,
    b_query,
    w_key,
    w_value,
    b_value,
    w_out,
    b_out,
    gain_one,
    shift_one,
    w_up,
    b_up,
    w_down,
    b_down,
    gain_two,
    shift_two,
    grad_out,
):
    length = block_of.shape[1]
    half = length // 2
    place = lax.axis_index("tensor")
    sequence = place // 2
    core = place % 2
    width = w_query.shape[1]
    rise_half = w_up.shape[0] // 2
    fall_half = w_down.shape[0] // 2

    bias_row = jnp.concatenate([b_query, jnp.zeros_like(b_query), b_value])
    qkv_mine = jnp.concatenate(
        [jnp.concatenate([w_query, w_key, w_value], axis=1), three_terms(bias_row)], axis=0
    )
    out_mine = jnp.concatenate([w_out, three_terms(b_up)], axis=0)
    odd = lax.axis_index("dp") % 2
    qkv_other = across(qkv_mine)
    up_first = across(lax.dynamic_slice_in_dim(w_up, odd * rise_half, rise_half, 0))
    out_other = across(out_mine)
    down_first = across(lax.dynamic_slice_in_dim(w_down, odd * fall_half, fall_half, 0))

    tokens = lax.dynamic_slice_in_dim(layer_in, sequence * length, length, 0)
    tokens_mine = lax.dynamic_slice_in_dim(tokens, core * half, half, 0).astype(F32)
    blocks = lax.dynamic_index_in_dim(block_of, sequence, 0, keepdims=False)
    links = lax.dynamic_index_in_dim(block_links, sequence, 0, keepdims=False)
    table, marks = mask_terms(blocks, links)
    chosen = jnp.full((1,), sequence, jnp.int32)

    saved_mine = attend_forward(chosen, layer_in, qkv_mine, table, marks, length)
    saved_other = attend_forward(chosen, layer_in, qkv_other, table, marks, length)
    context_mine = saved_mine[0]
    context_other = after(saved_other[0], up_first)
    up_second = swap_dp(up_first, 1)
    context = jnp.concatenate([context_mine, context_other], axis=1)
    out_both = jnp.concatenate([w_out, out_other[:width]], axis=0)
    b_up_other = jnp.sum(out_other[width:].astype(F32), axis=0)

    far = lax.dynamic_slice_in_dim(context, (1 - core) * half, half, 0)
    near = lax.dynamic_slice_in_dim(context, core * half, half, 0)
    branch = matmul(near, out_both) + partner(matmul(far, out_both).astype(BF16)).astype(F32)
    normed_one, inverse_one = normalize(tokens_mine + branch + b_out)
    hidden_one = normed_one * gain_one + shift_one
    hidden_low_mine = after(hidden_one.astype(BF16), down_first)
    down_second = swap_dp(down_first, 1)
    hidden_low = jnp.concatenate([hidden_low_mine, partner(hidden_low_mine)], axis=0)

    def rise(weights, bias):
        up = matmul(hidden_low, weights) + bias
        phi = 0.5 * (1.0 + lax.erf(up * ROOT_HALF))
        slope = phi + up * INV_ROOT_TWO_PI * jnp.exp(-0.5 * up * up)
        return (up * phi).astype(BF16), slope

    active_mine, slope_mine = rise(w_up, b_up)
    up_other = from_halves(up_first, up_second, odd == 1)
    active_other, slope_other = rise(up_other, b_up_other)
    down_other = from_halves(down_first, down_second, odd == 1)
    ffn_terms = matmul(active_mine, w_down) + matmul(active_other, down_other)
    ffn = ffn_terms[:half] + partner(ffn_terms[half:].astype(BF16)).astype(F32)
    normed_two, inverse_two = normalize(hidden_one + ffn + b_down)
    layer_out = (normed_two * gain_two + shift_two).astype(BF16)

    upstream = grad_out.astype(F32)
    grad_gain_two = jnp.sum(upstream * normed_two, axis=0)
    grad_shift_two = jnp.sum(upstream, axis=0)
    grad_two = norm_back(upstream, normed_two, inverse_two, gain_two)
    grad_b_down = jnp.sum(grad_two, axis=0)
    ffn_grad_mine = grad_two.astype(BF16)
    ffn_grad = jnp.concatenate([ffn_grad_mine, partner(ffn_grad_mine)], axis=0)

    down_received = across(matmul_tn(ffn_grad, active_other).astype(BF16))
    grad_up_other = matmul_nt(ffn_grad, down_other) * slope_other
    up_low_other = grad_up_other.astype(BF16)
    up_received = across(matmul_tn(hidden_low, up_low_other).astype(BF16))
    grad_up_mine = matmul_nt(ffn_grad, w_down) * slope_mine
    up_low_mine = grad_up_mine.astype(BF16)
    hidden_terms = matmul_nt(up_low_mine, w_up) + matmul_nt(up_low_other, up_other)
    grad_hidden = grad_two + hidden_terms[:half] + partner(
        hidden_terms[half:].astype(BF16)
    ).astype(F32)
    down_mine = matmul_tn(ffn_grad, active_mine)
    up_mine = matmul_tn(hidden_low, up_low_mine)

    grad_gain_one = jnp.sum(grad_hidden * normed_one, axis=0)
    grad_shift_one = jnp.sum(grad_hidden, axis=0)
    grad_one = norm_back(grad_hidden, normed_one, inverse_one, gain_one)
    grad_b_out = jnp.sum(grad_one, axis=0)
    one_low = grad_one.astype(BF16)
    one_partner = partner(one_low)
    pair = jnp.concatenate([one_low, one_partner, one_low], axis=0)
    branch_grad = lax.dynamic_slice_in_dim(pair, core * half, length, 0)

    out_received = across(matmul_tn(branch_grad, context_other).astype(BF16))

    row_sums = jnp.stack(
        [grad_b_out, grad_gain_one, grad_shift_one, grad_b_down, grad_gain_two, grad_shift_two]
    )
    row_sums = row_sums + partner(row_sums)
    hidden_mine = jnp.sum(grad_up_mine, axis=0).reshape(-1, D)
    hidden_other = jnp.sum(grad_up_other, axis=0).reshape(-1, D)
    sums = jnp.concatenate([row_sums, hidden_mine], axis=0) + across(
        jnp.concatenate([row_sums, hidden_other], axis=0)
    )
    sum_high = lax.reduce_precision(sums, 8, 7)
    sum_terms = jnp.concatenate([sum_high, sums - sum_high], axis=0).astype(BF16)

    low_other, columns_other = attend_backward(branch_grad, out_other, saved_other)
    low_mine, columns_mine = attend_backward(
        after(branch_grad, low_other, sums), out_mine, saved_mine
    )

    down_received = after(down_received, low_other)
    down_pieces = by_rows((down_mine + down_received.astype(F32)).astype(BF16))
    ways, share = down_pieces.shape[:2]
    count = sum_terms.shape[0]
    sum_pieces = jnp.broadcast_to(
        jnp.pad(sum_terms, ((0, -count % 8), (0, 0)))[None], (ways, count + -count % 8, D)
    )
    down_sums = scatter_pieces(jnp.concatenate([down_pieces, sum_pieces], axis=1))
    grad_w_down = down_sums[:share].T
    sums = jnp.sum(down_sums[share : share + count].reshape(2, count // 2, D), axis=0)

    def with_bias(columns):
        row = jnp.concatenate([columns[0], jnp.zeros_like(columns[0]), columns[2]])
        return row, three_terms(row)

    other_row, other_terms = with_bias(columns_other)
    qkv_received = across(
        jnp.concatenate([matmul_tn(tokens, low_other).astype(BF16), other_terms], axis=0)
    )

    up_received, out_received = (
        lax.optimization_barrier((up_received, out_received, low_mine))[:2]
    )
    up_sum = (up_mine + up_received.astype(F32)).astype(BF16)
    out_sum = matmul_tn(branch_grad, context_mine) + out_received.astype(F32)
    up_pieces = jnp.concatenate([by_rows(up_sum), by_rows(out_sum.astype(BF16))], axis=2)
    up_out = scatter_pieces(up_pieces)
    grad_w_up, grad_w_out = up_out[:, : w_up.shape[1]], up_out[:, w_up.shape[1] :].T

    mine_row, _ = with_bias(columns_mine)
    qkv_received = qkv_received.astype(F32)
    qkv_sum = matmul_tn(tokens, low_mine) + qkv_received[:D]
    bias_terms = three_terms(mine_row + jnp.sum(qkv_received[D:], axis=0))
    qkv_pieces = by_rows(qkv_sum.astype(BF16))
    bias_pieces = jnp.broadcast_to(bias_terms[None], (ways,) + bias_terms.shape)
    qkv = scatter_pieces(jnp.concatenate([qkv_pieces, bias_pieces], axis=1))
    bias_sums = jnp.sum(qkv[share:], axis=0)
    qkv = qkv[:share]

    in_terms = matmul_nt(low_mine, qkv_mine[:D]) + matmul_nt(low_other, qkv_other[:D])
    in_far = lax.dynamic_slice_in_dim(in_terms, (1 - core) * half, half, 0)
    in_near = lax.dynamic_slice_in_dim(in_terms, core * half, half, 0)
    grad_in = grad_one + in_near + partner(in_far.astype(BF16)).astype(F32)

    return (
        layer_out,
        grad_in,
        qkv[:, :width],
        bias_sums[:width],
        qkv[:, width : 2 * width],
        qkv[:, 2 * width :],
        bias_sums[2 * width :],
        grad_w_out,
        sums[0],
        sums[1],
        sums[2],
        grad_w_up,
        sums[6:].reshape(-1),
        grad_w_down,
        sums[3],
        sums[4],
        sums[5],
    )


def solution(mesh):
    in_specs = (
        P("dp", None),
        P("dp", None),
        P("dp", None, None),
        P(None, "tensor"),
        P("tensor"),
        P(None, "tensor"),
        P(None, "tensor"),
        P("tensor"),
        P("tensor", None),
        P(),
        P(),
        P(),
        P(None, "tensor"),
        P("tensor"),
        P("tensor", None),
        P(),
        P(),
        P(),
        P(("dp", "tensor"), None),
    )
    out_specs = (
        P(("dp", "tensor"), None),
        P(("dp", "tensor"), None),
        P("dp", "tensor"),
        P("tensor"),
        P("dp", "tensor"),
        P("dp", "tensor"),
        P("tensor"),
        P("tensor", "dp"),
        P(),
        P(),
        P(),
        P("dp", "tensor"),
        P("tensor"),
        P("tensor", "dp"),
        P(),
        P(),
        P(),
    )
    return jax.shard_map(
        on_device, mesh=mesh, in_specs=in_specs, out_specs=out_specs, check_vma=False
    )
```

```python
import functools

import jax
import jax.numpy as jnp
from jax import lax
from jax.experimental import pallas as pl
from jax.experimental.pallas import tpu as pltpu
from jax.sharding import PartitionSpec as P

D = 768
HEADS = 12
HEAD_DIM = D // HEADS

EPS = 1e-06
NEG = -1e30
ROOT_HALF = 0.7071067811865476
INV_ROOT_TWO_PI = 0.3989422804014327
BF16 = jnp.bfloat16
F32 = jnp.float32
BLOCK_MOST = 256
EXTRA = 8
NOMINAL = pl.CostEstimate(flops=1000, bytes_accessed=1000, transcendentals=0)
QTILE = 256
KTILE = 256


def matmul(left, right):
    return jnp.dot(left, right, preferred_element_type=F32)


def matmul_tn(left, right):
    return lax.dot_general(left, right, (((0,), (0,)), ((), ())), preferred_element_type=F32)


def matmul_nt(left, right):
    return lax.dot_general(left, right, (((1,), (1,)), ((), ())), preferred_element_type=F32)


def normalize(values):
    centre = values - jnp.mean(values, axis=-1, keepdims=True)
    inverse = lax.rsqrt(jnp.mean(centre * centre, axis=-1, keepdims=True) + EPS)
    return (centre * inverse, inverse)


def norm_back(upstream, normed, inverse, gain):
    shaped = upstream * gain
    centred = jnp.mean(shaped, axis=-1, keepdims=True)
    aligned = jnp.mean(shaped * normed, axis=-1, keepdims=True)
    return inverse * (shaped - centred - normed * aligned)


def pieces_of(column):
    high = column.astype(BF16).astype(F32)
    middle = (column - high).astype(BF16).astype(F32)
    return high, middle, column - high - middle


def with_pieces(base, lane, first, column):
    high, middle, low = pieces_of(column)
    base = jnp.where(lane == first, -high, base)
    base = jnp.where(lane == first + 1, -middle, base)
    return jnp.where(lane == first + 2, -low, base)


def lanes_of(head, rows):
    odd = lax.rem(head, 2)
    lane = lax.broadcasted_iota(jnp.int32, (rows, 2 * HEAD_DIM), 1)
    own = (lane >= HEAD_DIM * odd) & (lane < HEAD_DIM * (odd + 1))
    return odd, lane, own, HEAD_DIM * (1 - odd) + EXTRA


def nt(left, right):
    return lax.dot_general(left, right, (((1,), (1,)), ((), ())), preferred_element_type=F32)


def forward_kernel(
    reach, place_ref, tokens_ref, w_query_ref, w_key_ref, w_value_ref, b_query_ref, b_value_ref,
    table_ref, marks_ref, context_ref, query_ref, key_ref, value_ref, query_s, key_s, value_s, context_s
):
    length = tokens_ref.shape[0]
    width = w_query_ref.shape[1]
    tiles = pl.cdiv(width, 128)
    tokens = tokens_ref[...]
    for store, made in (
        (query_s, (nn(tokens, w_query_ref[...]) + b_query_ref[...]) * HEAD_DIM**-0.5),
        (key_s, nn(tokens, w_key_ref[...])),
        (value_s, nn(tokens, w_value_ref[...]) + b_value_ref[...]),
    ):
        for tile in range(tiles):
            last = min(128, width - 128 * tile)
            store[tile, :, :last] = made[:, 128 * tile : 128 * tile + last]

    def one_head(head, carry):
        tile = head // 2
        odd, lane, own, first = lanes_of(head, length)
        marks = marks_ref[0, odd].astype(F32)
        key_ref[head] = jnp.where(own, key_s[tile], marks).astype(BF16)
        ones = jnp.where((lane >= first) & (lane < first + 3), 1.0, 0.0)
        value_ref[head] = jnp.where(own, value_s[tile], ones).astype(BF16)
        odd, lane, own, first = lanes_of(head, QTILE)
        for start in range(0, length, QTILE):
            rows = slice(start, start + QTILE)
            seen = min(length, start + QTILE + reach)
            query = jnp.where(own, query_s[tile, rows], table_ref[0, odd, rows].astype(F32))
            scores = nt(query.astype(BF16), key_ref[head, :seen])
            highest = jnp.max(scores, axis=-1, keepdims=True)
            weights = jnp.exp(scores - highest).astype(BF16)
            mixed = nn(weights, value_ref[head, :seen])
            total = jnp.sum(jnp.where(lane == first, mixed, 0.0), axis=-1, keepdims=True)
            context_s[tile, rows] = jnp.where(own, mixed * (1.0 / total), context_s[tile, rows])
            query_ref[head, rows] = with_pieces(
                query, lane, first, highest + jnp.log(total)
            ).astype(BF16)
        return carry

    lax.fori_loop(0, width // HEAD_DIM, one_head, 0)
    for tile in range(tiles):
        last = min(128, width - 128 * tile)
        context_ref[:, 128 * tile : 128 * tile + last] = context_s[tile, :, :last].astype(BF16)


def nn(left, right):
    return jnp.dot(left, right, preferred_element_type=F32)


def tn(left, right):
    return lax.dot_general(left, right, (((0,), (0,)), ((), ())), preferred_element_type=F32)


def attend_forward(place, layer_in, weights, table, marks):
    length = table.shape[2]
    depth, width = weights[0].shape
    heads = width // HEAD_DIM
    tiles = pl.cdiv(width, 128)
    whole = pl.BlockSpec(memory_space=pltpu.VMEM)
    terms = pl.BlockSpec((1, 2, length, 128), lambda i, at: (at[0], 0, 0, 0))
    big = jax.ShapeDtypeStruct((heads, length, 128), BF16)
    return pl.pallas_call(
        functools.partial(forward_kernel, BLOCK_MOST),
        out_shape=(jax.ShapeDtypeStruct((length, width), BF16), big, big, big),
        grid_spec=pltpu.PrefetchScalarGridSpec(
            num_scalar_prefetch=1,
            grid=(1,),
            in_specs=[pl.BlockSpec((length, depth), lambda i, at: (at[0], 0))]
            + [whole] * 5
            + [terms] * 2,
            out_specs=(whole,) * 4,
            scratch_shapes=[pltpu.VMEM((tiles, length, 128), F32)] * 4,
        ),
        cost_estimate=NOMINAL,
        name="attend_forward",
    )(place, layer_in, *weights, table, marks)


def backward_kernel(
    reach, core_ref, first_ref, second_ref, out_ref, w_query_ref, w_key_ref, w_value_ref,
    context_ref, query_ref, key_ref, value_ref, grads_ref, sums_ref, in_ref, w_out_ref,
    grad_s, context_s, query_s, query_t, key_s, value_s, extended_s
):
    length, width = context_ref.shape
    half = length // 2
    tiles = pl.cdiv(width, 128)
    outward = jnp.zeros((width, out_ref.shape[1]), F32)
    for part, upstream_ref in enumerate((first_ref, second_ref)):
        begin = pl.multiple_of(lax.rem(core_ref[0] + part, 2) * half, half)
        rows = pl.ds(begin, half)
        made = nt(upstream_ref[...], out_ref[...]).astype(BF16).astype(F32)
        context = context_ref[rows]
        outward += tn(context, upstream_ref[...])
        aligned = made * context.astype(F32)
        for tile in range(tiles):
            last = min(128, width - 128 * tile)
            grad_s[tile, rows, :last] = made[:, 128 * tile : 128 * tile + last]
            context_s[tile, rows, :last] = aligned[:, 128 * tile : 128 * tile + last]
    w_out_ref[...] = outward

    def one_head(head, carry):
        tile = head // 2
        odd, lane, own, first = lanes_of(head, length)
        centre = jnp.sum(jnp.where(own, context_s[tile], 0.0), axis=-1, keepdims=True)
        grad = jnp.where(own, grad_s[tile], 0.0)
        extended_s[...] = with_pieces(grad, lane, first, centre).astype(BF16)
        odd, lane, own, first = lanes_of(head, KTILE)
        query_s[...] = jnp.zeros_like(query_s)
        for start in range(0, length, KTILE):
            rows = slice(start, start + KTILE)
            seen = max(0, start - reach)
            scores = nt(key_ref[head, rows], query_ref[head, seen:])
            probs = jnp.exp(scores)
            pulled = nt(value_ref[head, rows], extended_s[seen:])
            changed = (probs * pulled).astype(BF16)
            grad_value = nn(probs.astype(BF16), extended_s[seen:])
            grad_key = nn(changed, query_ref[head, seen:])
            value_s[tile, rows] = jnp.where(own, grad_value, value_s[tile, rows])
            key_s[tile, rows] = jnp.where(own, grad_key, key_s[tile, rows])
            query_s[seen:] += tn(changed, key_ref[head, rows])
        odd, lane, own, first = lanes_of(head, length)
        query_t[tile] = jnp.where(own, query_s[...] * HEAD_DIM**-0.5, query_t[tile])
        return carry

    lax.fori_loop(0, width // HEAD_DIM, one_head, 0)
    inward = jnp.zeros((length, in_ref.shape[1]), F32)
    for kind, (store, weight_ref) in enumerate(
        ((query_t, w_query_ref), (key_s, w_key_ref), (value_s, w_value_ref))
    ):
        for tile in range(tiles):
            last = min(128, width - 128 * tile)
            made = store[tile, :, :last]
            low = made.astype(BF16)
            begin = kind * width + 128 * tile
            grads_ref[:, begin : begin + last] = low
            inward += nt(low, weight_ref[:, 128 * tile : 128 * tile + last])
            if kind != 1:
                sums_ref[kind : kind + 1, 128 * tile : 128 * tile + last] = jnp.sum(
                    made, axis=0, keepdims=True
                )
    in_ref[...] = inward.astype(BF16)


def attend_backward(core, upstream, out, weights, saved):
    context, query, key, value = saved
    length, width = context.shape
    heads = width // HEAD_DIM
    depth = out.shape[1]
    tiles = pl.cdiv(width, 128)
    whole = pl.BlockSpec(memory_space=pltpu.VMEM)
    tall = pltpu.VMEM((tiles, length, 128), F32)
    return pl.pallas_call(
        functools.partial(backward_kernel, BLOCK_MOST),
        out_shape=(
            jax.ShapeDtypeStruct((length, 3 * width), BF16),
            jax.ShapeDtypeStruct((3, width), F32),
            jax.ShapeDtypeStruct((length, depth), BF16),
            jax.ShapeDtypeStruct((width, depth), F32),
        ),
        in_specs=[pl.BlockSpec(memory_space=pltpu.SMEM)] + [whole] * 10,
        out_specs=(whole,) * 4,
        scratch_shapes=[
            tall, tall, pltpu.VMEM((length, 128), F32), tall, tall, tall,
            pltpu.VMEM((length, 128), BF16),
        ],
        cost_estimate=NOMINAL,
        name="attend_backward",
    )(core, *upstream, out, *weights, context, query, key, value)


def flip_kernel(array_ref, flipped_ref):
    flipped_ref[...] = array_ref[...].T


def flip_pair_kernel(first_ref, second_ref, flipped_ref):
    rows = first_ref.shape[0]
    flipped_ref[:, :rows] = first_ref[...].T
    flipped_ref[:, rows:] = second_ref[...].T


def flipped_pair(first, second):
    rows, columns = first.shape
    return pl.pallas_call(
        flip_pair_kernel,
        out_shape=jax.ShapeDtypeStruct((columns, 2 * rows), first.dtype),
        in_specs=[pl.BlockSpec(memory_space=pltpu.VMEM)] * 2,
        out_specs=pl.BlockSpec(memory_space=pltpu.VMEM),
        cost_estimate=pl.CostEstimate(
            flops=0, bytes_accessed=8 * first.size, transcendentals=0
        ),
        name="flip_pair",
    )(first, second)


def flipped(array, rows):
    columns = array.shape[1]
    count = array.shape[0] // rows
    return pl.pallas_call(
        flip_kernel,
        out_shape=jax.ShapeDtypeStruct((count, columns, rows), array.dtype),
        grid=(count,),
        in_specs=[pl.BlockSpec((rows, columns), lambda i: (i, 0))],
        out_specs=pl.BlockSpec((None, columns, rows), lambda i: (i, 0, 0)),
        cost_estimate=pl.CostEstimate(
            flops=0, bytes_accessed=4 * array.size, transcendentals=0
        ),
        name="flip",
    )(array)


def mask_terms(blocks, links):
    count = links.shape[0]
    numbers = lax.iota(jnp.int32, count)
    same_block = numbers[:, None] == numbers[None, :]
    earlier = (numbers[:, None] > numbers[None, :]) & (links == 1)
    table = jnp.where(same_block | earlier, 0.0, NEG).astype(BF16)
    onehot = (blocks[:, None] == numbers[None, :]).astype(BF16)
    seen = matmul(onehot, table).astype(BF16)
    ones = jnp.ones((blocks.shape[0], 3), BF16)
    marks = jnp.concatenate([onehot, ones], axis=1)

    def both(terms):
        after = ((0, 0), (HEAD_DIM, HEAD_DIM - terms.shape[1]))
        before = ((0, 0), (0, 2 * HEAD_DIM - terms.shape[1]))
        return jnp.stack([jnp.pad(terms, after), jnp.pad(terms, before)])

    return both(seen), both(marks)


def swap_tensor(array, mask):
    ways = lax.axis_size("tensor")
    return lax.ppermute(array, "tensor", [(i, i ^ mask) for i in range(ways)])


def swap_dp(array, mask):
    ways = lax.axis_size("dp")
    return lax.ppermute(array, "dp", [(i, i ^ mask) for i in range(ways)])


def across(array):
    return swap_tensor(array, 2)


def partner(array):
    return swap_tensor(array, 1)


def after(array, *earlier):
    return lax.optimization_barrier((array,) + earlier)[0]


def three_terms(row):
    high = lax.reduce_precision(row, 8, 7)
    middle = lax.reduce_precision(row - high, 8, 7)
    terms = jnp.stack([high, middle, row - high - middle]).astype(BF16)
    return jnp.pad(terms, ((0, 5), (0, 0)))


def scatter_pieces(pieces):
    return jnp.sum(lax.all_to_all(pieces, "dp", 0, 0).astype(F32), axis=0)


def by_rows(grad):
    ways = lax.axis_size("dp")
    return grad.reshape(ways, grad.shape[0] // ways, grad.shape[1])


def from_halves(first, second, swapped):
    return jnp.where(
        swapped,
        jnp.concatenate([second, first], axis=0),
        jnp.concatenate([first, second], axis=0),
    )


def on_device(
    layer_in,
    block_of,
    block_links,
    w_query,
    b_query,
    w_key,
    w_value,
    b_value,
    w_out,
    b_out,
    gain_one,
    shift_one,
    w_up,
    b_up,
    w_down,
    b_down,
    gain_two,
    shift_two,
    grad_out,
):
    length = block_of.shape[1]
    half = length // 2
    place = lax.axis_index("tensor")
    sequence = place // 2
    core = place % 2
    width = w_query.shape[1]
    rise_half = w_up.shape[0] // 2
    fall_half = w_down.shape[0] // 2
    ways = lax.axis_size("dp")
    odd = lax.axis_index("dp") % 2

    out_mine = jnp.concatenate([w_out, three_terms(b_up)], axis=0)
    up_first = across(lax.dynamic_slice_in_dim(w_up, odd * rise_half, rise_half, 0))

    table, marks = jax.vmap(mask_terms)(block_of, block_links)
    weights = (w_query, w_key, w_value)
    inputs = weights + (b_query.reshape(1, -1), b_value.reshape(1, -1))
    near_place = jnp.full((1,), sequence, jnp.int32)
    saved_far = attend_forward(1 - near_place, layer_in, inputs, table, marks)
    context_other = across(saved_far[0])
    saved_near = attend_forward(
        after(near_place, saved_far[0]), layer_in, inputs, table, marks
    )
    context_mine = after(saved_near[0], up_first)
    up_second = swap_dp(up_first, 1)
    out_received = across(after(out_mine, saved_far[0]))
    down_first = across(
        after(lax.dynamic_slice_in_dim(w_down, odd * fall_half, fall_half, 0), saved_far[0])
    )
    tokens_t = flipped(after(layer_in, saved_near[0]), length)
    out_other = after(out_received, tokens_t)

    context = jnp.concatenate([context_mine, context_other], axis=1)
    out_both = jnp.concatenate([w_out, out_other[:width]], axis=0)
    b_up_other = jnp.sum(out_other[width:].astype(F32), axis=0)
    tokens_mine = lax.dynamic_slice_in_dim(layer_in, place * half, half, 0).astype(F32)

    far = lax.dynamic_slice_in_dim(context, (1 - core) * half, half, 0)
    near = lax.dynamic_slice_in_dim(context, core * half, half, 0)
    far_branch = partner(matmul(far, out_both).astype(BF16))
    far_branch = after(far_branch, down_first)
    down_second = swap_dp(down_first, 1)
    branch = matmul(near, out_both) + far_branch.astype(F32)
    normed_one, inverse_one = normalize(tokens_mine + branch + b_out)
    hidden_one = normed_one * gain_one + shift_one
    hidden_low_mine = hidden_one.astype(BF16)
    hidden_partner = partner(hidden_low_mine)
    hidden_low = jnp.concatenate([hidden_low_mine, hidden_partner], axis=0)

    def rise(weights, bias):
        up = matmul(hidden_low, weights) + bias
        phi = 0.5 * (1.0 + lax.erf(up * ROOT_HALF))
        slope = phi + up * INV_ROOT_TWO_PI * jnp.exp(-0.5 * up * up)
        return (up * phi).astype(BF16), slope

    active_mine, slope_mine = rise(w_up, b_up)
    up_other = from_halves(up_first, up_second, odd == 1)
    active_other, slope_other = rise(up_other, b_up_other)
    hidden_t = flipped_pair(after(hidden_low_mine, active_other), hidden_partner)
    down_other = from_halves(down_first, after(down_second, hidden_t), odd == 1)
    ffn_terms = matmul(active_mine, w_down) + matmul(active_other, down_other)
    ffn = ffn_terms[:half] + partner(ffn_terms[half:].astype(BF16)).astype(F32)
    normed_two, inverse_two = normalize(hidden_one + ffn + b_down)
    layer_out = (normed_two * gain_two + shift_two).astype(BF16)

    upstream = grad_out.astype(F32)
    grad_gain_two = jnp.sum(upstream * normed_two, axis=0)
    grad_shift_two = jnp.sum(upstream, axis=0)
    grad_two = norm_back(upstream, normed_two, inverse_two, gain_two)
    grad_b_down = jnp.sum(grad_two, axis=0)
    ffn_grad_mine = grad_two.astype(BF16)
    ffn_grad_partner = partner(ffn_grad_mine)
    ffn_grad = jnp.concatenate([ffn_grad_mine, ffn_grad_partner], axis=0)

    ffn_grad_t = flipped_pair(ffn_grad_mine, ffn_grad_partner)
    down_sent = matmul(ffn_grad_t, active_other).astype(BF16)
    down_received = across(down_sent)
    ffn_grad = after(ffn_grad, down_sent)
    grad_up_other = matmul_nt(ffn_grad, down_other) * slope_other
    up_low_other = grad_up_other.astype(BF16)
    grad_up_mine = matmul_nt(ffn_grad, w_down) * slope_mine
    up_low_mine = grad_up_mine.astype(BF16)
    hidden_terms = matmul_nt(up_low_mine, w_up) + matmul_nt(up_low_other, up_other)
    grad_hidden = grad_two + hidden_terms[:half] + partner(
        hidden_terms[half:].astype(BF16)
    ).astype(F32)

    grad_gain_one = jnp.sum(grad_hidden * normed_one, axis=0)
    grad_shift_one = jnp.sum(grad_hidden, axis=0)
    grad_one = norm_back(grad_hidden, normed_one, inverse_one, gain_one)
    grad_b_out = jnp.sum(grad_one, axis=0)
    one_low = grad_one.astype(BF16)
    one_partner = partner(one_low)
    one_across = across(one_low)

    row_sums = jnp.stack(
        [grad_b_out, grad_gain_one, grad_shift_one, grad_b_down, grad_gain_two, grad_shift_two]
    )
    row_sums = row_sums + partner(row_sums)
    hidden_mine = jnp.sum(grad_up_mine, axis=0).reshape(-1, D)
    hidden_other = jnp.sum(grad_up_other, axis=0).reshape(-1, D)
    sums_received = across(jnp.concatenate([row_sums, hidden_other], axis=0))

    def by_parity(grad):
        pieces = by_rows(grad.astype(BF16))
        pieces = pieces.reshape((ways // 2, 2) + pieces.shape[1:])
        return tuple(
            lax.dynamic_index_in_dim(pieces, which, 1, keepdims=False)
            for which in (odd, 1 - odd)
        )

    hidden_t = after(hidden_t, one_low)
    other_kept, other_sent = by_parity(matmul(hidden_t, up_low_other))
    mine_kept, mine_sent = by_parity(matmul(hidden_t, up_low_mine))
    up_sent = jnp.concatenate([mine_sent, other_sent], axis=0)
    up_received = swap_dp(up_sent, 1)

    here = jnp.full((1,), core, jnp.int32)
    low_near, columns_near, in_near, out_near = attend_backward(
        here, (one_low, after(one_partner, up_sent)), w_out, weights, saved_near
    )
    down_mine = matmul(ffn_grad_t, active_mine)

    one_across = after(one_across, low_near)
    across_partner = partner(one_across)
    down_received = after(down_received, one_across)
    sums_received = after(sums_received, one_across)
    sums = jnp.concatenate([row_sums, hidden_mine], axis=0) + sums_received
    sum_high = lax.reduce_precision(sums, 8, 7)
    sum_terms = jnp.concatenate([sum_high, sums - sum_high], axis=0).astype(BF16)
    down_pieces = by_rows((down_mine + down_received.astype(F32)).astype(BF16))
    share = down_pieces.shape[1]
    count = sum_terms.shape[0]
    sum_pieces = jnp.broadcast_to(
        jnp.pad(sum_terms, ((0, -count % 8), (0, 0)))[None], (ways, count + -count % 8, D)
    )
    down_pieces = jnp.concatenate([down_pieces, sum_pieces], axis=1)
    down_sums = scatter_pieces(down_pieces)
    grad_w_down = down_sums[:share].T
    sums = jnp.sum(down_sums[share : share + count].reshape(2, count // 2, D), axis=0)

    up_received = after(up_received, one_across)
    up_mine = mine_kept.astype(F32) + up_received[: ways // 2].astype(F32)
    up_other = other_kept.astype(F32) + up_received[ways // 2 :].astype(F32)
    up_other = up_other.astype(BF16)
    up_across = across(up_other)

    low_far, columns_far, in_far, out_far = attend_backward(
        here,
        (one_across, after(across_partner, down_pieces, up_other)),
        w_out,
        weights,
        saved_far,
    )
    in_sent = lax.dynamic_slice_in_dim(in_far, (1 - core) * half, half, 0)
    in_kept = lax.dynamic_slice_in_dim(in_far, core * half, half, 0)
    up_across = after(up_across, low_far)
    up_pieces = (up_mine + up_across.astype(F32)).astype(BF16)
    member = lax.axis_index("dp") // 2
    grad_w_up = lax.dynamic_index_in_dim(up_pieces, member, 0, keepdims=False).astype(F32)
    for step in range(1, ways // 2):
        piece = lax.dynamic_index_in_dim(up_pieces, member ^ step, 0, keepdims=False)
        grad_w_up = grad_w_up + swap_dp(piece, 2 * step).astype(F32)

    in_other = across(
        (in_kept.astype(F32) + partner(in_sent).astype(F32)).astype(BF16)
    )

    near_t = lax.dynamic_index_in_dim(tokens_t, sequence, 0, keepdims=False)
    far_t = lax.dynamic_index_in_dim(tokens_t, 1 - sequence, 0, keepdims=False)
    qkv_sum = matmul(near_t, low_near) + matmul(far_t, low_far)
    columns = columns_near + columns_far
    row = jnp.concatenate([columns[0], jnp.zeros_like(columns[0]), columns[2]])
    out_sum = (out_near + out_far).T.astype(BF16)
    bias_terms = jnp.pad(three_terms(row), ((0, 0), (0, width)))
    pieces = jnp.concatenate(
        [
            jnp.concatenate([by_rows(qkv_sum.astype(BF16)), by_rows(out_sum)], axis=2),
            jnp.broadcast_to(bias_terms[None], (ways,) + bias_terms.shape),
        ],
        axis=1,
    )
    qkv = scatter_pieces(pieces)
    bias_sums = jnp.sum(qkv[share:], axis=0)
    qkv = qkv[:share]
    grad_w_out = qkv[:, 3 * width :].T

    in_sent = lax.dynamic_slice_in_dim(in_near, (1 - core) * half, half, 0)
    in_kept = lax.dynamic_slice_in_dim(in_near, core * half, half, 0)
    grad_in = (
        grad_one
        + in_kept.astype(F32)
        + partner(in_sent).astype(F32)
        + in_other.astype(F32)
    )

    return (
        layer_out,
        grad_in,
        qkv[:, :width],
        bias_sums[:width],
        qkv[:, width : 2 * width],
        qkv[:, 2 * width : 3 * width],
        bias_sums[2 * width : 3 * width],
        grad_w_out,
        sums[0],
        sums[1],
        sums[2],
        grad_w_up,
        sums[6:].reshape(-1),
        grad_w_down,
        sums[3],
        sums[4],
        sums[5],
    )


def solution(mesh):
    in_specs = (
        P("dp", None),
        P("dp", None),
        P("dp", None, None),
        P(None, "tensor"),
        P("tensor"),
        P(None, "tensor"),
        P(None, "tensor"),
        P("tensor"),
        P("tensor", None),
        P(),
        P(),
        P(),
        P(None, "tensor"),
        P("tensor"),
        P("tensor", None),
        P(),
        P(),
        P(),
        P(("dp", "tensor"), None),
    )
    out_specs = (
        P(("dp", "tensor"), None),
        P(("dp", "tensor"), None),
        P("dp", "tensor"),
        P("tensor"),
        P("dp", "tensor"),
        P("dp", "tensor"),
        P("tensor"),
        P("tensor", "dp"),
        P(),
        P(),
        P(),
        P("dp", "tensor"),
        P("tensor"),
        P("tensor", "dp"),
        P(),
        P(),
        P(),
    )
    return jax.shard_map(
        on_device, mesh=mesh, in_specs=in_specs, out_specs=out_specs, check_vma=False
    )
```

```python
import functools

import jax
import jax.numpy as jnp
from jax import lax
from jax.experimental import pallas as pl
from jax.experimental.pallas import tpu as pltpu
from jax.sharding import PartitionSpec as P

D = 768
HEADS = 12
HEAD_DIM = D // HEADS

EPS = 1e-06
NEG = -1e30
ROOT_HALF = 0.7071067811865476
INV_ROOT_TWO_PI = 0.3989422804014327
BF16 = jnp.bfloat16
F32 = jnp.float32
BLOCK_MOST = 256
EXTRA = 8
NOMINAL = pl.CostEstimate(flops=1000, bytes_accessed=1000, transcendentals=0)
QTILE = 256
KTILE = 256
TILE = 256
SUMS = 8


def nn(left, right):
    return jnp.dot(left, right, preferred_element_type=F32)


def tn(left, right):
    return lax.dot_general(left, right, (((0,), (0,)), ((), ())), preferred_element_type=F32)


def nt(left, right):
    return lax.dot_general(left, right, (((1,), (1,)), ((), ())), preferred_element_type=F32)


VMEM = pl.BlockSpec(memory_space=pltpu.VMEM)
SMEM = pl.BlockSpec(memory_space=pltpu.SMEM)


def call(kernel, name, scalars, arrays, outs, scratch=()):
    return pl.pallas_call(
        kernel,
        out_shape=tuple(jax.ShapeDtypeStruct(shape, kind) for shape, kind in outs),
        in_specs=[SMEM] * len(scalars) + [VMEM] * len(arrays),
        out_specs=(VMEM,) * len(outs),
        scratch_shapes=list(scratch),
        cost_estimate=NOMINAL,
        name=name,
    )(*scalars, *arrays)


def pieces_of(column):
    high = column.astype(BF16).astype(F32)
    middle = (column - high).astype(BF16).astype(F32)
    return high, middle, column - high - middle


def with_pieces(base, lane, first, column):
    high, middle, low = pieces_of(column)
    base = jnp.where(lane == first, -high, base)
    base = jnp.where(lane == first + 1, -middle, base)
    return jnp.where(lane == first + 2, -low, base)


def lanes_of(head, rows):
    odd = lax.rem(head, 2)
    lane = lax.broadcasted_iota(jnp.int32, (rows, 2 * HEAD_DIM), 1)
    own = (lane >= HEAD_DIM * odd) & (lane < HEAD_DIM * (odd + 1))
    return odd, lane, own, HEAD_DIM * (1 - odd) + EXTRA


def forward_kernel(
    reach, place_ref, tokens_ref, w_query_ref, w_key_ref, w_value_ref, b_query_ref, b_value_ref,
    blocks_ref, links_ref, context_ref, query_ref, key_ref, value_ref,
    query_s, key_s, value_s, context_s, table_s, marks_s
):
    length = blocks_ref.shape[1]
    width = w_query_ref.shape[0]
    tiles = pl.cdiv(width, 128)
    chosen = place_ref[0]
    tokens = tokens_ref[pl.ds(pl.multiple_of(chosen * length, length), length)]
    for store, made in (
        (query_s, (nt(tokens, w_query_ref[...]) + b_query_ref[...]) * HEAD_DIM**-0.5),
        (key_s, nt(tokens, w_key_ref[...])),
        (value_s, nt(tokens, w_value_ref[...]) + b_value_ref[...]),
    ):
        for tile in range(tiles):
            last = min(128, width - 128 * tile)
            store[tile, :, :last] = made[:, 128 * tile : 128 * tile + last]

    row = blocks_ref[pl.ds(chosen, 1)].astype(F32)
    column = jnp.broadcast_to(row, (8, length)).T[:, :1]
    lane = lax.broadcasted_iota(jnp.int32, (length, 128), 1)
    onehot = jnp.where(column == lane.astype(F32), 1.0, 0.0)
    links = links_ref[chosen]
    count = links.shape[0]
    above = lax.broadcasted_iota(jnp.int32, (count, count), 0)
    below = lax.broadcasted_iota(jnp.int32, (count, count), 1)
    seen = (above == below) | ((above > below) & (links == 1))
    pairs = jnp.where(seen, 0.0, NEG).astype(BF16)
    sees = nn(onehot[:, :count].astype(BF16), pairs)
    table_s[...] = jnp.zeros_like(table_s)
    table_s[1, :, :count] = sees
    table_s[0, :, HEAD_DIM : HEAD_DIM + count] = sees
    ones = jnp.where((lane >= EXTRA) & (lane < EXTRA + 3), 1.0, onehot)
    marks_s[1] = ones
    marks_s[0] = pltpu.roll(ones, HEAD_DIM, 1)

    def one_head(head, carry):
        tile = head // 2
        odd, lane, own, first = lanes_of(head, length)
        marks = marks_s[odd]
        key_ref[head] = jnp.where(own, key_s[tile], marks).astype(BF16)
        ones = jnp.where((lane >= first) & (lane < first + 3), 1.0, 0.0)
        value_ref[head] = jnp.where(own, value_s[tile], ones).astype(BF16)
        odd, lane, own, first = lanes_of(head, QTILE)
        for start in range(0, length, QTILE):
            rows = slice(start, start + QTILE)
            seen = min(length, start + QTILE + reach)
            query = jnp.where(own, query_s[tile, rows], table_s[odd, rows])
            scores = nt(query.astype(BF16), key_ref[head, :seen])
            highest = jnp.max(scores, axis=-1, keepdims=True)
            weights = jnp.exp(scores - highest).astype(BF16)
            mixed = nn(weights, value_ref[head, :seen])
            total = jnp.sum(jnp.where(lane == first, mixed, 0.0), axis=-1, keepdims=True)
            context_s[tile, rows] = jnp.where(own, mixed * (1.0 / total), context_s[tile, rows])
            query_ref[head, rows] = with_pieces(
                query, lane, first, highest + jnp.log(total)
            ).astype(BF16)
        return carry

    lax.fori_loop(0, width // HEAD_DIM, one_head, 0)
    for tile in range(tiles):
        last = min(128, width - 128 * tile)
        context_ref[:, 128 * tile : 128 * tile + last] = context_s[tile, :, :last].astype(BF16)


def attend_forward(place, layer_in, weights, block_of, block_links):
    length = block_of.shape[1]
    width = weights[0].shape[0]
    heads = width // HEAD_DIM
    tiles = pl.cdiv(width, 128)
    big = ((heads, length, 128), BF16)
    tall = pltpu.VMEM((tiles, length, 128), F32)
    both = pltpu.VMEM((2, length, 128), F32)
    return call(
        functools.partial(forward_kernel, BLOCK_MOST),
        "attend_forward",
        [place],
        [layer_in, *weights, block_of, block_links],
        [((length, width), BF16), big, big, big],
        [tall] * 4 + [both] * 2,
    )


def backward_kernel(
    reach, core_ref, first_ref, second_ref, out_ref, w_query_ref, w_key_ref, w_value_ref,
    context_ref, query_ref, key_ref, value_ref, grads_ref, sums_ref, in_ref, w_out_ref,
    grad_s, context_s, query_s, query_t, key_s, value_s, extended_s
):
    length, width = context_ref.shape
    half = length // 2
    tiles = pl.cdiv(width, 128)
    outward = jnp.zeros((width, out_ref.shape[1]), F32)
    for part, upstream_ref in enumerate((first_ref, second_ref)):
        begin = pl.multiple_of(lax.rem(core_ref[0] + part, 2) * half, half)
        rows = pl.ds(begin, half)
        made = nt(upstream_ref[...], out_ref[...]).astype(BF16).astype(F32)
        context = context_ref[rows]
        outward += tn(context, upstream_ref[...])
        aligned = made * context.astype(F32)
        for tile in range(tiles):
            last = min(128, width - 128 * tile)
            grad_s[tile, rows, :last] = made[:, 128 * tile : 128 * tile + last]
            context_s[tile, rows, :last] = aligned[:, 128 * tile : 128 * tile + last]
    w_out_ref[...] = outward

    def one_head(head, carry):
        tile = head // 2
        odd, lane, own, first = lanes_of(head, length)
        centre = jnp.sum(jnp.where(own, context_s[tile], 0.0), axis=-1, keepdims=True)
        grad = jnp.where(own, grad_s[tile], 0.0)
        extended_s[...] = with_pieces(grad, lane, first, centre).astype(BF16)
        odd, lane, own, first = lanes_of(head, KTILE)
        query_s[...] = jnp.zeros_like(query_s)
        for start in range(0, length, KTILE):
            rows = slice(start, start + KTILE)
            seen = max(0, start - reach)
            scores = nt(key_ref[head, rows], query_ref[head, seen:])
            probs = jnp.exp(scores)
            pulled = nt(value_ref[head, rows], extended_s[seen:])
            changed = (probs * pulled).astype(BF16)
            grad_value = nn(probs.astype(BF16), extended_s[seen:])
            grad_key = nn(changed, query_ref[head, seen:])
            value_s[tile, rows] = jnp.where(own, grad_value, value_s[tile, rows])
            key_s[tile, rows] = jnp.where(own, grad_key, key_s[tile, rows])
            query_s[seen:] += tn(changed, key_ref[head, rows])
        odd, lane, own, first = lanes_of(head, length)
        query_t[tile] = jnp.where(own, query_s[...] * HEAD_DIM**-0.5, query_t[tile])
        return carry

    lax.fori_loop(0, width // HEAD_DIM, one_head, 0)
    inward = jnp.zeros((length, in_ref.shape[1]), F32)
    for kind, (store, weight_ref) in enumerate(
        ((query_t, w_query_ref), (key_s, w_key_ref), (value_s, w_value_ref))
    ):
        for tile in range(tiles):
            last = min(128, width - 128 * tile)
            made = store[tile, :, :last]
            low = made.astype(BF16)
            begin = kind * width + 128 * tile
            grads_ref[:, begin : begin + last] = low
            inward += nn(low, weight_ref[128 * tile : 128 * tile + last])
            if kind != 1:
                sums_ref[kind : kind + 1, 128 * tile : 128 * tile + last] = jnp.sum(
                    made, axis=0, keepdims=True
                )
    in_ref[...] = inward.astype(BF16)


def attend_backward(core, upstream, out, weights, saved):
    length, width = saved[0].shape
    depth = out.shape[1]
    tall = pltpu.VMEM((pl.cdiv(width, 128), length, 128), F32)
    return call(
        functools.partial(backward_kernel, BLOCK_MOST),
        "attend_backward",
        [core],
        [*upstream, out, *weights, *saved],
        [
            ((length, 3 * width), BF16),
            ((3, width), F32),
            ((length, depth), BF16),
            ((width, depth), F32),
        ],
        [tall, tall, pltpu.VMEM((length, 128), F32), tall, tall, tall]
        + [pltpu.VMEM((length, 128), BF16)],
    )


def out_kernel(core_ref, mine_ref, other_ref, w_mine_ref, w_other_ref, far_ref, near_ref):
    width = mine_ref.shape[1]
    half = near_ref.shape[0]
    for begin, made_ref in ((1 - core_ref[0], far_ref), (core_ref[0], near_ref)):
        rows = pl.ds(pl.multiple_of(begin * half, half), half)
        made = nn(mine_ref[rows], w_mine_ref[...]) + nn(other_ref[rows], w_other_ref[:width])
        made_ref[...] = made.astype(made_ref.dtype)


def mean(values):
    return jnp.mean(values, axis=-1, keepdims=True)


def norm_one_kernel(
    place_ref, tokens_ref, near_ref, far_ref, bias_ref, gain_ref, shift_ref,
    hidden_ref, low_ref, normed_ref, inverse_ref
):
    half = near_ref.shape[0]
    tokens = tokens_ref[pl.ds(pl.multiple_of(place_ref[0] * half, half), half)].astype(F32)
    values = tokens + near_ref[...] + far_ref[...].astype(F32) + bias_ref[...]
    centre = values - mean(values)
    inverse = lax.rsqrt(mean(centre * centre) + EPS)
    normed = centre * inverse
    hidden = normed * gain_ref[...] + shift_ref[...]
    hidden_ref[...] = hidden
    low_ref[...] = hidden.astype(BF16)
    normed_ref[...] = normed
    inverse_ref[...] = inverse


def gelu_into(up, rows, active_ref, slope_ref):
    phi = 0.5 * (1.0 + lax.erf(up * ROOT_HALF))
    active_ref[rows] = (up * phi).astype(BF16)
    slope_ref[rows] = phi + up * INV_ROOT_TWO_PI * jnp.exp(-0.5 * up * up)


def rise_kernel(mine_ref, other_ref, w_up_ref, bias_ref, active_ref, slope_ref):
    half = mine_ref.shape[0]
    for part, ref in enumerate((mine_ref, other_ref)):
        def tile(step, carry):
            begin = pl.multiple_of(step * TILE, TILE)
            up = nn(ref[pl.ds(begin, TILE)], w_up_ref[...]) + bias_ref[...]
            gelu_into(up, pl.ds(part * half + begin, TILE), active_ref, slope_ref)
            return carry

        lax.fori_loop(0, half // TILE, tile, 0)


def rise_other_kernel(
    order_ref, mine_ref, other_ref, first_ref, second_ref, out_ref, active_ref, slope_ref, joined_ref
):
    rows = first_ref.shape[0]
    for begin, ref in ((order_ref[0], first_ref), (1 - order_ref[0], second_ref)):
        joined_ref[pl.ds(pl.multiple_of(begin * rows, rows), rows)] = ref[...]
    bias = jnp.sum(out_ref[out_ref.shape[0] - 8 :].astype(F32), axis=0, keepdims=True)
    half = mine_ref.shape[0]
    for part, ref in enumerate((mine_ref, other_ref)):
        def tile(step, carry):
            begin = pl.multiple_of(step * TILE, TILE)
            up = nn(ref[pl.ds(begin, TILE)], joined_ref[...]) + bias
            gelu_into(up, pl.ds(part * half + begin, TILE), active_ref, slope_ref)
            return carry

        lax.fori_loop(0, half // TILE, tile, 0)


def fall_kernel(
    order_ref, mine_ref, other_ref, w_down_ref, first_ref, second_ref, near_ref, far_ref, joined_ref
):
    rows = first_ref.shape[0]
    half = near_ref.shape[0]
    for begin, ref in ((order_ref[0], first_ref), (1 - order_ref[0], second_ref)):
        joined_ref[pl.ds(pl.multiple_of(begin * rows, rows), rows)] = ref[...]
    for begin, made_ref in ((half, far_ref), (0, near_ref)):
        part = slice(begin, begin + half)
        made = nn(mine_ref[part], w_down_ref[...]) + nn(other_ref[part], joined_ref[...])
        made_ref[...] = made.astype(made_ref.dtype)


def store_rows(sums_ref, rows):
    sums_ref[...] = jnp.zeros_like(sums_ref)
    for index, row in rows:
        sums_ref[index : index + 1] = row


def total(values):
    return jnp.sum(values, axis=0, keepdims=True)


def norm_two_kernel(
    hidden_ref, near_ref, far_ref, bias_ref, gain_ref, shift_ref, upstream_ref,
    layer_ref, grad_ref, low_ref, sums_ref
):
    values = hidden_ref[...] + near_ref[...] + far_ref[...].astype(F32) + bias_ref[...]
    centre = values - mean(values)
    inverse = lax.rsqrt(mean(centre * centre) + EPS)
    normed = centre * inverse
    layer_ref[...] = (normed * gain_ref[...] + shift_ref[...]).astype(BF16)
    upstream = upstream_ref[...].astype(F32)
    shaped = upstream * gain_ref[...]
    grad = inverse * (shaped - mean(shaped) - normed * mean(shaped * normed))
    grad_ref[...] = grad
    low_ref[...] = grad.astype(BF16)
    store_rows(
        sums_ref, ((3, total(grad)), (4, total(upstream * normed)), (5, total(upstream)))
    )


def norm_one_back_kernel(
    grad_two_ref, near_ref, far_ref, normed_ref, inverse_ref, gain_ref, sums_two_ref, sums_up_ref,
    grad_ref, low_ref, sums_ref
):
    upstream = grad_two_ref[...] + near_ref[...] + far_ref[...].astype(F32)
    normed = normed_ref[...]
    shaped = upstream * gain_ref[...]
    grad = inverse_ref[...] * (shaped - mean(shaped) - normed * mean(shaped * normed))
    grad_ref[...] = grad
    low_ref[...] = grad.astype(BF16)
    store_rows(
        sums_ref,
        (
            (0, total(grad)),
            (1, total(upstream * normed)),
            (2, total(upstream)),
            (3, sums_two_ref[3:4]),
            (4, sums_two_ref[4:5]),
            (5, sums_two_ref[5:6]),
            (6, sums_up_ref[0:1]),
            (7, sums_up_ref[1:2]),
        ),
    )


def down_other_kernel(mine_ref, other_ref, active_ref, sent_ref):
    half = mine_ref.shape[0]
    sent_ref[...] = (
        tn(mine_ref[...], active_ref[:half]) + tn(other_ref[...], active_ref[half:])
    ).astype(BF16)


def ffn_back_kernel(
    mine_ref, other_ref, w_down_ref, joined_down_ref, slope_mine_ref, slope_other_ref,
    w_up_ref, joined_up_ref, low_mine_ref, low_other_ref, near_ref, far_ref, sums_ref
):
    half = mine_ref.shape[0]
    sums_ref[...] = jnp.zeros_like(sums_ref)
    for start, grads_ref, made_ref in ((half, other_ref, far_ref), (0, mine_ref, near_ref)):
        def tile(step, carry):
            begin = pl.multiple_of(step * TILE, TILE)
            rows = pl.ds(start + begin, TILE)
            grads = grads_ref[pl.ds(begin, TILE)]
            made = jnp.zeros((TILE, near_ref.shape[1]), F32)
            for index, (down_ref, slope_ref, up_ref, low_ref) in enumerate(
                (
                    (w_down_ref, slope_mine_ref, w_up_ref, low_mine_ref),
                    (joined_down_ref, slope_other_ref, joined_up_ref, low_other_ref),
                )
            ):
                grad = nt(grads, down_ref[...]) * slope_ref[rows]
                sums_ref[index : index + 1] += total(grad)
                low = grad.astype(BF16)
                low_ref[rows] = low
                made += nt(low, up_ref[...])
            made_ref[pl.ds(begin, TILE)] = made.astype(made_ref.dtype)
            return carry

        lax.fori_loop(0, half // TILE, tile, 0)


def up_grads_kernel(
    odd_ref, mine_ref, other_ref, low_mine_ref, low_other_ref, kept_ref, sent_ref, whole_s
):
    half = mine_ref.shape[0]
    count, share = kept_ref.shape[0] // 2, kept_ref.shape[1]
    odd = odd_ref[0]
    for index, low_ref in enumerate((low_mine_ref, low_other_ref)):
        whole_s[...] = tn(mine_ref[...], low_ref[:half]) + tn(other_ref[...], low_ref[half:])
        for member in range(count):
            for parity, made_ref in ((odd, kept_ref), (1 - odd, sent_ref)):
                begin = pl.multiple_of((2 * member + parity) * share, 8)
                made_ref[index * count + member] = whole_s[pl.ds(begin, share)].astype(
                    made_ref.dtype
                )


def down_pieces_kernel(
    mine_ref, other_ref, active_ref, received_ref, sums_ref, sums_received_ref, pieces_ref
):
    half = mine_ref.shape[0]
    ways, rows = pieces_ref.shape[:2]
    share = rows - 2 * SUMS
    made = tn(mine_ref[...], active_ref[:half]) + tn(other_ref[...], active_ref[half:])
    made = (made + received_ref[...].astype(F32)).astype(BF16)
    sums = sums_ref[...]
    received = sums_received_ref[...]
    row = lax.broadcasted_iota(jnp.int32, sums.shape, 0)
    crossed = jnp.where(row == 6, received[7:8], received)
    sums = sums + crossed
    high = sums.astype(BF16)
    low = (sums - high.astype(F32)).astype(BF16)
    for index in range(ways):
        pieces_ref[index, :share] = made[index * share : (index + 1) * share]
        pieces_ref[index, share : share + SUMS] = high
        pieces_ref[index, share + SUMS :] = low


def qkv_pieces_kernel(
    place_ref, tokens_ref, near_ref, far_ref, sums_near_ref, sums_far_ref, out_near_ref, out_far_ref,
    pieces_ref
):
    ways, rows = pieces_ref.shape[:2]
    share = rows - SUMS
    length, columns = near_ref.shape
    width = out_near_ref.shape[0]
    made = jnp.zeros((tokens_ref.shape[1], columns), F32)
    for chosen, low_ref in ((place_ref[0], near_ref), (1 - place_ref[0], far_ref)):
        tokens = tokens_ref[pl.ds(pl.multiple_of(chosen * length, length), length)]
        made += tn(tokens, low_ref[...])
    made = made.astype(BF16)
    out = (out_near_ref[...] + out_far_ref[...]).T.astype(BF16)
    sums = sums_near_ref[...] + sums_far_ref[...]
    high, middle, low = pieces_of(sums)
    zeros = jnp.zeros((SUMS, columns + width), BF16)
    for index in range(ways):
        pieces_ref[index, share:] = zeros
        for kind in (0, 2):
            lanes = slice(kind * width, (kind + 1) * width)
            for term, rows in enumerate((high, middle, low)):
                pieces_ref[index, share + term : share + term + 1, lanes] = rows[
                    kind : kind + 1
                ].astype(BF16)
        part = slice(index * share, (index + 1) * share)
        pieces_ref[index, :share, :columns] = made[part]
        pieces_ref[index, :share, columns:] = out[part]


def swap_tensor(array, mask):
    ways = lax.axis_size("tensor")
    return lax.ppermute(array, "tensor", [(i, i ^ mask) for i in range(ways)])


def swap_dp(array, mask):
    ways = lax.axis_size("dp")
    return lax.ppermute(array, "dp", [(i, i ^ mask) for i in range(ways)])


def across(array):
    return swap_tensor(array, 2)


def partner(array):
    return swap_tensor(array, 1)


def after(array, *earlier):
    return lax.optimization_barrier((array,) + earlier)[0]


def three_terms(row):
    high = lax.reduce_precision(row, 8, 7)
    middle = lax.reduce_precision(row - high, 8, 7)
    terms = jnp.stack([high, middle, row - high - middle]).astype(BF16)
    return jnp.pad(terms, ((0, 5), (0, 0)))


def scatter_pieces(pieces):
    return jnp.sum(lax.all_to_all(pieces, "dp", 0, 0).astype(F32), axis=0)


def on_device(
    layer_in,
    block_of,
    block_links,
    w_query,
    b_query,
    w_key,
    w_value,
    b_value,
    w_out,
    b_out,
    gain_one,
    shift_one,
    w_up,
    b_up,
    w_down,
    b_down,
    gain_two,
    shift_two,
    grad_out,
):
    length = block_of.shape[1]
    half = length // 2
    place = lax.axis_index("tensor")
    sequence = place // 2
    core = place % 2
    width = w_query.shape[1]
    hidden = w_up.shape[1]
    fall_half = w_down.shape[0] // 2
    rise_half = w_up.shape[0] // 2
    ways = lax.axis_size("dp")
    share = D // ways
    odd = lax.axis_index("dp") % 2

    def scalar(value):
        return jnp.full((1,), value, jnp.int32)

    def row(vector):
        return vector.reshape(1, -1)

    up_first = across(lax.dynamic_slice_in_dim(w_up, odd * rise_half, rise_half, 0))
    down_sent = lax.dynamic_slice_in_dim(w_down, odd * fall_half, fall_half, 0)
    out_sent = jnp.concatenate([w_out, three_terms(b_up)], axis=0)

    weights = (w_query.T, w_key.T, w_value.T)
    inputs = weights + (row(b_query), row(b_value))
    near_place, far_place = scalar(sequence), scalar(1 - sequence)
    saved_far = attend_forward(
        after(far_place, down_sent, out_sent), layer_in, inputs, block_of, block_links
    )
    context_other = across(saved_far[0])
    out_received = across(after(out_sent, saved_far[0]))
    down_first = across(after(down_sent, saved_far[0]))
    saved_near = attend_forward(
        after(near_place, saved_far[0]), layer_in, inputs, block_of, block_links
    )
    context_mine = after(saved_near[0], up_first)
    up_second = swap_dp(up_first, 1)

    here = scalar(core)
    far, near = call(
        out_kernel,
        "out",
        [here],
        [context_mine, context_other, w_out, out_received],
        [((half, D), BF16), ((half, D), F32)],
    )
    hidden_one, hidden_mine, normed_one, inverse_one = call(
        norm_one_kernel,
        "norm_one",
        [scalar(place)],
        [layer_in, near, partner(far), row(b_out), row(gain_one), row(shift_one)],
        [((half, D), F32), ((half, D), BF16), ((half, D), F32), ((half, 1), F32)],
    )
    hidden_partner = partner(hidden_mine)
    active_mine, slope_mine = call(
        rise_kernel,
        "rise_mine",
        [],
        [hidden_mine, hidden_partner, w_up, row(b_up)],
        [((length, hidden), BF16), ((length, hidden), F32)],
    )
    down_first = after(down_first, active_mine)
    down_second = swap_dp(down_first, 1)
    order = scalar(odd)
    active_other, slope_other, up_other = call(
        rise_other_kernel,
        "rise_other",
        [order],
        [hidden_mine, hidden_partner, up_first, after(up_second, active_mine), out_received],
        [((length, hidden), BF16), ((length, hidden), F32), (w_up.shape, BF16)],
    )
    near, far, down_other = call(
        fall_kernel,
        "fall",
        [order],
        [active_mine, active_other, w_down, down_first, after(down_second, active_other)],
        [((half, D), F32), ((half, D), BF16), (w_down.shape, BF16)],
    )
    layer_out, grad_two, ffn_mine, sums_two = call(
        norm_two_kernel,
        "norm_two",
        [],
        [hidden_one, near, partner(far), row(b_down), row(gain_two), row(shift_two), grad_out],
        [((half, D), BF16), ((half, D), F32), ((half, D), BF16), ((SUMS, D), F32)],
    )
    ffn_partner = partner(ffn_mine)

    (down_sent,) = call(
        down_other_kernel,
        "down_other",
        [],
        [ffn_mine, ffn_partner, active_other],
        [((D, hidden), BF16)],
    )
    down_received = across(down_sent)
    low_mine, low_other, near, far, sums_up = call(
        ffn_back_kernel,
        "ffn_back",
        [],
        [ffn_mine, after(ffn_partner, down_sent), w_down, down_other]
        + [slope_mine, slope_other, w_up, up_other],
        [((length, hidden), BF16)] * 2
        + [((half, D), F32), ((half, D), BF16), ((SUMS, hidden), F32)],
    )
    grad_one, one_mine, sums = call(
        norm_one_back_kernel,
        "norm_one_back",
        [],
        [grad_two, near, partner(far), normed_one, inverse_one, row(gain_one), sums_two, sums_up],
        [((half, D), F32), ((half, D), BF16), ((SUMS, D), F32)],
    )
    one_partner = partner(one_mine)
    sums_partner = partner(sums)
    rows = lax.broadcasted_iota(jnp.int32, sums.shape, 0)
    sums = sums + jnp.where(rows < 6, sums_partner, 0.0)
    sums_received = across(sums)
    one_across = across(after(one_mine, sums))

    up_kept, up_sent = call(
        up_grads_kernel,
        "up_grads",
        [order],
        [hidden_mine, hidden_partner, after(low_mine, one_mine), low_other],
        [((ways, share, hidden), F32), ((ways, share, hidden), BF16)],
        [pltpu.VMEM((D, hidden), F32)],
    )
    up_received = swap_dp(up_sent, 1)
    low_near, columns_near, in_near, out_near = attend_backward(
        here, (one_mine, after(one_partner, up_sent)), w_out, weights, saved_near
    )

    down_received = after(down_received, low_near)
    (down_pieces,) = call(
        down_pieces_kernel,
        "down_pieces",
        [],
        [ffn_mine, ffn_partner, active_mine, down_received, sums, sums_received],
        [((ways, share + 2 * SUMS, hidden), BF16)],
    )
    down_sums = scatter_pieces(down_pieces)
    grad_w_down = down_sums[:share].T
    sums = down_sums[share : share + SUMS] + down_sums[share + SUMS :]

    one_across = after(one_across, down_pieces)
    across_partner = partner(one_across)
    up_received = after(up_received, down_pieces)
    up_terms = up_kept + up_received.astype(F32)
    up_mine = up_terms[: ways // 2]
    up_other = up_terms[ways // 2 :].astype(BF16)
    up_across = across(up_other)

    low_far, columns_far, in_far, out_far = attend_backward(
        here, (one_across, after(across_partner, up_other)), w_out, weights, saved_far
    )
    (pieces,) = call(
        qkv_pieces_kernel,
        "qkv_pieces",
        [near_place],
        [layer_in, low_near, low_far, columns_near, columns_far, out_near, out_far],
        [((ways, share + SUMS, 4 * width), BF16)],
    )
    qkv = scatter_pieces(pieces)
    bias_sums = jnp.sum(qkv[share:], axis=0)
    qkv = qkv[:share]
    grad_w_out = qkv[:, 3 * width :].T

    def core_parts(terms):
        parts = terms.reshape(2, half, D)
        kept = lax.dynamic_index_in_dim(parts, core, 0, keepdims=False)
        sent = lax.dynamic_index_in_dim(parts, 1 - core, 0, keepdims=False)
        return kept.astype(F32), partner(sent).astype(F32)

    far_kept, far_received = core_parts(in_far)
    in_other = across((far_kept + far_received).astype(BF16))
    near_kept, near_received = core_parts(in_near)

    up_across = after(up_across, low_far)
    up_pieces = (up_mine + up_across.astype(F32)).astype(BF16)
    member = lax.axis_index("dp") // 2
    grad_w_up = lax.dynamic_index_in_dim(up_pieces, member, 0, keepdims=False).astype(F32)
    for step in range(1, ways // 2):
        piece = lax.dynamic_index_in_dim(up_pieces, member ^ step, 0, keepdims=False)
        grad_w_up = grad_w_up + swap_dp(piece, 2 * step).astype(F32)

    grad_in = grad_one + near_kept + near_received + in_other.astype(F32)

    return (
        layer_out,
        grad_in,
        qkv[:, :width],
        bias_sums[:width],
        qkv[:, width : 2 * width],
        qkv[:, 2 * width : 3 * width],
        bias_sums[2 * width : 3 * width],
        grad_w_out,
        sums[0],
        sums[1],
        sums[2],
        grad_w_up,
        sums[6:7].reshape(-1),
        grad_w_down,
        sums[3],
        sums[4],
        sums[5],
    )


def solution(mesh):
    in_specs = (
        P("dp", None),
        P("dp", None),
        P("dp", None, None),
        P(None, "tensor"),
        P("tensor"),
        P(None, "tensor"),
        P(None, "tensor"),
        P("tensor"),
        P("tensor", None),
        P(),
        P(),
        P(),
        P(None, "tensor"),
        P("tensor"),
        P("tensor", None),
        P(),
        P(),
        P(),
        P(("dp", "tensor"), None),
    )
    out_specs = (
        P(("dp", "tensor"), None),
        P(("dp", "tensor"), None),
        P("dp", "tensor"),
        P("tensor"),
        P("dp", "tensor"),
        P("dp", "tensor"),
        P("tensor"),
        P("tensor", "dp"),
        P(),
        P(),
        P(),
        P("dp", "tensor"),
        P("tensor"),
        P("tensor", "dp"),
        P(),
        P(),
        P(),
    )
    return jax.shard_map(
        on_device, mesh=mesh, in_specs=in_specs, out_specs=out_specs, check_vma=False
    )
```

```python
import functools

import jax
import jax.numpy as jnp
from jax import lax
from jax.experimental import pallas as pl
from jax.experimental.pallas import tpu as pltpu
from jax.sharding import PartitionSpec as P

D = 768
HEADS = 12
HEAD_DIM = D // HEADS

EPS = 1e-06
NEG = -1e30
ROOT_HALF = 0.7071067811865476
INV_ROOT_TWO_PI = 0.3989422804014327
BF16 = jnp.bfloat16
F32 = jnp.float32
BLOCK_MOST = 256
EXTRA = 8
COST_FLOPS = 500_000_000
COST_BYTES = 1_000_000
QTILE = 256
KTILE = 256
TILE = 256
SUMS = 8
HELD = True


def nn(left, right):
    return jnp.dot(left, right, preferred_element_type=F32)


def tn(left, right):
    return lax.dot_general(left, right, (((0,), (0,)), ((), ())), preferred_element_type=F32)


def nt(left, right):
    return lax.dot_general(left, right, (((1,), (1,)), ((), ())), preferred_element_type=F32)


VMEM = pl.BlockSpec(memory_space=pltpu.VMEM)
SMEM = pl.BlockSpec(memory_space=pltpu.SMEM)


def call(kernel, name, cost, scalars, arrays, outs, scratch=()):
    return pl.pallas_call(
        kernel,
        out_shape=tuple(
            jax.ShapeDtypeStruct(*out[:2]) if len(out) > 2 else pltpu.VMEM(*out) for out in outs
        ),
        in_specs=[SMEM] * len(scalars) + [VMEM] * len(arrays),
        out_specs=(VMEM,) * len(outs),
        scratch_shapes=list(scratch),
        cost_estimate=pl.CostEstimate(
            flops=int(cost * COST_FLOPS), bytes_accessed=int(cost * COST_BYTES), transcendentals=0
        ),
        name=name,
        compiler_params=pltpu.CompilerParams(
            vmem_limit_bytes=(16 if name.startswith("attend") else 8) * 2**20
        ),
    )(*scalars, *[pltpu.with_memory_space_constraint(array, pltpu.VMEM) for array in arrays])


def pieces_of(column):
    high = column.astype(BF16).astype(F32)
    middle = (column - high).astype(BF16).astype(F32)
    return high, middle, column - high - middle


def with_pieces(base, lane, first, column):
    high, middle, low = pieces_of(column)
    base = jnp.where(lane == first, -high, base)
    base = jnp.where(lane == first + 1, -middle, base)
    return jnp.where(lane == first + 2, -low, base)


def lanes_of(head, rows):
    odd = lax.rem(head, 2)
    lane = lax.broadcasted_iota(jnp.int32, (rows, 2 * HEAD_DIM), 1)
    own = (lane >= HEAD_DIM * odd) & (lane < HEAD_DIM * (odd + 1))
    return odd, lane, own, HEAD_DIM * (1 - odd) + EXTRA


def forward_kernel(
    reach, place_ref, tokens_ref, w_query_ref, w_key_ref, w_value_ref, b_query_ref, b_value_ref,
    blocks_ref, links_ref, context_ref, query_ref, key_ref, value_ref,
    query_s, key_s, value_s, context_s, table_s, marks_s
):
    length = blocks_ref.shape[1]
    width = w_query_ref.shape[0]
    tiles = pl.cdiv(width, 128)
    chosen = place_ref[0]
    tokens = tokens_ref[pl.ds(pl.multiple_of(chosen * length, length), length)]
    for store, made in (
        (query_s, (nt(tokens, w_query_ref[...]) + b_query_ref[...]) * HEAD_DIM**-0.5),
        (key_s, nt(tokens, w_key_ref[...])),
        (value_s, nt(tokens, w_value_ref[...]) + b_value_ref[...]),
    ):
        for tile in range(tiles):
            last = min(128, width - 128 * tile)
            store[tile, :, :last] = made[:, 128 * tile : 128 * tile + last]

    row = blocks_ref[pl.ds(chosen, 1)].astype(F32)
    column = jnp.broadcast_to(row, (8, length)).T[:, :1]
    lane = lax.broadcasted_iota(jnp.int32, (length, 128), 1)
    onehot = jnp.where(column == lane.astype(F32), 1.0, 0.0)
    links = links_ref[chosen]
    count = links.shape[0]
    above = lax.broadcasted_iota(jnp.int32, (count, count), 0)
    below = lax.broadcasted_iota(jnp.int32, (count, count), 1)
    seen = (above == below) | ((above > below) & (links == 1))
    pairs = jnp.where(seen, 0.0, NEG).astype(BF16)
    sees = nn(onehot[:, :count].astype(BF16), pairs)
    table_s[...] = jnp.zeros_like(table_s)
    table_s[1, :, :count] = sees
    table_s[0, :, HEAD_DIM : HEAD_DIM + count] = sees
    ones = jnp.where((lane >= EXTRA) & (lane < EXTRA + 3), 1.0, onehot)
    marks_s[1] = ones
    marks_s[0] = pltpu.roll(ones, HEAD_DIM, 1)

    def one_head(head, carry):
        tile = head // 2
        odd, lane, own, first = lanes_of(head, length)
        marks = marks_s[odd]
        key_ref[head] = jnp.where(own, key_s[tile], marks).astype(BF16)
        ones = jnp.where((lane >= first) & (lane < first + 3), 1.0, 0.0)
        value_ref[head] = jnp.where(own, value_s[tile], ones).astype(BF16)
        odd, lane, own, first = lanes_of(head, QTILE)
        for start in range(0, length, QTILE):
            rows = slice(start, start + QTILE)
            seen = min(length, start + QTILE + reach)
            query = jnp.where(own, query_s[tile, rows], table_s[odd, rows])
            scores = nt(query.astype(BF16), key_ref[head, :seen])
            highest = jnp.max(scores, axis=-1, keepdims=True)
            weights = jnp.exp(scores - highest).astype(BF16)
            mixed = nn(weights, value_ref[head, :seen])
            total = jnp.sum(jnp.where(lane == first, mixed, 0.0), axis=-1, keepdims=True)
            context_s[tile, rows] = jnp.where(own, mixed * (1.0 / total), context_s[tile, rows])
            query_ref[head, rows] = with_pieces(
                query, lane, first, highest + jnp.log(total)
            ).astype(BF16)
        return carry

    lax.fori_loop(0, width // HEAD_DIM, one_head, 0)
    for tile in range(tiles):
        last = min(128, width - 128 * tile)
        context_ref[:, 128 * tile : 128 * tile + last] = context_s[tile, :, :last].astype(BF16)


def attend_forward(place, layer_in, weights, block_of, block_links):
    length = block_of.shape[1]
    width = weights[0].shape[0]
    heads = width // HEAD_DIM
    tiles = pl.cdiv(width, 128)
    big = ((heads, length, 128), BF16, HELD)
    tall = pltpu.VMEM((tiles, length, 128), F32)
    both = pltpu.VMEM((2, length, 128), F32)
    return call(
        functools.partial(forward_kernel, BLOCK_MOST),
        "attend_forward",
        8,
        [place],
        [layer_in, *weights, block_of, block_links],
        [((length, width), BF16), big, big, big],
        [tall] * 4 + [both] * 2,
    )


def backward_kernel(
    reach, core_ref, first_ref, second_ref, out_ref, w_query_ref, w_key_ref, w_value_ref,
    context_ref, query_ref, key_ref, value_ref, grads_ref, sums_ref, in_ref, w_out_ref,
    grad_s, context_s, query_s, query_t, key_s, value_s, extended_s
):
    length, width = context_ref.shape
    half = length // 2
    tiles = pl.cdiv(width, 128)
    outward = jnp.zeros((width, out_ref.shape[1]), F32)
    for part, upstream_ref in enumerate((first_ref, second_ref)):
        begin = pl.multiple_of(lax.rem(core_ref[0] + part, 2) * half, half)
        rows = pl.ds(begin, half)
        made = nt(upstream_ref[...], out_ref[...]).astype(BF16).astype(F32)
        context = context_ref[rows]
        outward += tn(context, upstream_ref[...])
        aligned = made * context.astype(F32)
        for tile in range(tiles):
            last = min(128, width - 128 * tile)
            grad_s[tile, rows, :last] = made[:, 128 * tile : 128 * tile + last]
            context_s[tile, rows, :last] = aligned[:, 128 * tile : 128 * tile + last]
    w_out_ref[...] = outward

    def one_head(head, carry):
        tile = head // 2
        odd, lane, own, first = lanes_of(head, length)
        centre = jnp.sum(jnp.where(own, context_s[tile], 0.0), axis=-1, keepdims=True)
        grad = jnp.where(own, grad_s[tile], 0.0)
        extended_s[...] = with_pieces(grad, lane, first, centre).astype(BF16)
        odd, lane, own, first = lanes_of(head, KTILE)
        query_s[...] = jnp.zeros_like(query_s)
        for start in range(0, length, KTILE):
            rows = slice(start, start + KTILE)
            seen = max(0, start - reach)
            scores = nt(key_ref[head, rows], query_ref[head, seen:])
            probs = jnp.exp(scores)
            pulled = nt(value_ref[head, rows], extended_s[seen:])
            changed = (probs * pulled).astype(BF16)
            grad_value = nn(probs.astype(BF16), extended_s[seen:])
            grad_key = nn(changed, query_ref[head, seen:])
            value_s[tile, rows] = jnp.where(own, grad_value, value_s[tile, rows])
            key_s[tile, rows] = jnp.where(own, grad_key, key_s[tile, rows])
            query_s[seen:] += tn(changed, key_ref[head, rows])
        odd, lane, own, first = lanes_of(head, length)
        query_t[tile] = jnp.where(own, query_s[...] * HEAD_DIM**-0.5, query_t[tile])
        return carry

    lax.fori_loop(0, width // HEAD_DIM, one_head, 0)
    inward = jnp.zeros((length, in_ref.shape[1]), F32)
    for kind, (store, weight_ref) in enumerate(
        ((query_t, w_query_ref), (key_s, w_key_ref), (value_s, w_value_ref))
    ):
        for tile in range(tiles):
            last = min(128, width - 128 * tile)
            made = store[tile, :, :last]
            low = made.astype(BF16)
            begin = kind * width + 128 * tile
            grads_ref[:, begin : begin + last] = low
            inward += nn(low, weight_ref[128 * tile : 128 * tile + last])
            if kind != 1:
                sums_ref[kind : kind + 1, 128 * tile : 128 * tile + last] = jnp.sum(
                    made, axis=0, keepdims=True
                )
    in_ref[...] = inward.astype(BF16)


def attend_backward(core, upstream, out, weights, saved):
    length, width = saved[0].shape
    depth = out.shape[1]
    tall = pltpu.VMEM((pl.cdiv(width, 128), length, 128), F32)
    return call(
        functools.partial(backward_kernel, BLOCK_MOST),
        "attend_backward",
        12,
        [core],
        [*upstream, out, *weights, *saved],
        [
            ((length, 3 * width), BF16, HELD),
            ((3, width), F32),
            ((length, depth), BF16, HELD),
            ((width, depth), F32, HELD),
        ],
        [tall, tall, pltpu.VMEM((length, 128), F32), tall, tall, tall]
        + [pltpu.VMEM((length, 128), BF16)],
    )


def out_kernel(core_ref, mine_ref, other_ref, w_mine_ref, w_other_ref, far_ref, near_ref):
    width = mine_ref.shape[1]
    half = near_ref.shape[0]
    for begin, made_ref in ((1 - core_ref[0], far_ref), (core_ref[0], near_ref)):
        rows = pl.ds(pl.multiple_of(begin * half, half), half)
        made = nn(mine_ref[rows], w_mine_ref[...]) + nn(other_ref[rows], w_other_ref[:width])
        made_ref[...] = made.astype(made_ref.dtype)


def mean(values):
    return jnp.mean(values, axis=-1, keepdims=True)


def norm_one_kernel(
    place_ref, tokens_ref, near_ref, far_ref, bias_ref, gain_ref, shift_ref,
    hidden_ref, low_ref, normed_ref, inverse_ref
):
    half = near_ref.shape[0]
    tokens = tokens_ref[pl.ds(pl.multiple_of(place_ref[0] * half, half), half)].astype(F32)
    values = tokens + near_ref[...] + far_ref[...].astype(F32) + bias_ref[...]
    centre = values - mean(values)
    inverse = lax.rsqrt(mean(centre * centre) + EPS)
    normed = centre * inverse
    hidden = normed * gain_ref[...] + shift_ref[...]
    hidden_ref[...] = hidden
    low_ref[...] = hidden.astype(BF16)
    normed_ref[...] = normed
    inverse_ref[...] = inverse


def gelu_into(up, rows, active_ref, slope_ref):
    phi = 0.5 * (1.0 + lax.erf(up * ROOT_HALF))
    active_ref[rows] = (up * phi).astype(BF16)
    slope_ref[rows] = phi + up * INV_ROOT_TWO_PI * jnp.exp(-0.5 * up * up)


def rise_kernel(mine_ref, other_ref, w_up_ref, bias_ref, active_ref, slope_ref):
    half = mine_ref.shape[0]
    for part, ref in enumerate((mine_ref, other_ref)):
        def tile(step, carry):
            begin = pl.multiple_of(step * TILE, TILE)
            up = nn(ref[pl.ds(begin, TILE)], w_up_ref[...]) + bias_ref[...]
            gelu_into(up, pl.ds(part * half + begin, TILE), active_ref, slope_ref)
            return carry

        lax.fori_loop(0, half // TILE, tile, 0)


def rise_other_kernel(
    order_ref, mine_ref, other_ref, first_ref, second_ref, out_ref, active_ref, slope_ref, joined_ref
):
    rows = first_ref.shape[0]
    for begin, ref in ((order_ref[0], first_ref), (1 - order_ref[0], second_ref)):
        joined_ref[pl.ds(pl.multiple_of(begin * rows, rows), rows)] = ref[...]
    bias = jnp.sum(out_ref[out_ref.shape[0] - 8 :].astype(F32), axis=0, keepdims=True)
    half = mine_ref.shape[0]
    for part, ref in enumerate((mine_ref, other_ref)):
        def tile(step, carry):
            begin = pl.multiple_of(step * TILE, TILE)
            up = nn(ref[pl.ds(begin, TILE)], joined_ref[...]) + bias
            gelu_into(up, pl.ds(part * half + begin, TILE), active_ref, slope_ref)
            return carry

        lax.fori_loop(0, half // TILE, tile, 0)


def fall_kernel(
    order_ref, mine_ref, other_ref, w_down_ref, first_ref, second_ref, near_ref, far_ref, joined_ref
):
    rows = first_ref.shape[0]
    half = near_ref.shape[0]
    for begin, ref in ((order_ref[0], first_ref), (1 - order_ref[0], second_ref)):
        joined_ref[pl.ds(pl.multiple_of(begin * rows, rows), rows)] = ref[...]
    for begin, made_ref in ((half, far_ref), (0, near_ref)):
        part = slice(begin, begin + half)
        made = nn(mine_ref[part], w_down_ref[...]) + nn(other_ref[part], joined_ref[...])
        made_ref[...] = made.astype(made_ref.dtype)


def store_rows(sums_ref, rows):
    sums_ref[...] = jnp.zeros_like(sums_ref)
    for index, row in rows:
        sums_ref[index : index + 1] = row


def total(values):
    return jnp.sum(values, axis=0, keepdims=True)


def norm_two_kernel(
    hidden_ref, near_ref, far_ref, bias_ref, gain_ref, shift_ref, upstream_ref,
    layer_ref, grad_ref, low_ref, sums_ref
):
    values = hidden_ref[...] + near_ref[...] + far_ref[...].astype(F32) + bias_ref[...]
    centre = values - mean(values)
    inverse = lax.rsqrt(mean(centre * centre) + EPS)
    normed = centre * inverse
    layer_ref[...] = (normed * gain_ref[...] + shift_ref[...]).astype(BF16)
    upstream = upstream_ref[...].astype(F32)
    shaped = upstream * gain_ref[...]
    grad = inverse * (shaped - mean(shaped) - normed * mean(shaped * normed))
    grad_ref[...] = grad
    low_ref[...] = grad.astype(BF16)
    store_rows(
        sums_ref, ((3, total(grad)), (4, total(upstream * normed)), (5, total(upstream)))
    )


def norm_one_back_kernel(
    grad_two_ref, near_ref, far_ref, normed_ref, inverse_ref, gain_ref, sums_two_ref, sums_up_ref,
    grad_ref, low_ref, sums_ref
):
    upstream = grad_two_ref[...] + near_ref[...] + far_ref[...].astype(F32)
    normed = normed_ref[...]
    shaped = upstream * gain_ref[...]
    grad = inverse_ref[...] * (shaped - mean(shaped) - normed * mean(shaped * normed))
    grad_ref[...] = grad
    low_ref[...] = grad.astype(BF16)
    store_rows(
        sums_ref,
        (
            (0, total(grad)),
            (1, total(upstream * normed)),
            (2, total(upstream)),
            (3, sums_two_ref[3:4]),
            (4, sums_two_ref[4:5]),
            (5, sums_two_ref[5:6]),
            (6, sums_up_ref[0:1]),
            (7, sums_up_ref[1:2]),
        ),
    )


def down_other_kernel(mine_ref, other_ref, active_ref, sent_ref):
    half = mine_ref.shape[0]
    sent_ref[...] = (
        tn(mine_ref[...], active_ref[:half]) + tn(other_ref[...], active_ref[half:])
    ).astype(BF16)


def ffn_back_kernel(
    mine_ref, other_ref, w_down_ref, joined_down_ref, slope_mine_ref, slope_other_ref,
    w_up_ref, joined_up_ref, low_mine_ref, low_other_ref, near_ref, far_ref, sums_ref
):
    half = mine_ref.shape[0]
    sums_ref[...] = jnp.zeros_like(sums_ref)
    for start, grads_ref, made_ref in ((half, other_ref, far_ref), (0, mine_ref, near_ref)):
        def tile(step, carry):
            begin = pl.multiple_of(step * TILE, TILE)
            rows = pl.ds(start + begin, TILE)
            grads = grads_ref[pl.ds(begin, TILE)]
            made = jnp.zeros((TILE, near_ref.shape[1]), F32)
            for index, (down_ref, slope_ref, up_ref, low_ref) in enumerate(
                (
                    (w_down_ref, slope_mine_ref, w_up_ref, low_mine_ref),
                    (joined_down_ref, slope_other_ref, joined_up_ref, low_other_ref),
                )
            ):
                grad = nt(grads, down_ref[...]) * slope_ref[rows]
                sums_ref[index : index + 1] += total(grad)
                low = grad.astype(BF16)
                low_ref[rows] = low
                made += nt(low, up_ref[...])
            made_ref[pl.ds(begin, TILE)] = made.astype(made_ref.dtype)
            return carry

        lax.fori_loop(0, half // TILE, tile, 0)


def up_grads_kernel(
    odd_ref, mine_ref, other_ref, low_mine_ref, low_other_ref, kept_ref, sent_ref, whole_s
):
    half = mine_ref.shape[0]
    count, share = kept_ref.shape[0] // 2, kept_ref.shape[1]
    odd = odd_ref[0]
    for index, low_ref in enumerate((low_mine_ref, low_other_ref)):
        whole_s[...] = tn(mine_ref[...], low_ref[:half]) + tn(other_ref[...], low_ref[half:])
        for member in range(count):
            for parity, made_ref in ((odd, kept_ref), (1 - odd, sent_ref)):
                begin = pl.multiple_of((2 * member + parity) * share, 8)
                made_ref[index * count + member] = whole_s[pl.ds(begin, share)].astype(
                    made_ref.dtype
                )


def down_pieces_kernel(
    mine_ref, other_ref, active_ref, received_ref, sums_ref, sums_received_ref, pieces_ref
):
    half = mine_ref.shape[0]
    ways, rows = pieces_ref.shape[:2]
    share = rows - 2 * SUMS
    made = tn(mine_ref[...], active_ref[:half]) + tn(other_ref[...], active_ref[half:])
    made = (made + received_ref[...].astype(F32)).astype(BF16)
    sums = sums_ref[...]
    received = sums_received_ref[...]
    row = lax.broadcasted_iota(jnp.int32, sums.shape, 0)
    crossed = jnp.where(row == 6, received[7:8], received)
    sums = sums + crossed
    high = sums.astype(BF16)
    low = (sums - high.astype(F32)).astype(BF16)
    for index in range(ways):
        pieces_ref[index, :share] = made[index * share : (index + 1) * share]
        pieces_ref[index, share : share + SUMS] = high
        pieces_ref[index, share + SUMS :] = low


def qkv_pieces_kernel(
    place_ref, tokens_ref, near_ref, far_ref, sums_near_ref, sums_far_ref, out_near_ref, out_far_ref,
    pieces_ref
):
    ways, rows = pieces_ref.shape[:2]
    share = rows - SUMS
    length, columns = near_ref.shape
    width = out_near_ref.shape[0]
    made = jnp.zeros((tokens_ref.shape[1], columns), F32)
    for chosen, low_ref in ((place_ref[0], near_ref), (1 - place_ref[0], far_ref)):
        tokens = tokens_ref[pl.ds(pl.multiple_of(chosen * length, length), length)]
        made += tn(tokens, low_ref[...])
    made = made.astype(BF16)
    out = (out_near_ref[...] + out_far_ref[...]).T.astype(BF16)
    sums = sums_near_ref[...] + sums_far_ref[...]
    high, middle, low = pieces_of(sums)
    zeros = jnp.zeros((SUMS, columns + width), BF16)
    for index in range(ways):
        pieces_ref[index, share:] = zeros
        for kind in (0, 2):
            lanes = slice(kind * width, (kind + 1) * width)
            for term, rows in enumerate((high, middle, low)):
                pieces_ref[index, share + term : share + term + 1, lanes] = rows[
                    kind : kind + 1
                ].astype(BF16)
        part = slice(index * share, (index + 1) * share)
        pieces_ref[index, :share, :columns] = made[part]
        pieces_ref[index, :share, columns:] = out[part]


def swap_tensor(array, mask):
    ways = lax.axis_size("tensor")
    return lax.ppermute(array, "tensor", [(i, i ^ mask) for i in range(ways)])


def swap_dp(array, mask):
    ways = lax.axis_size("dp")
    return lax.ppermute(array, "dp", [(i, i ^ mask) for i in range(ways)])


def across(array):
    return swap_tensor(array, 2)


def partner(array):
    return swap_tensor(array, 1)


def after(array, *earlier):
    return lax.optimization_barrier((array,) + earlier)[0]


def three_terms(row):
    high = lax.reduce_precision(row, 8, 7)
    middle = lax.reduce_precision(row - high, 8, 7)
    terms = jnp.stack([high, middle, row - high - middle]).astype(BF16)
    return jnp.pad(terms, ((0, 5), (0, 0)))


def scatter_pieces(pieces):
    return jnp.sum(lax.all_to_all(pieces, "dp", 0, 0).astype(F32), axis=0)


def on_device(
    layer_in,
    block_of,
    block_links,
    w_query,
    b_query,
    w_key,
    w_value,
    b_value,
    w_out,
    b_out,
    gain_one,
    shift_one,
    w_up,
    b_up,
    w_down,
    b_down,
    gain_two,
    shift_two,
    grad_out,
):
    length = block_of.shape[1]
    half = length // 2
    place = lax.axis_index("tensor")
    sequence = place // 2
    core = place % 2
    width = w_query.shape[1]
    hidden = w_up.shape[1]
    fall_half = w_down.shape[0] // 2
    rise_half = w_up.shape[0] // 2
    ways = lax.axis_size("dp")
    share = D // ways
    odd = lax.axis_index("dp") % 2

    def scalar(value):
        return jnp.full((1,), value, jnp.int32)

    def row(vector):
        return vector.reshape(1, -1)

    up_first = across(lax.dynamic_slice_in_dim(w_up, odd * rise_half, rise_half, 0))
    down_sent = lax.dynamic_slice_in_dim(w_down, odd * fall_half, fall_half, 0)
    out_sent = jnp.concatenate([w_out, three_terms(b_up)], axis=0)

    weights = (w_query.T, w_key.T, w_value.T)
    inputs = weights + (row(b_query), row(b_value))
    near_place, far_place = scalar(sequence), scalar(1 - sequence)
    saved_far = attend_forward(
        after(far_place, down_sent, out_sent), layer_in, inputs, block_of, block_links
    )
    context_other = across(saved_far[0])
    out_received = across(after(out_sent, saved_far[0]))
    down_first = across(after(down_sent, saved_far[0]))
    saved_near = attend_forward(
        after(near_place, saved_far[0]), layer_in, inputs, block_of, block_links
    )
    context_mine = after(saved_near[0], up_first)
    up_second = swap_dp(up_first, 1)

    here = scalar(core)
    far, near = call(
        out_kernel,
        "out",
        2,
        [here],
        [context_mine, context_other, w_out, out_received],
        [((half, D), BF16), ((half, D), F32)],
    )
    hidden_one, hidden_mine, normed_one, inverse_one = call(
        norm_one_kernel,
        "norm_one",
        1,
        [scalar(place)],
        [layer_in, near, partner(far), row(b_out), row(gain_one), row(shift_one)],
        [((half, D), F32), ((half, D), BF16), ((half, D), F32), ((half, 1), F32)],
    )
    hidden_partner = partner(hidden_mine)
    active_mine, slope_mine = call(
        rise_kernel,
        "rise_mine",
        2.6,
        [],
        [hidden_mine, hidden_partner, w_up, row(b_up)],
        [((length, hidden), BF16), ((length, hidden), F32)],
    )
    down_first = after(down_first, active_mine)
    down_second = swap_dp(down_first, 1)
    order = scalar(odd)
    active_other, slope_other, up_other = call(
        rise_other_kernel,
        "rise_other",
        4,
        [order],
        [hidden_mine, hidden_partner, up_first, after(up_second, active_mine), out_received],
        [((length, hidden), BF16), ((length, hidden), F32), (w_up.shape, BF16)],
    )
    near, far, down_other = call(
        fall_kernel,
        "fall",
        2.7,
        [order],
        [active_mine, active_other, w_down, down_first, after(down_second, active_other)],
        [((half, D), F32), ((half, D), BF16), (w_down.shape, BF16)],
    )
    layer_out, grad_two, ffn_mine, sums_two = call(
        norm_two_kernel,
        "norm_two",
        1.5,
        [],
        [hidden_one, near, partner(far), row(b_down), row(gain_two), row(shift_two), grad_out],
        [((half, D), BF16), ((half, D), F32), ((half, D), BF16), ((SUMS, D), F32)],
    )
    ffn_partner = partner(ffn_mine)

    (down_sent,) = call(
        down_other_kernel,
        "down_other",
        1.4,
        [],
        [ffn_mine, ffn_partner, active_other],
        [((D, hidden), BF16, HELD)],
    )
    down_received = across(down_sent)
    low_mine, low_other, near, far, sums_up = call(
        ffn_back_kernel,
        "ffn_back",
        7,
        [],
        [ffn_mine, after(ffn_partner, down_sent), w_down, down_other]
        + [slope_mine, slope_other, w_up, up_other],
        [((length, hidden), BF16)] * 2
        + [((half, D), F32), ((half, D), BF16), ((SUMS, hidden), F32)],
    )
    grad_one, one_mine, sums = call(
        norm_one_back_kernel,
        "norm_one_back",
        1.1,
        [],
        [grad_two, near, partner(far), normed_one, inverse_one, row(gain_one), sums_two, sums_up],
        [((half, D), F32, HELD), ((half, D), BF16, HELD), ((SUMS, D), F32)],
    )
    one_partner = partner(one_mine)
    sums_partner = partner(sums)
    rows = lax.broadcasted_iota(jnp.int32, sums.shape, 0)
    sums = sums + jnp.where(rows < 6, sums_partner, 0.0)
    sums_received = across(sums)
    one_across = across(after(one_mine, sums))

    up_kept, up_sent = call(
        up_grads_kernel,
        "up_grads",
        3,
        [order],
        [hidden_mine, hidden_partner, after(low_mine, one_mine), low_other],
        [((ways, share, hidden), F32, HELD), ((ways, share, hidden), BF16, HELD)],
        [pltpu.VMEM((D, hidden), F32)],
    )
    up_received = swap_dp(up_sent, 1)
    low_near, columns_near, in_near, out_near = attend_backward(
        here, (one_mine, after(one_partner, up_sent)), w_out, weights, saved_near
    )

    down_received = after(down_received, low_near)
    (down_pieces,) = call(
        down_pieces_kernel,
        "down_pieces",
        2.6,
        [],
        [ffn_mine, ffn_partner, active_mine, down_received, sums, sums_received],
        [((ways, share + 2 * SUMS, hidden), BF16, HELD)],
    )
    down_sums = scatter_pieces(down_pieces)
    grad_w_down = down_sums[:share].T
    sums = down_sums[share : share + SUMS] + down_sums[share + SUMS :]

    one_across = after(one_across, down_pieces)
    across_partner = partner(one_across)
    up_received = after(up_received, down_pieces)
    up_terms = up_kept + up_received.astype(F32)
    up_mine = up_terms[: ways // 2]
    up_other = up_terms[ways // 2 :].astype(BF16)
    up_across = across(up_other)

    low_far, columns_far, in_far, out_far = attend_backward(
        here, (one_across, after(across_partner, up_other)), w_out, weights, saved_far
    )
    (pieces,) = call(
        qkv_pieces_kernel,
        "qkv_pieces",
        3.7,
        [near_place],
        [layer_in, low_near, low_far, columns_near, columns_far, out_near, out_far],
        [((ways, share + SUMS, 4 * width), BF16, HELD)],
    )
    qkv = scatter_pieces(pieces)
    bias_sums = jnp.sum(qkv[share:], axis=0)
    qkv = qkv[:share]
    grad_w_out = qkv[:, 3 * width :].T

    def core_parts(terms):
        parts = terms.reshape(2, half, D)
        kept = lax.dynamic_index_in_dim(parts, core, 0, keepdims=False)
        sent = lax.dynamic_index_in_dim(parts, 1 - core, 0, keepdims=False)
        return kept.astype(F32), partner(sent).astype(F32)

    far_kept, far_received = core_parts(in_far)
    in_other = across((far_kept + far_received).astype(BF16))
    near_kept, near_received = core_parts(in_near)

    up_across = after(up_across, low_far)
    up_pieces = (up_mine + up_across.astype(F32)).astype(BF16)
    member = lax.axis_index("dp") // 2
    grad_w_up = lax.dynamic_index_in_dim(up_pieces, member, 0, keepdims=False).astype(F32)
    for step in range(1, ways // 2):
        piece = lax.dynamic_index_in_dim(up_pieces, member ^ step, 0, keepdims=False)
        grad_w_up = grad_w_up + swap_dp(piece, 2 * step).astype(F32)

    grad_in = grad_one + near_kept + near_received + in_other.astype(F32)

    return (
        layer_out,
        grad_in,
        qkv[:, :width],
        bias_sums[:width],
        qkv[:, width : 2 * width],
        qkv[:, 2 * width : 3 * width],
        bias_sums[2 * width : 3 * width],
        grad_w_out,
        sums[0],
        sums[1],
        sums[2],
        grad_w_up,
        sums[6:7].reshape(-1),
        grad_w_down,
        sums[3],
        sums[4],
        sums[5],
    )


def solution(mesh):
    in_specs = (
        P("dp", None),
        P("dp", None),
        P("dp", None, None),
        P(None, "tensor"),
        P("tensor"),
        P(None, "tensor"),
        P(None, "tensor"),
        P("tensor"),
        P("tensor", None),
        P(),
        P(),
        P(),
        P(None, "tensor"),
        P("tensor"),
        P("tensor", None),
        P(),
        P(),
        P(),
        P(("dp", "tensor"), None),
    )
    out_specs = (
        P(("dp", "tensor"), None),
        P(("dp", "tensor"), None),
        P("dp", "tensor"),
        P("tensor"),
        P("dp", "tensor"),
        P("dp", "tensor"),
        P("tensor"),
        P("tensor", "dp"),
        P(),
        P(),
        P(),
        P("dp", "tensor"),
        P("tensor"),
        P("tensor", "dp"),
        P(),
        P(),
        P(),
    )
    return jax.shard_map(
        on_device, mesh=mesh, in_specs=in_specs, out_specs=out_specs, check_vma=False
    )
```

```python
import functools

import jax
import jax.numpy as jnp
from jax import lax
from jax.experimental import pallas as pl
from jax.experimental.pallas import tpu as pltpu
from jax.sharding import PartitionSpec as P

D = 768
HEADS = 12
HEAD_DIM = D // HEADS

EPS = 1e-06
NEG = -1e30
ROOT_HALF = 0.7071067811865476
INV_ROOT_TWO_PI = 0.3989422804014327
BF16 = jnp.bfloat16
F32 = jnp.float32
BLOCK_MOST = 256
EXTRA = 8
COST_FLOPS = 50_000_000
COST_BYTES = 100_000
QTILE = 256
KTILE = 256
TILE = 256
SUMS = 8
HELD = True


def nn(left, right):
    return jnp.dot(left, right, preferred_element_type=F32)


def tn(left, right):
    return lax.dot_general(left, right, (((0,), (0,)), ((), ())), preferred_element_type=F32)


def nt(left, right):
    return lax.dot_general(left, right, (((1,), (1,)), ((), ())), preferred_element_type=F32)


VMEM = pl.BlockSpec(memory_space=pltpu.VMEM)
SMEM = pl.BlockSpec(memory_space=pltpu.SMEM)


def call(kernel, name, cost, scalars, arrays, outs, scratch=(), outside=()):
    arrays = [
        pltpu.with_memory_space_constraint(array, pltpu.HBM if index in outside else pltpu.VMEM)
        for index, array in enumerate(arrays)
    ]
    return pl.pallas_call(
        kernel,
        out_shape=tuple(
            pltpu.HBM(*out[:2]) if len(out) > 2 else pltpu.VMEM(*out) for out in outs
        ),
        in_specs=[SMEM] * len(scalars) + [VMEM] * len(arrays),
        out_specs=(VMEM,) * len(outs),
        scratch_shapes=list(scratch),
        cost_estimate=pl.CostEstimate(
            flops=int(cost * COST_FLOPS), bytes_accessed=int(cost * COST_BYTES), transcendentals=0
        ),
        name=name,
        compiler_params=pltpu.CompilerParams(
            vmem_limit_bytes=20 * 2**20
        ),
    )(*scalars, *arrays)


def pieces_of(column):
    high = column.astype(BF16).astype(F32)
    middle = (column - high).astype(BF16).astype(F32)
    return high, middle, column - high - middle


def with_pieces(base, lane, first, column):
    high, middle, low = pieces_of(column)
    base = jnp.where(lane == first, -high, base)
    base = jnp.where(lane == first + 1, -middle, base)
    return jnp.where(lane == first + 2, -low, base)


def lanes_of(head, rows):
    odd = lax.rem(head, 2)
    lane = lax.broadcasted_iota(jnp.int32, (rows, 2 * HEAD_DIM), 1)
    own = (lane >= HEAD_DIM * odd) & (lane < HEAD_DIM * (odd + 1))
    return odd, lane, own, HEAD_DIM * (1 - odd) + EXTRA


def forward_kernel(
    reach, place_ref, tokens_ref, w_query_ref, w_key_ref, w_value_ref, b_query_ref, b_value_ref,
    blocks_ref, links_ref, context_ref, query_ref, key_ref, value_ref,
    query_s, key_s, value_s, context_s, table_s, marks_s
):
    length = blocks_ref.shape[1]
    width = w_query_ref.shape[0]
    tiles = pl.cdiv(width, 128)
    chosen = place_ref[0]
    tokens = tokens_ref[pl.ds(pl.multiple_of(chosen * length, length), length)]
    for store, made in (
        (query_s, (nt(tokens, w_query_ref[...]) + b_query_ref[...]) * HEAD_DIM**-0.5),
        (key_s, nt(tokens, w_key_ref[...])),
        (value_s, nt(tokens, w_value_ref[...]) + b_value_ref[...]),
    ):
        for tile in range(tiles):
            last = min(128, width - 128 * tile)
            store[tile, :, :last] = made[:, 128 * tile : 128 * tile + last]

    row = blocks_ref[pl.ds(chosen, 1)].astype(F32)
    column = jnp.broadcast_to(row, (8, length)).T[:, :1]
    lane = lax.broadcasted_iota(jnp.int32, (length, 128), 1)
    onehot = jnp.where(column == lane.astype(F32), 1.0, 0.0)
    links = links_ref[chosen]
    count = links.shape[0]
    above = lax.broadcasted_iota(jnp.int32, (count, count), 0)
    below = lax.broadcasted_iota(jnp.int32, (count, count), 1)
    seen = (above == below) | ((above > below) & (links == 1))
    pairs = jnp.where(seen, 0.0, NEG).astype(BF16)
    sees = nn(onehot[:, :count].astype(BF16), pairs)
    table_s[...] = jnp.zeros_like(table_s)
    table_s[1, :, :count] = sees
    table_s[0, :, HEAD_DIM : HEAD_DIM + count] = sees
    ones = jnp.where((lane >= EXTRA) & (lane < EXTRA + 3), 1.0, onehot)
    marks_s[1] = ones
    marks_s[0] = pltpu.roll(ones, HEAD_DIM, 1)

    def one_head(head, carry):
        tile = head // 2
        odd, lane, own, first = lanes_of(head, length)
        marks = marks_s[odd]
        key_ref[head] = jnp.where(own, key_s[tile], marks).astype(BF16)
        ones = jnp.where((lane >= first) & (lane < first + 3), 1.0, 0.0)
        value_ref[head] = jnp.where(own, value_s[tile], ones).astype(BF16)
        odd, lane, own, first = lanes_of(head, QTILE)
        for start in range(0, length, QTILE):
            rows = slice(start, start + QTILE)
            seen = min(length, start + QTILE + reach)
            query = jnp.where(own, query_s[tile, rows], table_s[odd, rows])
            scores = nt(query.astype(BF16), key_ref[head, :seen])
            highest = jnp.max(scores, axis=-1, keepdims=True)
            weights = jnp.exp(scores - highest).astype(BF16)
            mixed = nn(weights, value_ref[head, :seen])
            total = jnp.sum(jnp.where(lane == first, mixed, 0.0), axis=-1, keepdims=True)
            context_s[tile, rows] = jnp.where(own, mixed * (1.0 / total), context_s[tile, rows])
            query_ref[head, rows] = with_pieces(
                query, lane, first, highest + jnp.log(total)
            ).astype(BF16)
        return carry

    lax.fori_loop(0, width // HEAD_DIM, one_head, 0)
    for tile in range(tiles):
        last = min(128, width - 128 * tile)
        context_ref[:, 128 * tile : 128 * tile + last] = context_s[tile, :, :last].astype(BF16)


def attend_forward(place, layer_in, weights, block_of, block_links):
    length = block_of.shape[1]
    width = weights[0].shape[0]
    heads = width // HEAD_DIM
    tiles = pl.cdiv(width, 128)
    big = ((heads, length, 128), BF16, HELD)
    tall = pltpu.VMEM((tiles, length, 128), F32)
    both = pltpu.VMEM((2, length, 128), F32)
    return call(
        functools.partial(forward_kernel, BLOCK_MOST),
        "attend_forward",
        8,
        [place],
        [layer_in, *weights, block_of, block_links],
        [((length, width), BF16), big, big, big],
        [tall] * 4 + [both] * 2,
        outside=range(1, 8),
    )


def backward_kernel(
    reach, core_ref, first_ref, second_ref, out_ref, w_query_ref, w_key_ref, w_value_ref,
    context_ref, query_ref, key_ref, value_ref, grads_ref, sums_ref, kept_ref, sent_ref, w_out_ref,
    grad_s, context_s, query_s, query_t, key_s, value_s, extended_s
):
    length, width = context_ref.shape
    half = length // 2
    tiles = pl.cdiv(width, 128)
    outward = jnp.zeros((width, out_ref.shape[1]), F32)
    for part, upstream_ref in enumerate((first_ref, second_ref)):
        begin = pl.multiple_of(lax.rem(core_ref[0] + part, 2) * half, half)
        rows = pl.ds(begin, half)
        upstream = upstream_ref[:half]
        made = nt(upstream, out_ref[...]).astype(BF16).astype(F32)
        context = context_ref[rows]
        outward += tn(context, upstream)
        aligned = made * context.astype(F32)
        for tile in range(tiles):
            last = min(128, width - 128 * tile)
            grad_s[tile, rows, :last] = made[:, 128 * tile : 128 * tile + last]
            context_s[tile, rows, :last] = aligned[:, 128 * tile : 128 * tile + last]
    w_out_ref[...] = outward

    def one_head(head, carry):
        tile = head // 2
        odd, lane, own, first = lanes_of(head, length)
        centre = jnp.sum(jnp.where(own, context_s[tile], 0.0), axis=-1, keepdims=True)
        grad = jnp.where(own, grad_s[tile], 0.0)
        extended_s[...] = with_pieces(grad, lane, first, centre).astype(BF16)
        odd, lane, own, first = lanes_of(head, KTILE)
        query_s[...] = jnp.zeros_like(query_s)
        for start in range(0, length, KTILE):
            rows = slice(start, start + KTILE)
            seen = max(0, start - reach)
            scores = nt(key_ref[head, rows], query_ref[head, seen:])
            probs = jnp.exp(scores)
            pulled = nt(value_ref[head, rows], extended_s[seen:])
            changed = (probs * pulled).astype(BF16)
            grad_value = nn(probs.astype(BF16), extended_s[seen:])
            grad_key = nn(changed, query_ref[head, seen:])
            value_s[tile, rows] = jnp.where(own, grad_value, value_s[tile, rows])
            key_s[tile, rows] = jnp.where(own, grad_key, key_s[tile, rows])
            query_s[seen:] += tn(changed, key_ref[head, rows])
        odd, lane, own, first = lanes_of(head, length)
        query_t[tile] = jnp.where(own, query_s[...] * HEAD_DIM**-0.5, query_t[tile])
        return carry

    lax.fori_loop(0, width // HEAD_DIM, one_head, 0)
    for kind, store in enumerate((query_t, key_s, value_s)):
        for tile in range(tiles):
            last = min(128, width - 128 * tile)
            made = store[tile, :, :last]
            begin = kind * width + 128 * tile
            grads_ref[:, begin : begin + last] = made.astype(BF16)
            if kind != 1:
                sums_ref[kind : kind + 1, 128 * tile : 128 * tile + last] = jnp.sum(
                    made, axis=0, keepdims=True
                )
    for begin, made_ref in ((1 - core_ref[0], sent_ref), (core_ref[0], kept_ref)):
        rows = pl.ds(pl.multiple_of(begin * half, half), half)
        inward = jnp.zeros(made_ref.shape, F32)
        for kind, weight_ref in enumerate((w_query_ref, w_key_ref, w_value_ref)):
            inward += nn(grads_ref[rows, kind * width : (kind + 1) * width], weight_ref[...])
        made_ref[...] = inward.astype(made_ref.dtype)


def attend_backward(core, upstream, out, weights, saved):
    length, width = saved[0].shape
    depth = out.shape[1]
    tall = pltpu.VMEM((pl.cdiv(width, 128), length, 128), F32)
    return call(
        functools.partial(backward_kernel, BLOCK_MOST),
        "attend_backward",
        12,
        [core],
        [*upstream, out, *weights, *saved],
        [
            ((length, 3 * width), BF16, HELD),
            ((3, width), F32),
            ((length // 2, depth), F32, HELD),
            ((length // 2, depth), BF16),
            ((width, depth), F32, HELD),
        ],
        [tall, tall, pltpu.VMEM((length, 128), F32), tall, tall, tall]
        + [pltpu.VMEM((length, 128), BF16)],
    )


def out_kernel(core_ref, mine_ref, other_ref, w_mine_ref, w_other_ref, far_ref, near_ref):
    width = mine_ref.shape[1]
    half = near_ref.shape[0]
    for begin, made_ref in ((1 - core_ref[0], far_ref), (core_ref[0], near_ref)):
        rows = pl.ds(pl.multiple_of(begin * half, half), half)
        made = nn(mine_ref[rows], w_mine_ref[...]) + nn(other_ref[rows], w_other_ref[:width])
        made_ref[...] = made.astype(made_ref.dtype)


def mean(values):
    return jnp.mean(values, axis=-1, keepdims=True)


def norm_one_kernel(
    place_ref, tokens_ref, near_ref, far_ref, bias_ref, gain_ref, shift_ref,
    hidden_ref, low_ref, held_ref, normed_ref, inverse_ref
):
    half = near_ref.shape[0]
    tokens = tokens_ref[pl.ds(pl.multiple_of(place_ref[0] * half, half), half)].astype(F32)
    values = tokens + near_ref[...] + far_ref[...].astype(F32) + bias_ref[...]
    centre = values - mean(values)
    inverse = lax.rsqrt(mean(centre * centre) + EPS)
    normed = centre * inverse
    hidden = normed * gain_ref[...] + shift_ref[...]
    hidden_ref[...] = hidden
    low_ref[...] = hidden.astype(BF16)
    held_ref[...] = hidden.astype(BF16)
    normed_ref[...] = normed
    inverse_ref[...] = inverse


def gelu_into(up, rows, active_ref, held_ref, slope_ref):
    phi = 0.5 * (1.0 + lax.erf(up * ROOT_HALF))
    active = (up * phi).astype(BF16)
    active_ref[rows] = active
    held_ref[rows] = active
    slope_ref[rows] = phi + up * INV_ROOT_TWO_PI * jnp.exp(-0.5 * up * up)


def rise_kernel(
    mine_ref, other_ref, w_up_ref, bias_ref, active_ref, held_ref, slope_ref, other_held_ref
):
    half = mine_ref.shape[0]
    other_held_ref[...] = other_ref[...]
    for part, ref in enumerate((mine_ref, other_ref)):
        def tile(step, carry):
            begin = pl.multiple_of(step * TILE, TILE)
            up = nn(ref[pl.ds(begin, TILE)], w_up_ref[...]) + bias_ref[...]
            gelu_into(up, pl.ds(part * half + begin, TILE), active_ref, held_ref, slope_ref)
            return carry

        lax.fori_loop(0, half // TILE, tile, 0)


def join(order_ref, refs, joined_ref):
    rows = refs[0].shape[0]
    for step, ref in enumerate(refs):
        begin = jnp.bitwise_xor(order_ref[0], step) * rows
        joined_ref[pl.ds(pl.multiple_of(begin, rows), rows)] = ref[...]


def rise_other_kernel(
    order_ref, mine_ref, other_ref, *refs
):
    *pieces, out_ref, active_ref, held_ref, slope_ref, joined_ref = refs
    join(order_ref, pieces, joined_ref)
    bias = jnp.sum(out_ref[out_ref.shape[0] - 8 :].astype(F32), axis=0, keepdims=True)
    half = mine_ref.shape[0]
    for part, ref in enumerate((mine_ref, other_ref)):
        def tile(step, carry):
            begin = pl.multiple_of(step * TILE, TILE)
            up = nn(ref[pl.ds(begin, TILE)], joined_ref[...]) + bias
            gelu_into(up, pl.ds(part * half + begin, TILE), active_ref, held_ref, slope_ref)
            return carry

        lax.fori_loop(0, half // TILE, tile, 0)


def fall_kernel(order_ref, mine_ref, other_ref, w_down_ref, *refs):
    *pieces, near_ref, far_ref, joined_ref = refs
    half = near_ref.shape[0]
    join(order_ref, pieces, joined_ref)
    for begin, made_ref in ((half, far_ref), (0, near_ref)):
        part = slice(begin, begin + half)
        made = nn(mine_ref[part], w_down_ref[...]) + nn(other_ref[part], joined_ref[...])
        made_ref[...] = made.astype(made_ref.dtype)


def store_rows(sums_ref, rows):
    sums_ref[...] = jnp.zeros_like(sums_ref)
    for index, row in rows:
        sums_ref[index : index + 1] = row


def total(values):
    return jnp.sum(values, axis=0, keepdims=True)


def norm_two_kernel(
    hidden_ref, near_ref, far_ref, bias_ref, gain_ref, shift_ref, upstream_ref,
    layer_ref, grad_ref, low_ref, held_ref, sums_ref
):
    values = hidden_ref[...] + near_ref[...] + far_ref[...].astype(F32) + bias_ref[...]
    centre = values - mean(values)
    inverse = lax.rsqrt(mean(centre * centre) + EPS)
    normed = centre * inverse
    layer_ref[...] = (normed * gain_ref[...] + shift_ref[...]).astype(BF16)
    upstream = upstream_ref[...].astype(F32)
    shaped = upstream * gain_ref[...]
    grad = inverse * (shaped - mean(shaped) - normed * mean(shaped * normed))
    grad_ref[...] = grad
    low_ref[...] = grad.astype(BF16)
    held_ref[...] = grad.astype(BF16)
    store_rows(
        sums_ref, ((3, total(grad)), (4, total(upstream * normed)), (5, total(upstream)))
    )


def norm_one_back_kernel(
    grad_two_ref, near_ref, far_ref, normed_ref, inverse_ref, gain_ref, sums_two_ref, sums_up_ref,
    grad_ref, low_ref, sums_ref
):
    half = near_ref.shape[0]
    upstream = grad_two_ref[...] + near_ref[...] + far_ref[...].astype(F32)
    normed = normed_ref[...]
    shaped = upstream * gain_ref[...]
    grad = inverse_ref[...] * (shaped - mean(shaped) - normed * mean(shaped * normed))
    grad_ref[...] = grad
    low_ref[:half] = grad.astype(BF16)
    store_rows(
        sums_ref,
        (
            (0, total(grad)),
            (1, total(upstream * normed)),
            (2, total(upstream)),
            (3, sums_two_ref[3:4]),
            (4, sums_two_ref[4:5]),
            (5, sums_two_ref[5:6]),
            (6, sums_up_ref[0:1]),
            (7, sums_up_ref[1:2]),
        ),
    )
    for term, rows in enumerate(pieces_of(sums_ref[...])):
        low_ref[half + term * SUMS : half + (term + 1) * SUMS] = rows.astype(BF16)


def ffn_back_kernel(
    mine_ref, other_ref, w_down_ref, joined_down_ref, slope_mine_ref, slope_other_ref,
    w_up_ref, joined_up_ref, low_mine_ref, low_other_ref, near_ref, far_ref, sums_ref, held_ref
):
    half = mine_ref.shape[0]
    held_ref[...] = other_ref[...]
    sums_ref[...] = jnp.zeros_like(sums_ref)
    for start, grads_ref, made_ref in ((half, other_ref, far_ref), (0, mine_ref, near_ref)):
        def tile(step, carry):
            begin = pl.multiple_of(step * TILE, TILE)
            rows = pl.ds(start + begin, TILE)
            grads = grads_ref[pl.ds(begin, TILE)]
            made = jnp.zeros((TILE, near_ref.shape[1]), F32)
            for index, (down_ref, slope_ref, up_ref, low_ref) in enumerate(
                (
                    (w_down_ref, slope_mine_ref, w_up_ref, low_mine_ref),
                    (joined_down_ref, slope_other_ref, joined_up_ref, low_other_ref),
                )
            ):
                grad = nt(grads, down_ref[...]) * slope_ref[rows]
                sums_ref[index : index + 1] += total(grad)
                low = grad.astype(BF16)
                low_ref[rows] = low
                made += nt(low, up_ref[...])
            made_ref[pl.ds(begin, TILE)] = made.astype(made_ref.dtype)
            return carry

        lax.fori_loop(0, half // TILE, tile, 0)


def weight_grads_kernel(
    bit, place_ref, left_mine_ref, left_other_ref, mine_ref, other_ref,
    kept_mine_ref, kept_other_ref, sent_mine_ref, sent_other_ref, whole_s
):
    half = left_mine_ref.shape[0]
    count, share = kept_mine_ref.shape[:2]
    own = place_ref[0]
    for right_ref, kept_ref, sent_ref in (
        (mine_ref, kept_mine_ref, sent_mine_ref), (other_ref, kept_other_ref, sent_other_ref)
    ):
        whole_s[...] = tn(left_mine_ref[...], right_ref[:half]) + tn(
            left_other_ref[...], right_ref[half:]
        )
        for member in range(count):
            base = member % bit + member // bit * 2 * bit
            for parity, made_ref in ((own, kept_ref), (1 - own, sent_ref)):
                begin = pl.multiple_of((base + bit * parity) * share, 8)
                made_ref[member] = whole_s[pl.ds(begin, share)].astype(made_ref.dtype)


def combine_kernel(up_ref, up_received_ref, down_ref, down_received_ref, made_ref):
    count = up_ref.shape[0]
    for kind, (kept_ref, received_ref) in enumerate(
        ((up_ref, up_received_ref), (down_ref, down_received_ref))
    ):
        for member in range(count):
            made = kept_ref[member] + received_ref[member].astype(F32)
            made_ref[kind * count + member] = made.astype(BF16)


def split_kernel(
    members_ref, up_ref, up_received_ref, down_ref, down_received_ref, across_ref, *refs
):
    count = up_ref.shape[0]
    for kind, (kept_ref, received_ref) in enumerate(
        ((up_ref, up_received_ref), (down_ref, down_received_ref))
    ):
        for step in range(count):
            index = jnp.bitwise_xor(members_ref[kind], step)
            made = kept_ref[index] + received_ref[index].astype(F32)
            made += across_ref[kind * count + index].astype(F32)
            refs[kind * count + step][...] = made.astype(BF16)


def three_sums(values, first):
    return (
        values[first : first + SUMS]
        + values[first + SUMS : first + 2 * SUMS]
        + values[first + 2 * SUMS : first + 3 * SUMS]
    )


def qkv_split_kernel(members_ref, kept_ref, received_ref, *refs):
    count, rows = kept_ref.shape[:2]
    share = rows - 3 * SUMS
    for step in range(count):
        index = jnp.bitwise_xor(members_ref[0], step)
        made_ref = refs[step]
        made = kept_ref[index] + received_ref[index].astype(F32)
        made_ref[:share] = made[:share].astype(BF16)
        for term, part in enumerate(pieces_of(three_sums(made, share))):
            made_ref[share + term * SUMS : share + (term + 1) * SUMS] = part.astype(BF16)


def added(refs):
    made = refs[0][...].astype(F32)
    for ref in refs[1:]:
        made += ref[...].astype(F32)
    return made


def finish_kernel(*refs):
    *terms, query_ref, key_ref, value_ref, out_ref, bias_ref, sums_ref, up_ref, down_ref = refs
    count = len(terms) // 3
    share, width = query_ref.shape
    up_ref[...] = added(terms[:count])
    down_ref[...] = added(terms[count : 2 * count])
    made = added(terms[2 * count :])
    query_ref[...] = made[:share, :width]
    key_ref[...] = made[:share, width : 2 * width]
    value_ref[...] = made[:share, 2 * width : 3 * width]
    out_ref[...] = made[:share, 3 * width :].T
    sums = three_sums(made, share)
    sums_ref[...] = sums
    bias_ref[...] = sums[7:8]


def sum_kernel(*refs):
    *terms, made_ref = refs
    made = terms[0][...].astype(F32)
    for term in terms[1:]:
        made += term[...].astype(F32)
    made_ref[...] = made.astype(made_ref.dtype)


def qkv_pieces_kernel(
    place_ref, parity_ref, tokens_ref, near_ref, far_ref, sums_near_ref, sums_far_ref,
    out_near_ref, out_far_ref, norm_sums_ref, mine_ref, partner_ref, across_ref, diagonal_ref,
    kept_ref, sent_ref, whole_s
):
    count, rows = kept_ref.shape[:2]
    share = rows - 3 * SUMS
    length, columns = near_ref.shape
    width = out_near_ref.shape[0]
    half = mine_ref.shape[0] - 3 * SUMS
    made = jnp.zeros((tokens_ref.shape[1], columns), F32)
    for chosen, low_ref in ((place_ref[0], near_ref), (1 - place_ref[0], far_ref)):
        tokens = tokens_ref[pl.ds(pl.multiple_of(chosen * length, length), length)]
        made += tn(tokens, low_ref[...])
    whole_s[:, :columns] = made
    whole_s[:, columns:] = (out_near_ref[...] + out_far_ref[...]).T

    def sums_of(ref):
        terms = [ref[half + k * SUMS : half + (k + 1) * SUMS].astype(F32) for k in range(3)]
        return terms[0] + terms[1] + terms[2]

    across = sums_of(across_ref)
    sums = norm_sums_ref[...]
    row = lax.broadcasted_iota(jnp.int32, sums.shape, 0)
    bias = sums_near_ref[...] + sums_far_ref[...]
    lane = lax.broadcasted_iota(jnp.int32, (1, columns + width), 1)
    biases = jnp.concatenate(
        [bias[0:1], bias[1:2], bias[2:3], jnp.zeros((1, width), F32)], axis=1
    )
    biases = jnp.where((lane < width) | (lane >= 2 * width), biases, 0.0)
    sums = jnp.where(
        row < 6,
        sums + sums_of(partner_ref) + across + sums_of(diagonal_ref),
        jnp.where(row == 6, sums + across[7:8], biases),
    )
    terms = pieces_of(sums)
    for member in range(count):
        for parity, made_ref in ((parity_ref[0], kept_ref), (1 - parity_ref[0], sent_ref)):
            begin = pl.multiple_of((2 * member + parity) * share, 8)
            made_ref[member, :share] = whole_s[pl.ds(begin, share)].astype(made_ref.dtype)
            for k, term in enumerate(terms):
                made_ref[member, share + k * SUMS : share + (k + 1) * SUMS] = term.astype(
                    made_ref.dtype
                )


def swap_tensor(array, mask):
    ways = lax.axis_size("tensor")
    return lax.ppermute(array, "tensor", [(i, i ^ mask) for i in range(ways)])


def swap_dp(array, mask):
    ways = lax.axis_size("dp")
    return lax.ppermute(array, "dp", [(i, i ^ mask) for i in range(ways)])


def across(array):
    return swap_tensor(array, 2)


def partner(array):
    return swap_tensor(array, 1)


def after(array, *earlier):
    return lax.optimization_barrier((array,) + earlier)[0]


def three_terms(row):
    high = lax.reduce_precision(row, 8, 7)
    middle = lax.reduce_precision(row - high, 8, 7)
    terms = jnp.stack([high, middle, row - high - middle]).astype(BF16)
    return jnp.pad(terms, ((0, 5), (0, 0)))


def on_device(
    layer_in,
    block_of,
    block_links,
    w_query,
    b_query,
    w_key,
    w_value,
    b_value,
    w_out,
    b_out,
    gain_one,
    shift_one,
    w_up,
    b_up,
    w_down,
    b_down,
    gain_two,
    shift_two,
    grad_out,
):
    length = block_of.shape[1]
    half = length // 2
    place = lax.axis_index("tensor")
    sequence = place // 2
    core = place % 2
    width = w_query.shape[1]
    hidden = w_up.shape[1]
    ways = lax.axis_size("dp")
    share = D // ways
    group = lax.axis_index("dp")

    def scalar(value):
        return jnp.full((1,), value, jnp.int32)

    def row(vector):
        return vector.reshape(1, -1)

    def part_of(array, parts):
        rows = array.shape[0] // parts
        return lax.dynamic_slice_in_dim(array, group % parts * rows, rows, 0)

    def spread(part, parts):
        return [swap_dp(part, step) for step in range(1, parts)]

    out_received = across(jnp.concatenate([w_out, three_terms(b_up)], axis=0))
    up_part = across(part_of(w_up, 4))
    down_part = across(part_of(w_down, 4))

    weights = (w_query.T, w_key.T, w_value.T)
    inputs = weights + (row(b_query), row(b_value))
    near_place, far_place = scalar(sequence), scalar(1 - sequence)
    up_parts = spread(up_part, 4)
    saved_far = attend_forward(
        after(far_place, up_part), layer_in, inputs, block_of, block_links
    )
    context_other = across(saved_far[0])
    down_parts = spread(down_part, 4)
    saved_near = attend_forward(
        after(near_place, saved_far[0], down_part, *up_parts), layer_in, inputs, block_of, block_links
    )

    here = scalar(core)
    far, near = call(
        out_kernel,
        "out",
        2,
        [here],
        [after(saved_near[0], *down_parts), context_other, w_out, out_received],
        [((half, D), BF16), ((half, D), F32)],
    )
    hidden_one, hidden_mine, hidden_held, normed_one, inverse_one = call(
        norm_one_kernel,
        "norm_one",
        1,
        [scalar(place)],
        [layer_in, near, partner(far), row(b_out), row(gain_one), row(shift_one)],
        [((half, D), F32), ((half, D), BF16), ((half, D), BF16, HELD)]
        + [((half, D), F32), ((half, 1), F32)],
    )
    hidden_partner = partner(hidden_mine)
    active_mine, active_held, slope_mine, hidden_partner_held = call(
        rise_kernel,
        "rise_mine",
        2.6,
        [],
        [hidden_mine, hidden_partner, w_up, row(b_up)],
        [((length, hidden), BF16), ((length, hidden), BF16, HELD), ((length, hidden), F32)]
        + [((half, D), BF16, HELD)],
    )
    active_other, active_other_held, slope_other, up_other = call(
        rise_other_kernel,
        "rise_other",
        4,
        [scalar(group % 4)],
        [after(hidden_mine, active_mine), hidden_partner, up_part, *up_parts, out_received],
        [((length, hidden), BF16), ((length, hidden), BF16, HELD), ((length, hidden), F32)]
        + [(w_up.shape, BF16)],
    )
    near, far, down_whole = call(
        fall_kernel,
        "fall",
        2.7,
        [scalar(group % 4)],
        [active_mine, active_other, w_down, down_part, *down_parts],
        [((half, D), F32), ((half, D), BF16), (w_down.shape, BF16)],
    )
    layer_out, grad_two, ffn_mine, ffn_held, sums_two = call(
        norm_two_kernel,
        "norm_two",
        1.5,
        [],
        [hidden_one, near, partner(far), row(b_down), row(gain_two), row(shift_two), grad_out],
        [((half, D), BF16, HELD), ((half, D), F32), ((half, D), BF16), ((half, D), BF16, HELD)]
        + [((SUMS, D), F32)],
    )
    ffn_partner = partner(ffn_mine)
    low_mine, low_other, near, far, sums_up, ffn_partner_held = call(
        ffn_back_kernel,
        "ffn_back",
        7,
        [],
        [ffn_mine, ffn_partner, w_down, down_whole, slope_mine, slope_other, w_up, up_other],
        [((length, hidden), BF16, HELD)] * 2
        + [((half, D), F32), ((half, D), BF16), ((SUMS, hidden), F32), ((half, D), BF16, HELD)],
    )
    count = ways // 2

    def weight_grads(name, bit, left, right, outside):
        return call(
            functools.partial(weight_grads_kernel, bit),
            name,
            4,
            [scalar(group // bit % 2)],
            [*left, *right],
            [((count, share, hidden), F32, HELD)] * 2 + [((count, share, hidden), BF16, HELD)] * 2,
            [pltpu.VMEM((D, hidden), F32)],
            outside=outside,
        )

    up_mine, up_other, up_mine_sent, up_other_sent = weight_grads(
        "up_grads", 1, (hidden_held, hidden_partner_held), (low_mine, low_other), range(4)
    )
    up_other_received = swap_dp(up_other_sent, 1)
    down_mine, down_other, down_mine_sent, down_other_sent = weight_grads(
        "down_grads",
        2,
        (after(ffn_held, up_other_sent), ffn_partner_held),
        (active_held, active_other_held),
        range(4),
    )
    down_other_received = swap_dp(down_other_sent, 2)
    grad_one, one_mine, sums = call(
        norm_one_back_kernel,
        "norm_one_back",
        1.1,
        [],
        [grad_two, after(near, down_other_sent), partner(far), normed_one, inverse_one]
        + [row(gain_one), sums_two, sums_up],
        [((half, D), F32, HELD), ((half + 3 * SUMS, D), BF16, HELD), ((SUMS, D), F32)],
    )
    one_partner = partner(one_mine)
    one_across = across(one_mine)

    low_near, columns_near, near_kept, near_sent, out_near = attend_backward(
        here, (one_mine, one_partner), w_out, weights, saved_near
    )
    (other,) = call(
        combine_kernel,
        "combine",
        100,
        [],
        [up_other, after(up_other_received, low_near), down_other, down_other_received],
        [((ways, share, hidden), BF16, HELD)],
        outside=range(4),
    )
    across_partner = partner(after(one_across, low_near))
    other_received = across(other)
    near_received = partner(after(near_sent, other))
    up_mine_received = swap_dp(after(up_mine_sent, low_near), 1)
    down_mine_received = swap_dp(after(down_mine_sent, low_near), 2)
    low_far, columns_far, far_kept, far_sent, out_far = attend_backward(
        here, (one_across, after(across_partner, other)), w_out, weights, saved_far
    )
    qkv_kept, qkv_sent = call(
        qkv_pieces_kernel,
        "qkv_pieces",
        3.7,
        [after(near_place, up_mine_received, down_mine_received, other_received), scalar(group % 2)],
        [layer_in, low_near, low_far, columns_near, columns_far, out_near, out_far, sums]
        + [one_mine, one_partner, one_across, across_partner],
        [((count, share + 3 * SUMS, 4 * width), F32, HELD)]
        + [((count, share + 3 * SUMS, 4 * width), BF16, HELD)],
        [pltpu.VMEM((D, 4 * width), F32)],
        outside=range(1, 8),
    )
    qkv_received = swap_dp(qkv_sent, 1)
    (in_far,) = call(
        sum_kernel,
        "sum_far",
        0.7,
        [],
        [far_kept, partner(after(far_sent, qkv_kept))],
        [((half, D), BF16, HELD)],
        outside=range(2),
    )
    in_other = across(in_far)
    members = jnp.stack([group // 2, group // 4 * 2 + group % 2]).astype(jnp.int32)
    terms = call(
        split_kernel,
        "split",
        1,
        [members],
        [up_mine, up_mine_received, down_mine, down_mine_received]
        + [other_received],
        [((share, hidden), BF16, HELD)] * ways,
        outside=range(5),
    )
    qkv_terms = call(
        qkv_split_kernel,
        "qkv_split",
        1,
        [members],
        [qkv_kept, qkv_received],
        [((share + 3 * SUMS, 4 * width), BF16, HELD)] * count,
        outside=range(2),
    )
    swapped = [
        terms[step] if step == 0 else swap_dp(terms[step], 2 * step) for step in range(count)
    ] + [
        terms[count + step]
        if step == 0
        else swap_dp(terms[count + step], step // 2 * 4 + step % 2)
        for step in range(count)
    ]
    swapped += [
        qkv_terms[step] if step == 0 else swap_dp(qkv_terms[step], 2 * step)
        for step in range(count)
    ]
    (grad_in,) = call(
        sum_kernel,
        "sum_in",
        1,
        [],
        [grad_one, near_kept, near_received, in_other],
        [((half, D), F32, HELD)],
        outside=range(4),
    )
    grad_query, grad_key, grad_value, grad_w_out, bias_sums, sums, grad_w_up, grad_w_down = call(
        finish_kernel,
        "finish",
        1.5,
        [],
        [after(swapped[0], grad_in), *swapped[1:]],
        [((share, width), F32, HELD)] * 3
        + [((width, share), F32, HELD), ((1, 4 * width), F32), ((SUMS, D), F32)]
        + [((share, hidden), F32, HELD), ((share, hidden), F32, HELD)],
        outside=range(ways + count),
    )
    bias_sums = bias_sums.reshape(-1)
    return (
        layer_out,
        grad_in,
        grad_query,
        bias_sums[:width],
        grad_key,
        grad_value,
        bias_sums[2 * width : 3 * width],
        grad_w_out,
        sums[0],
        sums[1],
        sums[2],
        grad_w_up,
        sums[6],
        grad_w_down.T,
        sums[3],
        sums[4],
        sums[5],
    )


def solution(mesh):
    in_specs = (
        P("dp", None),
        P("dp", None),
        P("dp", None, None),
        P(None, "tensor"),
        P("tensor"),
        P(None, "tensor"),
        P(None, "tensor"),
        P("tensor"),
        P("tensor", None),
        P(),
        P(),
        P(),
        P(None, "tensor"),
        P("tensor"),
        P("tensor", None),
        P(),
        P(),
        P(),
        P(("dp", "tensor"), None),
    )
    out_specs = (
        P(("dp", "tensor"), None),
        P(("dp", "tensor"), None),
        P("dp", "tensor"),
        P("tensor"),
        P("dp", "tensor"),
        P("dp", "tensor"),
        P("tensor"),
        P("tensor", "dp"),
        P(),
        P(),
        P(),
        P("dp", "tensor"),
        P("tensor"),
        P("tensor", "dp"),
        P(),
        P(),
        P(),
    )
    return jax.shard_map(
        on_device, mesh=mesh, in_specs=in_specs, out_specs=out_specs, check_vma=False
    )
```

```python
import functools

import jax
import jax.numpy as jnp
from jax import lax
from jax.experimental import pallas as pl
from jax.experimental.pallas import tpu as pltpu
from jax.sharding import PartitionSpec as P

D = 768
HEADS = 12
HEAD_DIM = D // HEADS

EPS = 1e-06
NEG = -1e30
ROOT_HALF = 0.7071067811865476
INV_ROOT_TWO_PI = 0.3989422804014327
BF16 = jnp.bfloat16
F32 = jnp.float32
BLOCK_MOST = 256
EXTRA = 8
COST_FLOPS = 50_000_000
COST_BYTES = 100_000
QTILE = 256
KTILE = 256
TILE = 256
SUMS = 8
ROWS = 128
HELD = True


def nn(left, right):
    return jnp.dot(left, right, preferred_element_type=F32)


def tn(left, right):
    return lax.dot_general(left, right, (((0,), (0,)), ((), ())), preferred_element_type=F32)


def nt(left, right):
    return lax.dot_general(left, right, (((1,), (1,)), ((), ())), preferred_element_type=F32)


VMEM = pl.BlockSpec(memory_space=pltpu.VMEM)
SMEM = pl.BlockSpec(memory_space=pltpu.SMEM)


def call(kernel, name, cost, scalars, arrays, outs, scratch=(), outside=()):
    arrays = [
        pltpu.with_memory_space_constraint(array, pltpu.HBM if index in outside else pltpu.VMEM)
        for index, array in enumerate(arrays)
    ]
    return pl.pallas_call(
        kernel,
        out_shape=tuple(
            pltpu.HBM(*out[:2]) if len(out) > 2 else pltpu.VMEM(*out) for out in outs
        ),
        in_specs=[SMEM] * len(scalars) + [VMEM] * len(arrays),
        out_specs=(VMEM,) * len(outs),
        scratch_shapes=list(scratch),
        cost_estimate=pl.CostEstimate(
            flops=int(cost * COST_FLOPS), bytes_accessed=int(cost * COST_BYTES), transcendentals=0
        ),
        name=name,
        compiler_params=pltpu.CompilerParams(
            vmem_limit_bytes=20 * 2**20
        ),
    )(*scalars, *arrays)


def pieces_of(column):
    high = column.astype(BF16).astype(F32)
    middle = (column - high).astype(BF16).astype(F32)
    return high, middle, column - high - middle


def with_pieces(base, lane, first, column):
    high, middle, low = pieces_of(column)
    base = jnp.where(lane == first, -high, base)
    base = jnp.where(lane == first + 1, -middle, base)
    return jnp.where(lane == first + 2, -low, base)


def lanes_of(head, rows):
    odd = lax.rem(head, 2)
    lane = lax.broadcasted_iota(jnp.int32, (rows, 2 * HEAD_DIM), 1)
    own = (lane >= HEAD_DIM * odd) & (lane < HEAD_DIM * (odd + 1))
    return odd, lane, own, HEAD_DIM * (1 - odd) + EXTRA


def forward_kernel(
    reach, place_ref, tokens_ref, w_query_ref, w_key_ref, w_value_ref, b_query_ref, b_value_ref,
    blocks_ref, links_ref, context_ref, query_ref, key_ref, value_ref,
    query_s, key_s, value_s, context_s, table_s, marks_s
):
    length = blocks_ref.shape[1]
    width = w_query_ref.shape[0]
    tiles = pl.cdiv(width, 128)
    chosen = place_ref[0]
    tokens = tokens_ref[pl.ds(pl.multiple_of(chosen * length, length), length)]
    for store, made in (
        (query_s, (nt(tokens, w_query_ref[...]) + b_query_ref[...]) * HEAD_DIM**-0.5),
        (key_s, nt(tokens, w_key_ref[...])),
        (value_s, nt(tokens, w_value_ref[...]) + b_value_ref[...]),
    ):
        for tile in range(tiles):
            last = min(128, width - 128 * tile)
            store[tile, :, :last] = made[:, 128 * tile : 128 * tile + last]

    row = blocks_ref[pl.ds(chosen, 1)].astype(F32)
    column = jnp.broadcast_to(row, (8, length)).T[:, :1]
    lane = lax.broadcasted_iota(jnp.int32, (length, 128), 1)
    onehot = jnp.where(column == lane.astype(F32), 1.0, 0.0)
    links = links_ref[chosen]
    count = links.shape[0]
    above = lax.broadcasted_iota(jnp.int32, (count, count), 0)
    below = lax.broadcasted_iota(jnp.int32, (count, count), 1)
    seen = (above == below) | ((above > below) & (links == 1))
    pairs = jnp.where(seen, 0.0, NEG).astype(BF16)
    sees = nn(onehot[:, :count].astype(BF16), pairs)
    table_s[...] = jnp.zeros_like(table_s)
    table_s[1, :, :count] = sees
    table_s[0, :, HEAD_DIM : HEAD_DIM + count] = sees
    ones = jnp.where((lane >= EXTRA) & (lane < EXTRA + 3), 1.0, onehot)
    marks_s[1] = ones
    marks_s[0] = pltpu.roll(ones, HEAD_DIM, 1)

    def one_head(head, carry):
        tile = head // 2
        odd, lane, own, first = lanes_of(head, length)
        marks = marks_s[odd]
        key_ref[head] = jnp.where(own, key_s[tile], marks).astype(BF16)
        ones = jnp.where((lane >= first) & (lane < first + 3), 1.0, 0.0)
        value_ref[head] = jnp.where(own, value_s[tile], ones).astype(BF16)
        odd, lane, own, first = lanes_of(head, QTILE)
        for start in range(0, length, QTILE):
            rows = slice(start, start + QTILE)
            seen = min(length, start + QTILE + reach)
            query = jnp.where(own, query_s[tile, rows], table_s[odd, rows])
            scores = nt(query.astype(BF16), key_ref[head, :seen])
            highest = jnp.max(scores, axis=-1, keepdims=True)
            weights = jnp.exp(scores - highest).astype(BF16)
            mixed = nn(weights, value_ref[head, :seen])
            total = jnp.sum(jnp.where(lane == first, mixed, 0.0), axis=-1, keepdims=True)
            context_s[tile, rows] = jnp.where(own, mixed * (1.0 / total), context_s[tile, rows])
            query_ref[head, rows] = with_pieces(
                query, lane, first, highest + jnp.log(total)
            ).astype(BF16)
        return carry

    lax.fori_loop(0, width // HEAD_DIM, one_head, 0)
    for tile in range(tiles):
        last = min(128, width - 128 * tile)
        context_ref[:, 128 * tile : 128 * tile + last] = context_s[tile, :, :last].astype(BF16)


def attend_forward(place, layer_in, weights, block_of, block_links):
    length = block_of.shape[1]
    width = weights[0].shape[0]
    heads = width // HEAD_DIM
    tiles = pl.cdiv(width, 128)
    big = ((heads, length, 128), BF16, HELD)
    tall = pltpu.VMEM((tiles, length, 128), F32)
    both = pltpu.VMEM((2, length, 128), F32)
    return call(
        functools.partial(forward_kernel, BLOCK_MOST),
        "attend_forward",
        8,
        [place],
        [layer_in, *weights, block_of, block_links],
        [((length, width), BF16), big, big, big],
        [tall] * 4 + [both] * 2,
        outside=range(1, 8),
    )


def backward_kernel(
    reach, core_ref, first_ref, second_ref, out_ref, w_query_ref, w_key_ref, w_value_ref,
    context_ref, query_ref, key_ref, value_ref, grads_ref, sums_ref, kept_ref, sent_ref, w_out_ref,
    grad_s, context_s, query_s, query_t, key_s, value_s, extended_s
):
    length, width = context_ref.shape
    half = length // 2
    tiles = pl.cdiv(width, 128)
    outward = jnp.zeros((width, out_ref.shape[1]), F32)
    for part, upstream_ref in enumerate((first_ref, second_ref)):
        begin = pl.multiple_of(lax.rem(core_ref[0] + part, 2) * half, half)
        rows = pl.ds(begin, half)
        upstream = upstream_ref[:half]
        made = nt(upstream, out_ref[...]).astype(BF16).astype(F32)
        context = context_ref[rows]
        outward += tn(context, upstream)
        aligned = made * context.astype(F32)
        for tile in range(tiles):
            last = min(128, width - 128 * tile)
            grad_s[tile, rows, :last] = made[:, 128 * tile : 128 * tile + last]
            context_s[tile, rows, :last] = aligned[:, 128 * tile : 128 * tile + last]
    w_out_ref[...] = outward

    def one_head(head, carry):
        tile = head // 2
        odd, lane, own, first = lanes_of(head, length)
        centre = jnp.sum(jnp.where(own, context_s[tile], 0.0), axis=-1, keepdims=True)
        grad = jnp.where(own, grad_s[tile], 0.0)
        extended_s[...] = with_pieces(grad, lane, first, centre).astype(BF16)
        odd, lane, own, first = lanes_of(head, KTILE)
        query_s[...] = jnp.zeros_like(query_s)
        for start in range(0, length, KTILE):
            rows = slice(start, start + KTILE)
            seen = max(0, start - reach)
            scores = nt(key_ref[head, rows], query_ref[head, seen:])
            probs = jnp.exp(scores)
            pulled = nt(value_ref[head, rows], extended_s[seen:])
            changed = (probs * pulled).astype(BF16)
            grad_value = nn(probs.astype(BF16), extended_s[seen:])
            grad_key = nn(changed, query_ref[head, seen:])
            value_s[tile, rows] = jnp.where(own, grad_value, value_s[tile, rows])
            key_s[tile, rows] = jnp.where(own, grad_key, key_s[tile, rows])
            query_s[seen:] += tn(changed, key_ref[head, rows])
        odd, lane, own, first = lanes_of(head, length)
        query_t[tile] = jnp.where(own, query_s[...] * HEAD_DIM**-0.5, query_t[tile])
        return carry

    lax.fori_loop(0, width // HEAD_DIM, one_head, 0)
    for kind, store in enumerate((query_t, key_s, value_s)):
        for tile in range(tiles):
            last = min(128, width - 128 * tile)
            made = store[tile, :, :last]
            begin = kind * width + 128 * tile
            grads_ref[:, begin : begin + last] = made.astype(BF16)
            if kind != 1:
                sums_ref[kind : kind + 1, 128 * tile : 128 * tile + last] = jnp.sum(
                    made, axis=0, keepdims=True
                )
    for begin, made_ref in ((1 - core_ref[0], sent_ref), (core_ref[0], kept_ref)):
        rows = pl.ds(pl.multiple_of(begin * half, half), half)
        inward = jnp.zeros(made_ref.shape, F32)
        for kind, weight_ref in enumerate((w_query_ref, w_key_ref, w_value_ref)):
            inward += nn(grads_ref[rows, kind * width : (kind + 1) * width], weight_ref[...])
        made_ref[...] = inward.astype(made_ref.dtype)


def attend_backward(core, upstream, out, weights, saved):
    length, width = saved[0].shape
    depth = out.shape[1]
    tall = pltpu.VMEM((pl.cdiv(width, 128), length, 128), F32)
    return call(
        functools.partial(backward_kernel, BLOCK_MOST),
        "attend_backward",
        12,
        [core],
        [*upstream, out, *weights, *saved],
        [
            ((length, 3 * width), BF16, HELD),
            ((3, width), F32),
            ((length // 2, depth), F32, HELD),
            ((length // 2, depth), BF16),
            ((width, depth), F32, HELD),
        ],
        [tall, tall, pltpu.VMEM((length, 128), F32), tall, tall, tall]
        + [pltpu.VMEM((length, 128), BF16)],
    )


def out_kernel(core_ref, mine_ref, other_ref, w_mine_ref, w_other_ref, far_ref, near_ref):
    width = mine_ref.shape[1]
    half = near_ref.shape[0]
    for begin, made_ref in ((1 - core_ref[0], far_ref), (core_ref[0], near_ref)):
        rows = pl.ds(pl.multiple_of(begin * half, half), half)
        made = nn(mine_ref[rows], w_mine_ref[...]) + nn(other_ref[rows], w_other_ref[:width])
        made_ref[...] = made.astype(made_ref.dtype)


def mean(values):
    return jnp.mean(values, axis=-1, keepdims=True)


def over_rows(count, rows, body, carry):
    def step(index, carry):
        return body(pl.multiple_of(index * rows, rows), carry)

    return lax.fori_loop(0, count // rows, step, carry)


def norm_one_kernel(
    place_ref, tokens_ref, near_ref, far_ref, bias_ref, gain_ref, shift_ref,
    hidden_ref, low_ref, held_ref, normed_ref, inverse_ref
):
    half = near_ref.shape[0]
    first = place_ref[0] * half

    def block(begin, carry):
        rows = pl.ds(begin, ROWS)
        tokens = tokens_ref[pl.ds(pl.multiple_of(first + begin, ROWS), ROWS)].astype(F32)
        values = tokens + near_ref[rows] + far_ref[rows].astype(F32) + bias_ref[...]
        centre = values - mean(values)
        inverse = lax.rsqrt(mean(centre * centre) + EPS)
        normed = centre * inverse
        hidden = normed * gain_ref[...] + shift_ref[...]
        hidden_ref[rows] = hidden
        low_ref[rows] = hidden.astype(BF16)
        held_ref[rows] = hidden.astype(BF16)
        normed_ref[rows] = normed
        inverse_ref[rows] = inverse
        return carry

    over_rows(half, ROWS, block, 0)


def gelu_into(up, rows, active_ref, held_ref, slope_ref):
    phi = 0.5 * (1.0 + lax.erf(up * ROOT_HALF))
    active = (up * phi).astype(BF16)
    active_ref[rows] = active
    held_ref[rows] = active
    slope_ref[rows] = phi + up * INV_ROOT_TWO_PI * jnp.exp(-0.5 * up * up)


def rise_kernel(
    mine_ref, other_ref, w_up_ref, bias_ref, active_ref, held_ref, slope_ref, other_held_ref
):
    half = mine_ref.shape[0]
    other_held_ref[...] = other_ref[...]
    for part, ref in enumerate((mine_ref, other_ref)):
        def tile(step, carry):
            begin = pl.multiple_of(step * TILE, TILE)
            up = nn(ref[pl.ds(begin, TILE)], w_up_ref[...]) + bias_ref[...]
            gelu_into(up, pl.ds(part * half + begin, TILE), active_ref, held_ref, slope_ref)
            return carry

        lax.fori_loop(0, half // TILE, tile, 0)


def join(order_ref, refs, joined_ref):
    rows = refs[0].shape[0]
    for step, ref in enumerate(refs):
        begin = jnp.bitwise_xor(order_ref[0], step) * rows
        joined_ref[pl.ds(pl.multiple_of(begin, rows), rows)] = ref[...]


def rise_other_kernel(
    order_ref, mine_ref, other_ref, *refs
):
    *pieces, out_ref, active_ref, held_ref, slope_ref, joined_ref = refs
    join(order_ref, pieces, joined_ref)
    bias = jnp.sum(out_ref[out_ref.shape[0] - 8 :].astype(F32), axis=0, keepdims=True)
    half = mine_ref.shape[0]
    for part, ref in enumerate((mine_ref, other_ref)):
        def tile(step, carry):
            begin = pl.multiple_of(step * TILE, TILE)
            up = nn(ref[pl.ds(begin, TILE)], joined_ref[...]) + bias
            gelu_into(up, pl.ds(part * half + begin, TILE), active_ref, held_ref, slope_ref)
            return carry

        lax.fori_loop(0, half // TILE, tile, 0)


def fall_kernel(order_ref, mine_ref, other_ref, w_down_ref, *refs):
    *pieces, near_ref, far_ref, joined_ref = refs
    half = near_ref.shape[0]
    join(order_ref, pieces, joined_ref)
    for begin, made_ref in ((half, far_ref), (0, near_ref)):
        def block(start, carry):
            part = pl.ds(begin + start, TILE)
            made = nn(mine_ref[part], w_down_ref[...]) + nn(other_ref[part], joined_ref[...])
            made_ref[pl.ds(start, TILE)] = made.astype(made_ref.dtype)
            return carry

        over_rows(half, TILE, block, 0)


def store_rows(sums_ref, rows):
    sums_ref[...] = jnp.zeros_like(sums_ref)
    for index, row in rows:
        sums_ref[index : index + 1] = row


def total(values):
    return jnp.sum(values, axis=0, keepdims=True)


def norm_two_kernel(
    hidden_ref, near_ref, far_ref, bias_ref, gain_ref, shift_ref, upstream_ref,
    layer_ref, grad_ref, low_ref, held_ref, sums_ref
):
    def block(begin, carry):
        rows = pl.ds(begin, ROWS)
        values = hidden_ref[rows] + near_ref[rows] + far_ref[rows].astype(F32) + bias_ref[...]
        centre = values - mean(values)
        inverse = lax.rsqrt(mean(centre * centre) + EPS)
        normed = centre * inverse
        layer_ref[rows] = (normed * gain_ref[...] + shift_ref[...]).astype(BF16)
        upstream = upstream_ref[rows].astype(F32)
        shaped = upstream * gain_ref[...]
        grad = inverse * (shaped - mean(shaped) - normed * mean(shaped * normed))
        grad_ref[rows] = grad
        low_ref[rows] = grad.astype(BF16)
        held_ref[rows] = grad.astype(BF16)
        made = (total(grad), total(upstream * normed), total(upstream))
        return tuple(old + new for old, new in zip(carry, made))

    zero = jnp.zeros((1, near_ref.shape[1]), F32)
    sums = over_rows(near_ref.shape[0], ROWS, block, (zero, zero, zero))
    store_rows(sums_ref, ((3, sums[0]), (4, sums[1]), (5, sums[2])))


def norm_one_back_kernel(
    grad_two_ref, near_ref, far_ref, normed_ref, inverse_ref, gain_ref, sums_two_ref, sums_up_ref,
    grad_ref, low_ref, sums_ref
):
    half = near_ref.shape[0]

    def block(begin, carry):
        rows = pl.ds(begin, ROWS)
        upstream = grad_two_ref[rows] + near_ref[rows] + far_ref[rows].astype(F32)
        normed = normed_ref[rows]
        shaped = upstream * gain_ref[...]
        grad = inverse_ref[rows] * (shaped - mean(shaped) - normed * mean(shaped * normed))
        grad_ref[rows] = grad
        low_ref[rows] = grad.astype(BF16)
        made = (total(grad), total(upstream * normed), total(upstream))
        return tuple(old + new for old, new in zip(carry, made))

    zero = jnp.zeros((1, near_ref.shape[1]), F32)
    sums = over_rows(half, ROWS, block, (zero, zero, zero))
    store_rows(
        sums_ref,
        (
            (0, sums[0]),
            (1, sums[1]),
            (2, sums[2]),
            (3, sums_two_ref[3:4]),
            (4, sums_two_ref[4:5]),
            (5, sums_two_ref[5:6]),
            (6, sums_up_ref[0:1]),
            (7, sums_up_ref[1:2]),
        ),
    )
    for term, rows in enumerate(pieces_of(sums_ref[...])):
        low_ref[half + term * SUMS : half + (term + 1) * SUMS] = rows.astype(BF16)


def ffn_back_kernel(
    mine_ref, other_ref, w_down_ref, joined_down_ref, slope_mine_ref, slope_other_ref,
    w_up_ref, joined_up_ref, low_mine_ref, low_other_ref, near_ref, far_ref, sums_ref, held_ref
):
    half = mine_ref.shape[0]
    held_ref[...] = other_ref[...]
    sums_ref[...] = jnp.zeros_like(sums_ref)
    for start, grads_ref, made_ref in ((half, other_ref, far_ref), (0, mine_ref, near_ref)):
        def tile(step, carry):
            begin = pl.multiple_of(step * TILE, TILE)
            rows = pl.ds(start + begin, TILE)
            grads = grads_ref[pl.ds(begin, TILE)]
            made = jnp.zeros((TILE, near_ref.shape[1]), F32)
            for index, (down_ref, slope_ref, up_ref, low_ref) in enumerate(
                (
                    (w_down_ref, slope_mine_ref, w_up_ref, low_mine_ref),
                    (joined_down_ref, slope_other_ref, joined_up_ref, low_other_ref),
                )
            ):
                grad = nt(grads, down_ref[...]) * slope_ref[rows]
                sums_ref[index : index + 1] += total(grad)
                low = grad.astype(BF16)
                low_ref[rows] = low
                made += nt(low, up_ref[...])
            made_ref[pl.ds(begin, TILE)] = made.astype(made_ref.dtype)
            return carry

        lax.fori_loop(0, half // TILE, tile, 0)


def weight_grads_kernel(
    bit, place_ref, left_mine_ref, left_other_ref, mine_ref, other_ref,
    kept_mine_ref, kept_other_ref, sent_mine_ref, sent_other_ref, whole_s
):
    half = left_mine_ref.shape[0]
    count, share = kept_mine_ref.shape[:2]
    own = place_ref[0]
    for right_ref, kept_ref, sent_ref in (
        (mine_ref, kept_mine_ref, sent_mine_ref), (other_ref, kept_other_ref, sent_other_ref)
    ):
        def block(begin, carry, right_ref=right_ref):
            columns = pl.ds(begin, TILE)
            whole_s[columns] = tn(left_mine_ref[:, columns], right_ref[:half]) + tn(
                left_other_ref[:, columns], right_ref[half:]
            )
            return carry

        over_rows(whole_s.shape[0], TILE, block, 0)
        for member in range(count):
            base = member % bit + member // bit * 2 * bit
            for parity, made_ref in ((own, kept_ref), (1 - own, sent_ref)):
                begin = pl.multiple_of((base + bit * parity) * share, 8)
                made_ref[member] = whole_s[pl.ds(begin, share)].astype(made_ref.dtype)


def combine_kernel(up_ref, up_received_ref, down_ref, down_received_ref, made_ref):
    count = up_ref.shape[0]
    for kind, (kept_ref, received_ref) in enumerate(
        ((up_ref, up_received_ref), (down_ref, down_received_ref))
    ):
        for member in range(count):
            made = kept_ref[member] + received_ref[member].astype(F32)
            made_ref[kind * count + member] = made.astype(BF16)


def split_kernel(
    members_ref, up_ref, up_received_ref, down_ref, down_received_ref, across_ref, *refs
):
    count = up_ref.shape[0]
    for kind, (kept_ref, received_ref) in enumerate(
        ((up_ref, up_received_ref), (down_ref, down_received_ref))
    ):
        for step in range(count):
            index = jnp.bitwise_xor(members_ref[kind], step)
            made = kept_ref[index] + received_ref[index].astype(F32)
            made += across_ref[kind * count + index].astype(F32)
            refs[kind * count + step][...] = made.astype(BF16)


def three_sums(values, first):
    return (
        values[first : first + SUMS]
        + values[first + SUMS : first + 2 * SUMS]
        + values[first + 2 * SUMS : first + 3 * SUMS]
    )


def qkv_split_kernel(members_ref, kept_ref, received_ref, *refs):
    count, rows = kept_ref.shape[:2]
    share = rows - 3 * SUMS
    for step in range(count):
        index = jnp.bitwise_xor(members_ref[0], step)
        made_ref = refs[step]
        made = kept_ref[index] + received_ref[index].astype(F32)
        made_ref[:share] = made[:share].astype(BF16)
        for term, part in enumerate(pieces_of(three_sums(made, share))):
            made_ref[share + term * SUMS : share + (term + 1) * SUMS] = part.astype(BF16)


def added(refs):
    made = refs[0][...].astype(F32)
    for ref in refs[1:]:
        made += ref[...].astype(F32)
    return made


def finish_kernel(*refs):
    *terms, query_ref, key_ref, value_ref, out_ref, bias_ref, sums_ref, up_ref, down_ref = refs
    count = len(terms) // 3
    share, width = query_ref.shape
    up_ref[...] = added(terms[:count])
    down_ref[...] = added(terms[count : 2 * count])
    made = added(terms[2 * count :])
    query_ref[...] = made[:share, :width]
    key_ref[...] = made[:share, width : 2 * width]
    value_ref[...] = made[:share, 2 * width : 3 * width]
    out_ref[...] = made[:share, 3 * width :].T
    sums = three_sums(made, share)
    sums_ref[...] = sums
    bias_ref[...] = sums[7:8]


def sum_kernel(*refs):
    *terms, made_ref = refs
    made = terms[0][...].astype(F32)
    for term in terms[1:]:
        made += term[...].astype(F32)
    made_ref[...] = made.astype(made_ref.dtype)


def qkv_pieces_kernel(
    place_ref, parity_ref, tokens_ref, near_ref, far_ref, sums_near_ref, sums_far_ref,
    out_near_ref, out_far_ref, norm_sums_ref, mine_ref, partner_ref, across_ref, diagonal_ref,
    kept_ref, sent_ref, whole_s
):
    count, rows = kept_ref.shape[:2]
    share = rows - 3 * SUMS
    length, columns = near_ref.shape
    width = out_near_ref.shape[0]
    half = mine_ref.shape[0] - 3 * SUMS
    made = jnp.zeros((tokens_ref.shape[1], columns), F32)
    for chosen, low_ref in ((place_ref[0], near_ref), (1 - place_ref[0], far_ref)):
        tokens = tokens_ref[pl.ds(pl.multiple_of(chosen * length, length), length)]
        made += tn(tokens, low_ref[...])
    whole_s[:, :columns] = made
    whole_s[:, columns:] = (out_near_ref[...] + out_far_ref[...]).T

    def sums_of(ref):
        terms = [ref[half + k * SUMS : half + (k + 1) * SUMS].astype(F32) for k in range(3)]
        return terms[0] + terms[1] + terms[2]

    across = sums_of(across_ref)
    sums = norm_sums_ref[...]
    row = lax.broadcasted_iota(jnp.int32, sums.shape, 0)
    bias = sums_near_ref[...] + sums_far_ref[...]
    lane = lax.broadcasted_iota(jnp.int32, (1, columns + width), 1)
    biases = jnp.concatenate(
        [bias[0:1], bias[1:2], bias[2:3], jnp.zeros((1, width), F32)], axis=1
    )
    biases = jnp.where((lane < width) | (lane >= 2 * width), biases, 0.0)
    sums = jnp.where(
        row < 6,
        sums + sums_of(partner_ref) + across + sums_of(diagonal_ref),
        jnp.where(row == 6, sums + across[7:8], biases),
    )
    terms = pieces_of(sums)
    for member in range(count):
        for parity, made_ref in ((parity_ref[0], kept_ref), (1 - parity_ref[0], sent_ref)):
            begin = pl.multiple_of((2 * member + parity) * share, 8)
            made_ref[member, :share] = whole_s[pl.ds(begin, share)].astype(made_ref.dtype)
            for k, term in enumerate(terms):
                made_ref[member, share + k * SUMS : share + (k + 1) * SUMS] = term.astype(
                    made_ref.dtype
                )


def swap_tensor(array, mask):
    ways = lax.axis_size("tensor")
    return lax.ppermute(array, "tensor", [(i, i ^ mask) for i in range(ways)])


def swap_dp(array, mask):
    ways = lax.axis_size("dp")
    return lax.ppermute(array, "dp", [(i, i ^ mask) for i in range(ways)])


def across(array):
    return swap_tensor(array, 2)


def partner(array):
    return swap_tensor(array, 1)


def after(array, *earlier):
    return lax.optimization_barrier((array,) + earlier)[0]


def three_terms(row):
    high = lax.reduce_precision(row, 8, 7)
    middle = lax.reduce_precision(row - high, 8, 7)
    terms = jnp.stack([high, middle, row - high - middle]).astype(BF16)
    return jnp.pad(terms, ((0, 5), (0, 0)))


def on_device(
    layer_in,
    block_of,
    block_links,
    w_query,
    b_query,
    w_key,
    w_value,
    b_value,
    w_out,
    b_out,
    gain_one,
    shift_one,
    w_up,
    b_up,
    w_down,
    b_down,
    gain_two,
    shift_two,
    grad_out,
):
    length = block_of.shape[1]
    half = length // 2
    place = lax.axis_index("tensor")
    sequence = place // 2
    core = place % 2
    width = w_query.shape[1]
    hidden = w_up.shape[1]
    ways = lax.axis_size("dp")
    share = D // ways
    group = lax.axis_index("dp")

    def scalar(value):
        return jnp.full((1,), value, jnp.int32)

    def row(vector):
        return vector.reshape(1, -1)

    def part_of(array, parts):
        rows = array.shape[0] // parts
        return lax.dynamic_slice_in_dim(array, group % parts * rows, rows, 0)

    def spread(part, parts):
        return [swap_dp(part, step) for step in range(1, parts)]

    out_received = across(jnp.concatenate([w_out, three_terms(b_up)], axis=0))
    up_part = across(part_of(w_up, 4))
    down_part = across(part_of(w_down, 4))

    weights = (w_query.T, w_key.T, w_value.T)
    inputs = weights + (row(b_query), row(b_value))
    near_place, far_place = scalar(sequence), scalar(1 - sequence)
    up_parts = spread(up_part, 4)
    saved_far = attend_forward(
        after(far_place, up_part), layer_in, inputs, block_of, block_links
    )
    context_other = across(saved_far[0])
    down_parts = spread(down_part, 4)
    saved_near = attend_forward(
        after(near_place, saved_far[0], down_part, *up_parts), layer_in, inputs, block_of, block_links
    )

    here = scalar(core)
    far, near = call(
        out_kernel,
        "out",
        2,
        [here],
        [after(saved_near[0], *down_parts), context_other, w_out, out_received],
        [((half, D), BF16), ((half, D), F32)],
    )
    hidden_one, hidden_mine, hidden_held, normed_one, inverse_one = call(
        norm_one_kernel,
        "norm_one",
        1,
        [scalar(place)],
        [layer_in, near, partner(far), row(b_out), row(gain_one), row(shift_one)],
        [((half, D), F32), ((half, D), BF16), ((half, D), BF16, HELD)]
        + [((half, D), F32), ((half, 1), F32)],
    )
    hidden_partner = partner(hidden_mine)
    active_mine, active_held, slope_mine, hidden_partner_held = call(
        rise_kernel,
        "rise_mine",
        2.6,
        [],
        [hidden_mine, hidden_partner, w_up, row(b_up)],
        [((length, hidden), BF16), ((length, hidden), BF16, HELD), ((length, hidden), F32)]
        + [((half, D), BF16, HELD)],
    )
    active_other, active_other_held, slope_other, up_other = call(
        rise_other_kernel,
        "rise_other",
        4,
        [scalar(group % 4)],
        [after(hidden_mine, active_mine), hidden_partner, up_part, *up_parts, out_received],
        [((length, hidden), BF16), ((length, hidden), BF16, HELD), ((length, hidden), F32)]
        + [(w_up.shape, BF16)],
    )
    near, far, down_whole = call(
        fall_kernel,
        "fall",
        2.7,
        [scalar(group % 4)],
        [active_mine, active_other, w_down, down_part, *down_parts],
        [((half, D), F32), ((half, D), BF16), (w_down.shape, BF16)],
    )
    layer_out, grad_two, ffn_mine, ffn_held, sums_two = call(
        norm_two_kernel,
        "norm_two",
        1.5,
        [],
        [hidden_one, near, partner(far), row(b_down), row(gain_two), row(shift_two), grad_out],
        [((half, D), BF16, HELD), ((half, D), F32), ((half, D), BF16), ((half, D), BF16, HELD)]
        + [((SUMS, D), F32)],
    )
    ffn_partner = partner(ffn_mine)
    low_mine, low_other, near, far, sums_up, ffn_partner_held = call(
        ffn_back_kernel,
        "ffn_back",
        7,
        [],
        [ffn_mine, ffn_partner, w_down, down_whole, slope_mine, slope_other, w_up, up_other],
        [((length, hidden), BF16, HELD)] * 2
        + [((half, D), F32), ((half, D), BF16), ((SUMS, hidden), F32), ((half, D), BF16, HELD)],
    )
    count = ways // 2

    def weight_grads(name, bit, left, right, outside):
        return call(
            functools.partial(weight_grads_kernel, bit),
            name,
            4,
            [scalar(group // bit % 2)],
            [*left, *right],
            [((count, share, hidden), F32, HELD)] * 2 + [((count, share, hidden), BF16, HELD)] * 2,
            [pltpu.VMEM((D, hidden), F32)],
            outside=outside,
        )

    up_mine, up_other, up_mine_sent, up_other_sent = weight_grads(
        "up_grads", 1, (hidden_held, hidden_partner_held), (low_mine, low_other), range(4)
    )
    up_other_received = swap_dp(up_other_sent, 1)
    down_mine, down_other, down_mine_sent, down_other_sent = weight_grads(
        "down_grads",
        2,
        (after(ffn_held, up_other_sent), ffn_partner_held),
        (active_held, active_other_held),
        range(4),
    )
    down_other_received = swap_dp(down_other_sent, 2)
    grad_one, one_mine, sums = call(
        norm_one_back_kernel,
        "norm_one_back",
        1.1,
        [],
        [grad_two, after(near, down_other_sent), partner(far), normed_one, inverse_one]
        + [row(gain_one), sums_two, sums_up],
        [((half, D), F32, HELD), ((half + 3 * SUMS, D), BF16, HELD), ((SUMS, D), F32)],
    )
    one_partner = partner(one_mine)
    one_across = across(one_mine)

    low_near, columns_near, near_kept, near_sent, out_near = attend_backward(
        here, (one_mine, one_partner), w_out, weights, saved_near
    )
    (other,) = call(
        combine_kernel,
        "combine",
        100,
        [],
        [up_other, after(up_other_received, low_near), down_other, down_other_received],
        [((ways, share, hidden), BF16, HELD)],
        outside=range(4),
    )
    across_partner = partner(after(one_across, low_near))
    other_received = across(other)
    near_received = partner(after(near_sent, other))
    up_mine_received = swap_dp(after(up_mine_sent, low_near), 1)
    down_mine_received = swap_dp(after(down_mine_sent, low_near), 2)
    low_far, columns_far, far_kept, far_sent, out_far = attend_backward(
        here, (one_across, after(across_partner, other)), w_out, weights, saved_far
    )
    qkv_kept, qkv_sent = call(
        qkv_pieces_kernel,
        "qkv_pieces",
        3.7,
        [after(near_place, up_mine_received, down_mine_received, other_received), scalar(group % 2)],
        [layer_in, low_near, low_far, columns_near, columns_far, out_near, out_far, sums]
        + [one_mine, one_partner, one_across, across_partner],
        [((count, share + 3 * SUMS, 4 * width), F32, HELD)]
        + [((count, share + 3 * SUMS, 4 * width), BF16, HELD)],
        [pltpu.VMEM((D, 4 * width), F32)],
        outside=range(1, 8),
    )
    qkv_received = swap_dp(qkv_sent, 1)
    (in_far,) = call(
        sum_kernel,
        "sum_far",
        0.7,
        [],
        [far_kept, partner(after(far_sent, qkv_kept))],
        [((half, D), BF16, HELD)],
        outside=range(2),
    )
    in_other = across(in_far)
    members = jnp.stack([group // 2, group // 4 * 2 + group % 2]).astype(jnp.int32)
    terms = call(
        split_kernel,
        "split",
        1,
        [members],
        [up_mine, up_mine_received, down_mine, down_mine_received]
        + [other_received],
        [((share, hidden), BF16, HELD)] * ways,
        outside=range(5),
    )
    qkv_terms = call(
        qkv_split_kernel,
        "qkv_split",
        1,
        [members],
        [qkv_kept, qkv_received],
        [((share + 3 * SUMS, 4 * width), BF16, HELD)] * count,
        outside=range(2),
    )
    swapped = [
        terms[step] if step == 0 else swap_dp(terms[step], 2 * step) for step in range(count)
    ] + [
        terms[count + step]
        if step == 0
        else swap_dp(terms[count + step], step // 2 * 4 + step % 2)
        for step in range(count)
    ]
    swapped += [
        qkv_terms[step] if step == 0 else swap_dp(qkv_terms[step], 2 * step)
        for step in range(count)
    ]
    (grad_in,) = call(
        sum_kernel,
        "sum_in",
        1,
        [],
        [grad_one, near_kept, near_received, in_other],
        [((half, D), F32, HELD)],
        outside=range(4),
    )
    grad_query, grad_key, grad_value, grad_w_out, bias_sums, sums, grad_w_up, grad_w_down = call(
        finish_kernel,
        "finish",
        1.5,
        [],
        [after(swapped[0], grad_in), *swapped[1:]],
        [((share, width), F32, HELD)] * 3
        + [((width, share), F32, HELD), ((1, 4 * width), F32), ((SUMS, D), F32)]
        + [((share, hidden), F32, HELD), ((share, hidden), F32, HELD)],
        outside=range(ways + count),
    )
    bias_sums = bias_sums.reshape(-1)
    return (
        layer_out,
        grad_in,
        grad_query,
        bias_sums[:width],
        grad_key,
        grad_value,
        bias_sums[2 * width : 3 * width],
        grad_w_out,
        sums[0],
        sums[1],
        sums[2],
        grad_w_up,
        sums[6],
        grad_w_down.T,
        sums[3],
        sums[4],
        sums[5],
    )


def solution(mesh):
    in_specs = (
        P("dp", None),
        P("dp", None),
        P("dp", None, None),
        P(None, "tensor"),
        P("tensor"),
        P(None, "tensor"),
        P(None, "tensor"),
        P("tensor"),
        P("tensor", None),
        P(),
        P(),
        P(),
        P(None, "tensor"),
        P("tensor"),
        P("tensor", None),
        P(),
        P(),
        P(),
        P(("dp", "tensor"), None),
    )
    out_specs = (
        P(("dp", "tensor"), None),
        P(("dp", "tensor"), None),
        P("dp", "tensor"),
        P("tensor"),
        P("dp", "tensor"),
        P("dp", "tensor"),
        P("tensor"),
        P("tensor", "dp"),
        P(),
        P(),
        P(),
        P("dp", "tensor"),
        P("tensor"),
        P("tensor", "dp"),
        P(),
        P(),
        P(),
    )
    return jax.shard_map(
        on_device, mesh=mesh, in_specs=in_specs, out_specs=out_specs, check_vma=False
    )
```

```python
import functools

import jax
import jax.numpy as jnp
from jax import lax
from jax.experimental import pallas as pl
from jax.experimental.pallas import tpu as pltpu
from jax.sharding import PartitionSpec as P

D = 768
HEADS = 12
HEAD_DIM = D // HEADS

EPS = 1e-06
NEG = -1e30
ROOT_HALF = 0.7071067811865476
INV_ROOT_TWO_PI = 0.3989422804014327
BF16 = jnp.bfloat16
F32 = jnp.float32
BLOCK_MOST = 256
EXTRA = 8
COST_FLOPS = 50_000_000
COST_BYTES = 100_000
QTILE = 256
KTILE = 256
TILE = 256
SUMS = 8
ROWS = 128
WIDE = 384
HELD = True


def nn(left, right):
    return jnp.dot(left, right, preferred_element_type=F32)


def tn(left, right):
    return lax.dot_general(left, right, (((0,), (0,)), ((), ())), preferred_element_type=F32)


def nt(left, right):
    return lax.dot_general(left, right, (((1,), (1,)), ((), ())), preferred_element_type=F32)


VMEM = pl.BlockSpec(memory_space=pltpu.VMEM)
SMEM = pl.BlockSpec(memory_space=pltpu.SMEM)


def call(kernel, name, cost, scalars, arrays, outs, scratch=(), outside=()):
    arrays = [
        pltpu.with_memory_space_constraint(array, pltpu.HBM if index in outside else pltpu.VMEM)
        for index, array in enumerate(arrays)
    ]
    return pl.pallas_call(
        kernel,
        out_shape=tuple(
            pltpu.HBM(*out[:2]) if len(out) > 2 else pltpu.VMEM(*out) for out in outs
        ),
        in_specs=[SMEM] * len(scalars) + [VMEM] * len(arrays),
        out_specs=(VMEM,) * len(outs),
        scratch_shapes=list(scratch),
        cost_estimate=pl.CostEstimate(
            flops=int(cost * COST_FLOPS), bytes_accessed=int(cost * COST_BYTES), transcendentals=0
        ),
        name=name,
        compiler_params=pltpu.CompilerParams(
            vmem_limit_bytes=20 * 2**20
        ),
    )(*scalars, *arrays)


def pieces_of(column):
    high = column.astype(BF16).astype(F32)
    middle = (column - high).astype(BF16).astype(F32)
    return high, middle, column - high - middle


def with_pieces(base, lane, first, column):
    high, middle, low = pieces_of(column)
    base = jnp.where(lane == first, -high, base)
    base = jnp.where(lane == first + 1, -middle, base)
    return jnp.where(lane == first + 2, -low, base)


def lanes_of(head, rows):
    odd = lax.rem(head, 2)
    lane = lax.broadcasted_iota(jnp.int32, (rows, 2 * HEAD_DIM), 1)
    own = (lane >= HEAD_DIM * odd) & (lane < HEAD_DIM * (odd + 1))
    return odd, lane, own, HEAD_DIM * (1 - odd) + EXTRA


def forward_kernel(
    reach, place_ref, tokens_ref, w_query_ref, w_key_ref, w_value_ref, b_query_ref, b_value_ref,
    blocks_ref, links_ref, context_ref, query_ref, key_ref, value_ref,
    query_s, key_s, value_s, context_s, table_s, marks_s
):
    length = blocks_ref.shape[1]
    width = w_query_ref.shape[0]
    tiles = pl.cdiv(width, 128)
    chosen = place_ref[0]
    tokens = tokens_ref[pl.ds(pl.multiple_of(chosen * length, length), length)]
    for store, made in (
        (query_s, (nt(tokens, w_query_ref[...]) + b_query_ref[...]) * HEAD_DIM**-0.5),
        (key_s, nt(tokens, w_key_ref[...])),
        (value_s, nt(tokens, w_value_ref[...]) + b_value_ref[...]),
    ):
        for tile in range(tiles):
            last = min(128, width - 128 * tile)
            store[tile, :, :last] = made[:, 128 * tile : 128 * tile + last]

    row = blocks_ref[pl.ds(chosen, 1)].astype(F32)
    column = jnp.broadcast_to(row, (8, length)).T[:, :1]
    lane = lax.broadcasted_iota(jnp.int32, (length, 128), 1)
    onehot = jnp.where(column == lane.astype(F32), 1.0, 0.0)
    links = links_ref[chosen]
    count = links.shape[0]
    above = lax.broadcasted_iota(jnp.int32, (count, count), 0)
    below = lax.broadcasted_iota(jnp.int32, (count, count), 1)
    seen = (above == below) | ((above > below) & (links == 1))
    pairs = jnp.where(seen, 0.0, NEG).astype(BF16)
    sees = nn(onehot[:, :count].astype(BF16), pairs)
    table_s[...] = jnp.zeros_like(table_s)
    table_s[1, :, :count] = sees
    table_s[0, :, HEAD_DIM : HEAD_DIM + count] = sees
    ones = jnp.where((lane >= EXTRA) & (lane < EXTRA + 3), 1.0, onehot)
    marks_s[1] = ones
    marks_s[0] = pltpu.roll(ones, HEAD_DIM, 1)

    def one_head(head, carry):
        tile = head // 2
        odd, lane, own, first = lanes_of(head, length)
        marks = marks_s[odd]
        key_ref[head] = jnp.where(own, key_s[tile], marks).astype(BF16)
        ones = jnp.where((lane >= first) & (lane < first + 3), 1.0, 0.0)
        value_ref[head] = jnp.where(own, value_s[tile], ones).astype(BF16)
        odd, lane, own, first = lanes_of(head, QTILE)
        for start in range(0, length, QTILE):
            rows = slice(start, start + QTILE)
            seen = min(length, start + QTILE + reach)
            query = jnp.where(own, query_s[tile, rows], table_s[odd, rows])
            scores = nt(query.astype(BF16), key_ref[head, :seen])
            highest = jnp.max(scores, axis=-1, keepdims=True)
            weights = jnp.exp(scores - highest).astype(BF16)
            mixed = nn(weights, value_ref[head, :seen])
            total = jnp.sum(jnp.where(lane == first, mixed, 0.0), axis=-1, keepdims=True)
            context_s[tile, rows] = jnp.where(own, mixed * (1.0 / total), context_s[tile, rows])
            query_ref[head, rows] = with_pieces(
                query, lane, first, highest + jnp.log(total)
            ).astype(BF16)
        return carry

    lax.fori_loop(0, width // HEAD_DIM, one_head, 0)
    for tile in range(tiles):
        last = min(128, width - 128 * tile)
        context_ref[:, 128 * tile : 128 * tile + last] = context_s[tile, :, :last].astype(BF16)


def attend_forward(place, layer_in, weights, block_of, block_links):
    length = block_of.shape[1]
    width = weights[0].shape[0]
    heads = width // HEAD_DIM
    tiles = pl.cdiv(width, 128)
    big = ((heads, length, 128), BF16, HELD)
    tall = pltpu.VMEM((tiles, length, 128), F32)
    both = pltpu.VMEM((2, length, 128), F32)
    return call(
        functools.partial(forward_kernel, BLOCK_MOST),
        "attend_forward",
        8,
        [place],
        [layer_in, *weights, block_of, block_links],
        [((length, width), BF16), big, big, big],
        [tall] * 4 + [both] * 2,
        outside=range(1, 8),
    )


def backward_kernel(
    reach, core_ref, first_ref, second_ref, out_ref, w_query_ref, w_key_ref, w_value_ref,
    context_ref, query_ref, key_ref, value_ref, grads_ref, sums_ref, kept_ref, sent_ref, w_out_ref,
    grad_s, context_s, query_s, query_t, key_s, value_s, extended_s
):
    length, width = context_ref.shape
    half = length // 2
    tiles = pl.cdiv(width, 128)
    outward = jnp.zeros((width, out_ref.shape[1]), F32)
    for part, upstream_ref in enumerate((first_ref, second_ref)):
        begin = pl.multiple_of(lax.rem(core_ref[0] + part, 2) * half, half)
        rows = pl.ds(begin, half)
        upstream = upstream_ref[:half]
        made = nt(upstream, out_ref[...]).astype(BF16).astype(F32)
        context = context_ref[rows]
        outward += tn(context, upstream)
        aligned = made * context.astype(F32)
        for tile in range(tiles):
            last = min(128, width - 128 * tile)
            grad_s[tile, rows, :last] = made[:, 128 * tile : 128 * tile + last]
            context_s[tile, rows, :last] = aligned[:, 128 * tile : 128 * tile + last]
    w_out_ref[...] = outward

    def one_head(head, carry):
        tile = head // 2
        odd, lane, own, first = lanes_of(head, length)
        centre = jnp.sum(jnp.where(own, context_s[tile], 0.0), axis=-1, keepdims=True)
        grad = jnp.where(own, grad_s[tile], 0.0)
        extended_s[...] = with_pieces(grad, lane, first, centre).astype(BF16)
        odd, lane, own, first = lanes_of(head, KTILE)
        query_s[...] = jnp.zeros_like(query_s)
        for start in range(0, length, KTILE):
            rows = slice(start, start + KTILE)
            seen = max(0, start - reach)
            scores = nt(key_ref[head, rows], query_ref[head, seen:])
            probs = jnp.exp(scores)
            pulled = nt(value_ref[head, rows], extended_s[seen:])
            changed = (probs * pulled).astype(BF16)
            grad_value = nn(probs.astype(BF16), extended_s[seen:])
            grad_key = nn(changed, query_ref[head, seen:])
            value_s[tile, rows] = jnp.where(own, grad_value, value_s[tile, rows])
            key_s[tile, rows] = jnp.where(own, grad_key, key_s[tile, rows])
            query_s[seen:] += tn(changed, key_ref[head, rows])
        odd, lane, own, first = lanes_of(head, length)
        query_t[tile] = jnp.where(own, query_s[...] * HEAD_DIM**-0.5, query_t[tile])
        return carry

    lax.fori_loop(0, width // HEAD_DIM, one_head, 0)
    for kind, store in enumerate((query_t, key_s, value_s)):
        for tile in range(tiles):
            last = min(128, width - 128 * tile)
            made = store[tile, :, :last]
            begin = kind * width + 128 * tile
            grads_ref[:, begin : begin + last] = made.astype(BF16)
            if kind != 1:
                sums_ref[kind : kind + 1, 128 * tile : 128 * tile + last] = jnp.sum(
                    made, axis=0, keepdims=True
                )
    for begin, made_ref in ((1 - core_ref[0], sent_ref), (core_ref[0], kept_ref)):
        rows = pl.ds(pl.multiple_of(begin * half, half), half)
        inward = jnp.zeros(made_ref.shape, F32)
        for kind, weight_ref in enumerate((w_query_ref, w_key_ref, w_value_ref)):
            inward += nn(grads_ref[rows, kind * width : (kind + 1) * width], weight_ref[...])
        made_ref[...] = inward.astype(made_ref.dtype)


def attend_backward(core, upstream, out, weights, saved):
    length, width = saved[0].shape
    depth = out.shape[1]
    tall = pltpu.VMEM((pl.cdiv(width, 128), length, 128), F32)
    return call(
        functools.partial(backward_kernel, BLOCK_MOST),
        "attend_backward",
        12,
        [core],
        [*upstream, out, *weights, *saved],
        [
            ((length, 3 * width), BF16, HELD),
            ((3, width), F32),
            ((length // 2, depth), F32, HELD),
            ((length // 2, depth), BF16),
            ((width, depth), F32, HELD),
        ],
        [tall, tall, pltpu.VMEM((length, 128), F32), tall, tall, tall]
        + [pltpu.VMEM((length, 128), BF16)],
    )


def out_kernel(core_ref, mine_ref, other_ref, w_mine_ref, w_other_ref, far_ref, near_ref):
    width = mine_ref.shape[1]
    half = near_ref.shape[0]
    for begin, made_ref in ((1 - core_ref[0], far_ref), (core_ref[0], near_ref)):
        rows = pl.ds(pl.multiple_of(begin * half, half), half)
        made = nn(mine_ref[rows], w_mine_ref[...]) + nn(other_ref[rows], w_other_ref[:width])
        made_ref[...] = made.astype(made_ref.dtype)


def mean(values):
    return jnp.mean(values, axis=-1, keepdims=True)


def over_rows(count, rows, body, carry):
    def step(index, carry):
        return body(pl.multiple_of(index * rows, rows), carry)

    return lax.fori_loop(0, count // rows, step, carry)


def norm_one_kernel(
    place_ref, tokens_ref, near_ref, far_ref, bias_ref, gain_ref, shift_ref,
    hidden_ref, low_ref, held_ref, normed_ref, inverse_ref
):
    half = near_ref.shape[0]
    first = place_ref[0] * half

    def block(begin, carry):
        rows = pl.ds(begin, ROWS)
        tokens = tokens_ref[pl.ds(pl.multiple_of(first + begin, ROWS), ROWS)].astype(F32)
        values = tokens + near_ref[rows] + far_ref[rows].astype(F32) + bias_ref[...]
        centre = values - mean(values)
        inverse = lax.rsqrt(mean(centre * centre) + EPS)
        normed = centre * inverse
        hidden = normed * gain_ref[...] + shift_ref[...]
        hidden_ref[rows] = hidden
        low_ref[rows] = hidden.astype(BF16)
        held_ref[rows] = hidden.astype(BF16)
        normed_ref[rows] = normed
        inverse_ref[rows] = inverse
        return carry

    over_rows(half, ROWS, block, 0)


def gelu_into(up, rows, active_ref, held_ref, slope_ref):
    phi = 0.5 * (1.0 + lax.erf(up * ROOT_HALF))
    active = (up * phi).astype(BF16)
    active_ref[rows] = active
    held_ref[rows] = active
    slope_ref[rows] = phi + up * INV_ROOT_TWO_PI * jnp.exp(-0.5 * up * up)


def rise_kernel(
    mine_ref, other_ref, w_up_ref, bias_ref, active_ref, held_ref, slope_ref, other_held_ref
):
    half = mine_ref.shape[0]
    other_held_ref[...] = other_ref[...]
    for part, ref in enumerate((mine_ref, other_ref)):
        def tile(step, carry):
            begin = pl.multiple_of(step * TILE, TILE)
            up = nn(ref[pl.ds(begin, TILE)], w_up_ref[...]) + bias_ref[...]
            gelu_into(up, pl.ds(part * half + begin, TILE), active_ref, held_ref, slope_ref)
            return carry

        lax.fori_loop(0, half // TILE, tile, 0)


def join(order_ref, refs, joined_ref):
    rows = refs[0].shape[0]
    for step, ref in enumerate(refs):
        begin = jnp.bitwise_xor(order_ref[0], step) * rows
        joined_ref[pl.ds(pl.multiple_of(begin, rows), rows)] = ref[...]


def rise_other_kernel(
    order_ref, mine_ref, other_ref, *refs
):
    *pieces, out_ref, active_ref, held_ref, slope_ref, joined_ref = refs
    join(order_ref, pieces, joined_ref)
    bias = jnp.sum(out_ref[out_ref.shape[0] - 8 :].astype(F32), axis=0, keepdims=True)
    half = mine_ref.shape[0]
    for part, ref in enumerate((mine_ref, other_ref)):
        def tile(step, carry):
            begin = pl.multiple_of(step * TILE, TILE)
            up = nn(ref[pl.ds(begin, TILE)], joined_ref[...]) + bias
            gelu_into(up, pl.ds(part * half + begin, TILE), active_ref, held_ref, slope_ref)
            return carry

        lax.fori_loop(0, half // TILE, tile, 0)


def fall_kernel(order_ref, mine_ref, other_ref, w_down_ref, *refs):
    *pieces, near_ref, far_ref, joined_ref = refs
    half = near_ref.shape[0]
    join(order_ref, pieces, joined_ref)
    for begin, made_ref in ((half, far_ref), (0, near_ref)):
        def block(start, carry):
            part = pl.ds(begin + start, TILE)
            made = nn(mine_ref[part], w_down_ref[...]) + nn(other_ref[part], joined_ref[...])
            made_ref[pl.ds(start, TILE)] = made.astype(made_ref.dtype)
            return carry

        over_rows(half, TILE, block, 0)


def store_rows(sums_ref, rows):
    sums_ref[...] = jnp.zeros_like(sums_ref)
    for index, row in rows:
        sums_ref[index : index + 1] = row


def total(values):
    return jnp.sum(values, axis=0, keepdims=True)


def norm_two_kernel(
    hidden_ref, near_ref, far_ref, bias_ref, gain_ref, shift_ref, upstream_ref,
    layer_ref, grad_ref, low_ref, held_ref, sums_ref
):
    def block(begin, carry):
        rows = pl.ds(begin, ROWS)
        values = hidden_ref[rows] + near_ref[rows] + far_ref[rows].astype(F32) + bias_ref[...]
        centre = values - mean(values)
        inverse = lax.rsqrt(mean(centre * centre) + EPS)
        normed = centre * inverse
        layer_ref[rows] = (normed * gain_ref[...] + shift_ref[...]).astype(BF16)
        upstream = upstream_ref[rows].astype(F32)
        shaped = upstream * gain_ref[...]
        grad = inverse * (shaped - mean(shaped) - normed * mean(shaped * normed))
        grad_ref[rows] = grad
        low_ref[rows] = grad.astype(BF16)
        held_ref[rows] = grad.astype(BF16)
        made = (total(grad), total(upstream * normed), total(upstream))
        return tuple(old + new for old, new in zip(carry, made))

    zero = jnp.zeros((1, near_ref.shape[1]), F32)
    sums = over_rows(near_ref.shape[0], ROWS, block, (zero, zero, zero))
    store_rows(sums_ref, ((3, sums[0]), (4, sums[1]), (5, sums[2])))


def norm_one_back_kernel(
    grad_two_ref, near_ref, far_ref, normed_ref, inverse_ref, gain_ref, sums_two_ref, sums_up_ref,
    grad_ref, low_ref, sums_ref
):
    half = near_ref.shape[0]

    def block(begin, carry):
        rows = pl.ds(begin, ROWS)
        upstream = grad_two_ref[rows] + near_ref[rows] + far_ref[rows].astype(F32)
        normed = normed_ref[rows]
        shaped = upstream * gain_ref[...]
        grad = inverse_ref[rows] * (shaped - mean(shaped) - normed * mean(shaped * normed))
        grad_ref[rows] = grad
        low_ref[rows] = grad.astype(BF16)
        made = (total(grad), total(upstream * normed), total(upstream))
        return tuple(old + new for old, new in zip(carry, made))

    zero = jnp.zeros((1, near_ref.shape[1]), F32)
    sums = over_rows(half, ROWS, block, (zero, zero, zero))
    store_rows(
        sums_ref,
        (
            (0, sums[0]),
            (1, sums[1]),
            (2, sums[2]),
            (3, sums_two_ref[3:4]),
            (4, sums_two_ref[4:5]),
            (5, sums_two_ref[5:6]),
            (6, sums_up_ref[0:1]),
            (7, sums_up_ref[1:2]),
        ),
    )
    for term, rows in enumerate(pieces_of(sums_ref[...])):
        low_ref[half + term * SUMS : half + (term + 1) * SUMS] = rows.astype(BF16)


def ffn_back_kernel(
    mine_ref, other_ref, w_down_ref, joined_down_ref, slope_mine_ref, slope_other_ref,
    w_up_ref, joined_up_ref, low_mine_ref, low_other_ref, near_ref, far_ref, sums_ref, held_ref
):
    half = mine_ref.shape[0]
    held_ref[...] = other_ref[...]
    sums_ref[...] = jnp.zeros_like(sums_ref)
    for start, grads_ref, made_ref in ((half, other_ref, far_ref), (0, mine_ref, near_ref)):
        def tile(step, carry):
            begin = pl.multiple_of(step * TILE, TILE)
            rows = pl.ds(start + begin, TILE)
            grads = grads_ref[pl.ds(begin, TILE)]
            made = jnp.zeros((TILE, near_ref.shape[1]), F32)
            for index, (down_ref, slope_ref, up_ref, low_ref) in enumerate(
                (
                    (w_down_ref, slope_mine_ref, w_up_ref, low_mine_ref),
                    (joined_down_ref, slope_other_ref, joined_up_ref, low_other_ref),
                )
            ):
                grad = nt(grads, down_ref[...]) * slope_ref[rows]
                sums_ref[index : index + 1] += total(grad)
                low = grad.astype(BF16)
                low_ref[rows] = low
                made += nt(low, up_ref[...])
            made_ref[pl.ds(begin, TILE)] = made.astype(made_ref.dtype)
            return carry

        lax.fori_loop(0, half // TILE, tile, 0)


def weight_grads_kernel(
    bit, place_ref, left_mine_ref, left_other_ref, mine_ref, other_ref,
    kept_mine_ref, kept_other_ref, sent_mine_ref, sent_other_ref, whole_s
):
    half = left_mine_ref.shape[0]
    count, share = kept_mine_ref.shape[:2]
    own = place_ref[0]
    for right_ref, kept_ref, sent_ref in (
        (mine_ref, kept_mine_ref, sent_mine_ref), (other_ref, kept_other_ref, sent_other_ref)
    ):
        def block(begin, carry, right_ref=right_ref):
            columns = pl.ds(begin, WIDE)
            whole_s[columns] = tn(left_mine_ref[:, columns], right_ref[:half]) + tn(
                left_other_ref[:, columns], right_ref[half:]
            )
            return carry

        over_rows(whole_s.shape[0], WIDE, block, 0)
        for member in range(count):
            base = member % bit + member // bit * 2 * bit
            for parity, made_ref in ((own, kept_ref), (1 - own, sent_ref)):
                begin = pl.multiple_of((base + bit * parity) * share, 8)
                made_ref[member] = whole_s[pl.ds(begin, share)].astype(made_ref.dtype)


def combine_kernel(up_ref, up_received_ref, down_ref, down_received_ref, made_ref):
    count = up_ref.shape[0]
    for kind, (kept_ref, received_ref) in enumerate(
        ((up_ref, up_received_ref), (down_ref, down_received_ref))
    ):
        for member in range(count):
            made = kept_ref[member] + received_ref[member].astype(F32)
            made_ref[kind * count + member] = made.astype(BF16)


def split_kernel(
    members_ref, up_ref, up_received_ref, down_ref, down_received_ref, across_ref, *refs
):
    count = up_ref.shape[0]
    for kind, (kept_ref, received_ref) in enumerate(
        ((up_ref, up_received_ref), (down_ref, down_received_ref))
    ):
        for step in range(count):
            index = jnp.bitwise_xor(members_ref[kind], step)
            made = kept_ref[index] + received_ref[index].astype(F32)
            made += across_ref[kind * count + index].astype(F32)
            refs[kind * count + step][...] = made.astype(BF16)


def three_sums(values, first):
    return (
        values[first : first + SUMS]
        + values[first + SUMS : first + 2 * SUMS]
        + values[first + 2 * SUMS : first + 3 * SUMS]
    )


def qkv_split_kernel(members_ref, kept_ref, received_ref, *refs):
    count, rows = kept_ref.shape[:2]
    share = rows - 3 * SUMS
    for step in range(count):
        index = jnp.bitwise_xor(members_ref[0], step)
        made_ref = refs[step]
        made = kept_ref[index] + received_ref[index].astype(F32)
        made_ref[:share] = made[:share].astype(BF16)
        for term, part in enumerate(pieces_of(three_sums(made, share))):
            made_ref[share + term * SUMS : share + (term + 1) * SUMS] = part.astype(BF16)


def added(refs):
    made = refs[0][...].astype(F32)
    for ref in refs[1:]:
        made += ref[...].astype(F32)
    return made


def finish_kernel(*refs):
    *terms, query_ref, key_ref, value_ref, out_ref, bias_ref, sums_ref, up_ref, down_ref = refs
    count = len(terms) // 3
    share, width = query_ref.shape
    up_ref[...] = added(terms[:count])
    down_ref[...] = added(terms[count : 2 * count])
    made = added(terms[2 * count :])
    query_ref[...] = made[:share, :width]
    key_ref[...] = made[:share, width : 2 * width]
    value_ref[...] = made[:share, 2 * width : 3 * width]
    out_ref[...] = made[:share, 3 * width :].T
    sums = three_sums(made, share)
    sums_ref[...] = sums
    bias_ref[...] = sums[7:8]


def sum_kernel(*refs):
    *terms, made_ref = refs
    made = terms[0][...].astype(F32)
    for term in terms[1:]:
        made += term[...].astype(F32)
    made_ref[...] = made.astype(made_ref.dtype)


def qkv_pieces_kernel(
    place_ref, parity_ref, tokens_ref, near_ref, far_ref, sums_near_ref, sums_far_ref,
    out_near_ref, out_far_ref, norm_sums_ref, mine_ref, partner_ref, across_ref, diagonal_ref,
    kept_ref, sent_ref, whole_s
):
    count, rows = kept_ref.shape[:2]
    share = rows - 3 * SUMS
    length, columns = near_ref.shape
    width = out_near_ref.shape[0]
    half = mine_ref.shape[0] - 3 * SUMS
    made = jnp.zeros((tokens_ref.shape[1], columns), F32)
    for chosen, low_ref in ((place_ref[0], near_ref), (1 - place_ref[0], far_ref)):
        tokens = tokens_ref[pl.ds(pl.multiple_of(chosen * length, length), length)]
        made += tn(tokens, low_ref[...])
    whole_s[:, :columns] = made
    whole_s[:, columns:] = (out_near_ref[...] + out_far_ref[...]).T

    def sums_of(ref):
        terms = [ref[half + k * SUMS : half + (k + 1) * SUMS].astype(F32) for k in range(3)]
        return terms[0] + terms[1] + terms[2]

    across = sums_of(across_ref)
    sums = norm_sums_ref[...]
    row = lax.broadcasted_iota(jnp.int32, sums.shape, 0)
    bias = sums_near_ref[...] + sums_far_ref[...]
    lane = lax.broadcasted_iota(jnp.int32, (1, columns + width), 1)
    biases = jnp.concatenate(
        [bias[0:1], bias[1:2], bias[2:3], jnp.zeros((1, width), F32)], axis=1
    )
    biases = jnp.where((lane < width) | (lane >= 2 * width), biases, 0.0)
    sums = jnp.where(
        row < 6,
        sums + sums_of(partner_ref) + across + sums_of(diagonal_ref),
        jnp.where(row == 6, sums + across[7:8], biases),
    )
    terms = pieces_of(sums)
    for member in range(count):
        for parity, made_ref in ((parity_ref[0], kept_ref), (1 - parity_ref[0], sent_ref)):
            begin = pl.multiple_of((2 * member + parity) * share, 8)
            made_ref[member, :share] = whole_s[pl.ds(begin, share)].astype(made_ref.dtype)
            for k, term in enumerate(terms):
                made_ref[member, share + k * SUMS : share + (k + 1) * SUMS] = term.astype(
                    made_ref.dtype
                )


def swap_tensor(array, mask):
    ways = lax.axis_size("tensor")
    return lax.ppermute(array, "tensor", [(i, i ^ mask) for i in range(ways)])


def swap_dp(array, mask):
    ways = lax.axis_size("dp")
    return lax.ppermute(array, "dp", [(i, i ^ mask) for i in range(ways)])


def across(array):
    return swap_tensor(array, 2)


def partner(array):
    return swap_tensor(array, 1)


def after(array, *earlier):
    return lax.optimization_barrier((array,) + earlier)[0]


def three_terms(row):
    high = lax.reduce_precision(row, 8, 7)
    middle = lax.reduce_precision(row - high, 8, 7)
    terms = jnp.stack([high, middle, row - high - middle]).astype(BF16)
    return jnp.pad(terms, ((0, 5), (0, 0)))


def on_device(
    layer_in,
    block_of,
    block_links,
    w_query,
    b_query,
    w_key,
    w_value,
    b_value,
    w_out,
    b_out,
    gain_one,
    shift_one,
    w_up,
    b_up,
    w_down,
    b_down,
    gain_two,
    shift_two,
    grad_out,
):
    length = block_of.shape[1]
    half = length // 2
    place = lax.axis_index("tensor")
    sequence = place // 2
    core = place % 2
    width = w_query.shape[1]
    hidden = w_up.shape[1]
    ways = lax.axis_size("dp")
    share = D // ways
    group = lax.axis_index("dp")

    def scalar(value):
        return jnp.full((1,), value, jnp.int32)

    def row(vector):
        return vector.reshape(1, -1)

    def part_of(array, parts):
        rows = array.shape[0] // parts
        return lax.dynamic_slice_in_dim(array, group % parts * rows, rows, 0)

    def spread(part, parts):
        return [swap_dp(part, step) for step in range(1, parts)]

    out_received = across(jnp.concatenate([w_out, three_terms(b_up)], axis=0))
    up_part = across(part_of(w_up, 4))
    down_part = across(part_of(w_down, 4))

    weights = (w_query.T, w_key.T, w_value.T)
    inputs = weights + (row(b_query), row(b_value))
    near_place, far_place = scalar(sequence), scalar(1 - sequence)
    up_parts = spread(up_part, 4)
    saved_far = attend_forward(
        after(far_place, up_part), layer_in, inputs, block_of, block_links
    )
    context_other = across(saved_far[0])
    down_parts = spread(down_part, 4)
    saved_near = attend_forward(
        after(near_place, saved_far[0], down_part, *up_parts), layer_in, inputs, block_of, block_links
    )

    here = scalar(core)
    far, near = call(
        out_kernel,
        "out",
        2,
        [here],
        [after(saved_near[0], *down_parts), context_other, w_out, out_received],
        [((half, D), BF16), ((half, D), F32)],
    )
    hidden_one, hidden_mine, hidden_held, normed_one, inverse_one = call(
        norm_one_kernel,
        "norm_one",
        1,
        [scalar(place)],
        [layer_in, near, partner(far), row(b_out), row(gain_one), row(shift_one)],
        [((half, D), F32), ((half, D), BF16), ((half, D), BF16, HELD)]
        + [((half, D), F32), ((half, 1), F32)],
    )
    hidden_partner = partner(hidden_mine)
    active_mine, active_held, slope_mine, hidden_partner_held = call(
        rise_kernel,
        "rise_mine",
        2.6,
        [],
        [hidden_mine, hidden_partner, w_up, row(b_up)],
        [((length, hidden), BF16), ((length, hidden), BF16, HELD), ((length, hidden), F32)]
        + [((half, D), BF16, HELD)],
    )
    active_other, active_other_held, slope_other, up_other = call(
        rise_other_kernel,
        "rise_other",
        4,
        [scalar(group % 4)],
        [after(hidden_mine, active_mine), hidden_partner, up_part, *up_parts, out_received],
        [((length, hidden), BF16), ((length, hidden), BF16, HELD), ((length, hidden), F32)]
        + [(w_up.shape, BF16)],
    )
    near, far, down_whole = call(
        fall_kernel,
        "fall",
        2.7,
        [scalar(group % 4)],
        [active_mine, active_other, w_down, down_part, *down_parts],
        [((half, D), F32), ((half, D), BF16), (w_down.shape, BF16)],
    )
    layer_out, grad_two, ffn_mine, ffn_held, sums_two = call(
        norm_two_kernel,
        "norm_two",
        1.5,
        [],
        [hidden_one, near, partner(far), row(b_down), row(gain_two), row(shift_two), grad_out],
        [((half, D), BF16, HELD), ((half, D), F32), ((half, D), BF16), ((half, D), BF16, HELD)]
        + [((SUMS, D), F32)],
    )
    ffn_partner = partner(ffn_mine)
    low_mine, low_other, near, far, sums_up, ffn_partner_held = call(
        ffn_back_kernel,
        "ffn_back",
        7,
        [],
        [ffn_mine, ffn_partner, w_down, down_whole, slope_mine, slope_other, w_up, up_other],
        [((length, hidden), BF16, HELD)] * 2
        + [((half, D), F32), ((half, D), BF16), ((SUMS, hidden), F32), ((half, D), BF16, HELD)],
    )
    count = ways // 2

    def weight_grads(name, bit, left, right, outside):
        return call(
            functools.partial(weight_grads_kernel, bit),
            name,
            4,
            [scalar(group // bit % 2)],
            [*left, *right],
            [((count, share, hidden), F32, HELD)] * 2 + [((count, share, hidden), BF16, HELD)] * 2,
            [pltpu.VMEM((D, hidden), F32)],
            outside=outside,
        )

    up_mine, up_other, up_mine_sent, up_other_sent = weight_grads(
        "up_grads", 1, (hidden_held, hidden_partner_held), (low_mine, low_other), range(4)
    )
    up_other_received = swap_dp(up_other_sent, 1)
    down_mine, down_other, down_mine_sent, down_other_sent = weight_grads(
        "down_grads",
        2,
        (after(ffn_held, up_other_sent), ffn_partner_held),
        (active_held, active_other_held),
        range(4),
    )
    down_other_received = swap_dp(down_other_sent, 2)
    grad_one, one_mine, sums = call(
        norm_one_back_kernel,
        "norm_one_back",
        1.1,
        [],
        [grad_two, after(near, down_other_sent), partner(far), normed_one, inverse_one]
        + [row(gain_one), sums_two, sums_up],
        [((half, D), F32, HELD), ((half + 3 * SUMS, D), BF16, HELD), ((SUMS, D), F32)],
    )
    one_partner = partner(one_mine)
    one_across = across(one_mine)

    low_near, columns_near, near_kept, near_sent, out_near = attend_backward(
        here, (one_mine, one_partner), w_out, weights, saved_near
    )
    (other,) = call(
        combine_kernel,
        "combine",
        100,
        [],
        [up_other, after(up_other_received, low_near), down_other, down_other_received],
        [((ways, share, hidden), BF16, HELD)],
        outside=range(4),
    )
    across_partner = partner(after(one_across, low_near))
    other_received = across(other)
    near_received = partner(after(near_sent, other))
    up_mine_received = swap_dp(after(up_mine_sent, low_near), 1)
    down_mine_received = swap_dp(after(down_mine_sent, low_near), 2)
    low_far, columns_far, far_kept, far_sent, out_far = attend_backward(
        here, (one_across, after(across_partner, other)), w_out, weights, saved_far
    )
    qkv_kept, qkv_sent = call(
        qkv_pieces_kernel,
        "qkv_pieces",
        3.7,
        [after(near_place, up_mine_received, down_mine_received, other_received), scalar(group % 2)],
        [layer_in, low_near, low_far, columns_near, columns_far, out_near, out_far, sums]
        + [one_mine, one_partner, one_across, across_partner],
        [((count, share + 3 * SUMS, 4 * width), F32, HELD)]
        + [((count, share + 3 * SUMS, 4 * width), BF16, HELD)],
        [pltpu.VMEM((D, 4 * width), F32)],
        outside=range(1, 8),
    )
    qkv_received = swap_dp(qkv_sent, 1)
    (in_far,) = call(
        sum_kernel,
        "sum_far",
        0.7,
        [],
        [far_kept, partner(after(far_sent, qkv_kept))],
        [((half, D), BF16, HELD)],
        outside=range(2),
    )
    in_other = across(in_far)
    members = jnp.stack([group // 2, group // 4 * 2 + group % 2]).astype(jnp.int32)
    terms = call(
        split_kernel,
        "split",
        1,
        [members],
        [up_mine, up_mine_received, down_mine, down_mine_received]
        + [other_received],
        [((share, hidden), BF16, HELD)] * ways,
        outside=range(5),
    )
    qkv_terms = call(
        qkv_split_kernel,
        "qkv_split",
        1,
        [members],
        [qkv_kept, qkv_received],
        [((share + 3 * SUMS, 4 * width), BF16, HELD)] * count,
        outside=range(2),
    )
    swapped = [
        terms[step] if step == 0 else swap_dp(terms[step], 2 * step) for step in range(count)
    ] + [
        terms[count + step]
        if step == 0
        else swap_dp(terms[count + step], step // 2 * 4 + step % 2)
        for step in range(count)
    ]
    swapped += [
        qkv_terms[step] if step == 0 else swap_dp(qkv_terms[step], 2 * step)
        for step in range(count)
    ]
    (grad_in,) = call(
        sum_kernel,
        "sum_in",
        1,
        [],
        [grad_one, near_kept, near_received, in_other],
        [((half, D), F32, HELD)],
        outside=range(4),
    )
    grad_query, grad_key, grad_value, grad_w_out, bias_sums, sums, grad_w_up, grad_w_down = call(
        finish_kernel,
        "finish",
        1.5,
        [],
        [after(swapped[0], grad_in), *swapped[1:]],
        [((share, width), F32, HELD)] * 3
        + [((width, share), F32, HELD), ((1, 4 * width), F32), ((SUMS, D), F32)]
        + [((share, hidden), F32, HELD), ((share, hidden), F32, HELD)],
        outside=range(ways + count),
    )
    bias_sums = bias_sums.reshape(-1)
    return (
        layer_out,
        grad_in,
        grad_query,
        bias_sums[:width],
        grad_key,
        grad_value,
        bias_sums[2 * width : 3 * width],
        grad_w_out,
        sums[0],
        sums[1],
        sums[2],
        grad_w_up,
        sums[6],
        grad_w_down.T,
        sums[3],
        sums[4],
        sums[5],
    )


def solution(mesh):
    in_specs = (
        P("dp", None),
        P("dp", None),
        P("dp", None, None),
        P(None, "tensor"),
        P("tensor"),
        P(None, "tensor"),
        P(None, "tensor"),
        P("tensor"),
        P("tensor", None),
        P(),
        P(),
        P(),
        P(None, "tensor"),
        P("tensor"),
        P("tensor", None),
        P(),
        P(),
        P(),
        P(("dp", "tensor"), None),
    )
    out_specs = (
        P(("dp", "tensor"), None),
        P(("dp", "tensor"), None),
        P("dp", "tensor"),
        P("tensor"),
        P("dp", "tensor"),
        P("dp", "tensor"),
        P("tensor"),
        P("tensor", "dp"),
        P(),
        P(),
        P(),
        P("dp", "tensor"),
        P("tensor"),
        P("tensor", "dp"),
        P(),
        P(),
        P(),
    )
    return jax.shard_map(
        on_device, mesh=mesh, in_specs=in_specs, out_specs=out_specs, check_vma=False
    )
```
